32 devices in a mesh: gx: 4 (over x, core), gy: 4 (over z), gz: 2 (over y).
Axes of the slice: x: 2, y: 2, z: 4, core: 2. Of those that a mesh axis runs over, the one named last changes fastest.
Arguments:
- embeds: bfloat16 [256, 128, 2048], P(('gx', 'gy', 'gz')), may hold values from -6 to 6
- dest_device: int32 [256], P(('gx', 'gy', 'gz')), may hold values from 0 to 31, as said below
- shuffle_key: int32 [256], P(('gx', 'gy', 'gz')), may hold values from 0 to 255, each once
- lengths: int32 [8], replicated, may hold values from 1 to 4096
- gain: float32 [2048], replicated, may hold values from 0.1 to 1.9
Outputs:
- packed: bfloat16 [512, 128, 2048], P(('gx', 'gy', 'gz'))
The draws below stay inside these ranges and needn't reach their ends.
Inputs may be any that keep to these rules, and one draw needn't show every extreme that they name: `dest_device`: device numbers are ((gx * 4) + gy) * 2 + gz. A device receives at most 16 tiles, and in every draw some devices receive exactly 16. The 2 devices sharing gx and gy send at most one tile to any one device and exactly 8 tiles to the devices of each gz index. Of one device's tiles at most 4 go to devices of one gz index, and some device reaches that.
All inputs are finite; a program needn't handle non-finite values.
Results may differ from the reference program's by a relative error of at most 0.001.
Values may be sent and summed in bfloat16 or wider, within the bound.
A program may use at most 128 MiB of HBM per device.

```python
import jax
import jax.numpy as jnp
from jax import lax

D = 2048
TILE = 128
TILES_SEQ = 32
TILES_DEV = 8
DEPTH = 2
GROUPS = 16
CAP = 16
TILES = 256
SEQ_LEN = 4096
SEQS = 8


def draw_dest_device(key, part):
    k_amount, k_label, k_column, k_shift = jax.random.split(key, 4)
    half = GROUPS // 2
    amount = jax.random.randint(k_amount, (DEPTH, half), 0, TILES_DEV + 1)
    amount = amount.at[:, 0].set(TILES_DEV)
    loads = jnp.concatenate([TILES_DEV + amount, TILES_DEV - amount], axis=1)
    labels = jax.vmap(lambda k: jax.random.permutation(k, GROUPS))(jax.random.split(k_label, DEPTH))
    columns = jax.vmap(lambda k: jax.random.permutation(k, GROUPS))(jax.random.split(k_column, DEPTH))
    shift = jax.random.randint(k_shift, (GROUPS,), 0, DEPTH)
    ends = jnp.cumsum(loads, axis=1)
    group = jnp.arange(GROUPS)[:, None, None]
    height = jnp.arange(DEPTH)[None, :, None]
    local = jnp.arange(TILES_DEV)[None, None, :]
    within = height * TILES_DEV + local
    target_z = (within + shift[:, None, None]) % DEPTH
    order = within // DEPTH
    column = columns[target_z, group]
    spot = column + GROUPS * order
    label_index = jnp.sum((spot[..., None] >= ends[target_z]).astype(jnp.int32), axis=-1)
    target_group = labels[target_z, label_index]
    return (target_group * DEPTH + target_z).reshape(-1).astype(jnp.int32)


def set_ends(array, rng, low, largest):
    place = [jax.random.randint(jax.random.fold_in(rng, axis), (), 0, length) for axis, length in enumerate(array.shape)]
    longest = array.shape.index(max(array.shape))
    beside = place[:longest] + [(place[longest] + 1) % array.shape[longest]] + place[longest + 1:]
    return array.at[tuple(place)].set(low).at[tuple(beside)].set(largest)


def steps_of(stream_key, dims, cuts, least, largest):
    level = 1.0
    for dim, shards_of in cuts:
        draws = jax.random.uniform(jax.random.fold_in(jax.random.fold_in(stream_key, 6), dim), (shards_of,), jnp.float32, least / len(cuts), largest / len(cuts))
        level = level * jnp.repeat(jnp.exp(draws), dims[dim] // shards_of).reshape((-1,) + (1,) * (len(dims) - 1 - dim))
    return level


def centred(own_key, dims, scale, most, shards=(), kind=jnp.bfloat16):
    result = jax.random.normal(own_key, dims, jnp.float32) * scale
    if len(shards) > 0:
        result = steps_of(own_key, dims, shards, -0.22, 0.18) * result
    return jnp.clip(result, min=-most, max=most).astype(kind)


def setup_inputs(seed: int = 0) -> dict:
    streams_of = jax.random.split(jax.random.key(seed), 6)
    embeds = centred(streams_of[0], (TILES, TILE, D), 1.0, 6.0, ((0, 32),))
    dest_device = draw_dest_device(jax.random.fold_in(streams_of[5], 71), 0)
    shuffle_key = jax.random.permutation(streams_of[2], TILES).astype(jnp.int32)
    lengths = set_ends(jax.random.randint(streams_of[3], (SEQS,), 1, SEQ_LEN + 1), jax.random.fold_in(streams_of[3], 1), 1, SEQ_LEN).astype(jnp.int32)
    gain = jnp.clip(1.0 + 0.18 * jax.random.normal(streams_of[4], (D,), jnp.float32), 0.1, 1.9)
    return {"embeds": embeds, "dest_device": dest_device, "shuffle_key": shuffle_key, "lengths": lengths, "gain": gain}


def normalize(rows, tile_ids, lengths, gain):
    values = rows.astype(jnp.float32)
    meansq = lax.optimization_barrier(jnp.mean(values * values, axis=-1, keepdims=True))
    scaled = values * lax.rsqrt(jnp.maximum(meansq, 0.25)) * gain.astype(jnp.float32)
    limit = lengths[tile_ids // TILES_SEQ]
    position = (tile_ids % TILES_SEQ)[:, None] * TILE + jnp.arange(TILE, dtype=jnp.int32)[None, :]
    keep = position < limit[:, None]
    return jnp.where(keep[:, :, None], scaled, 0.0).astype(jnp.bfloat16)

def reference(embeds, dest_device, shuffle_key, lengths, gain):
    tile_ids = jnp.arange(TILES, dtype=jnp.int32)
    normed = normalize(embeds, tile_ids, lengths, gain)
    same = dest_device[:, None] == dest_device[None, :]
    earlier = shuffle_key[None, :] < shuffle_key[:, None]
    rank = lax.optimization_barrier(jnp.sum((same & earlier).astype(jnp.int32), axis=1)).astype(jnp.int32)
    slots = (dest_device * CAP + rank).astype(jnp.int32)
    packed = jnp.zeros((GROUPS * DEPTH * CAP, TILE, D), jnp.bfloat16)
    return packed.at[slots].set(normed)
```

```python
import functools

import jax
import jax.numpy as jnp
from jax import lax
from jax.experimental import pallas as pl
from jax.experimental.pallas import tpu as pltpu
from jax.sharding import PartitionSpec as P

TILES_SEQ = 32
CLASSES = (10, 12, 16)
CHUNKS = (1, 1, 2, 2, 2, 2, 2, 2, 1, 1)
MESH = pl.DeviceIdType.MESH


def exchange_kernel(
    sizes, small_in, x_ref, gain_ref, recv_ref, keys_ref,
    small_ref, gain, small_sem, first_table, limit_table, note_out, notes, note_table, second, keys_out,
    x_sem, gain_sem, y_send, y_recv, g_send, g_recv, own_sem,
    note_send, note_recv, note_sem, key_send, key_recv, *buffers,
):
    nx, ny, depth, per_peer, chunk_rows = sizes
    chunks = len(chunk_rows)
    starts = [sum(chunk_rows[:c]) for c in range(chunks)]
    groups = nx * ny
    tiles_here, tile_rows, _ = x_ref.shape
    raw, first, arrived, outgoing = (buffers[i * chunks : (i + 1) * chunks] for i in range(4))
    gx, gy, gz = lax.axis_index("gx"), lax.axis_index("gy"), lax.axis_index("gz")
    group = gx * ny + gy
    me = group * depth + gz
    offsets = [(dx, dy) for dy in sorted(range(ny), key=lambda d: abs(d - ny // 2)) for dx in range(nx)]
    offsets.remove((0, 0))

    def load(c):
        return pltpu.make_async_copy(
            x_ref.at[:, pl.ds(starts[c], chunk_rows[c])], raw[c], x_sem.at[c]
        )

    def fill_tables():
        depths = [lax.rem(small_ref[0, i], depth) for i in range(tiles_here)]
        dest_groups = [lax.div(small_ref[0, i], depth) for i in range(tiles_here)]
        places, limits = [], []
        for i in range(tiles_here):
            spot = jnp.int32(0)
            for j in range(i):
                spot = spot + jnp.where(depths[j] == depths[i], 1, 0)
            places.append(depths[i] * per_peer + spot)
            tile = me * tiles_here + i
            length = small_ref[0, 2 * tiles_here + tile // TILES_SEQ]
            limits.append(jnp.maximum(length - tile % TILES_SEQ * tile_rows, 0))
        lane = lax.broadcasted_iota(jnp.int32, note_out.shape[1:], 1)
        for z in range(depth):
            row = jnp.zeros(note_out.shape[1:], jnp.int32)
            for p in range(per_peer):
                slot = z * per_peer + p
                tile, limit, dest_group, key = (jnp.int32(v) for v in (0, 0, -1, 0))
                for i in range(tiles_here):
                    hit = places[i] == slot
                    tile = jnp.where(hit, i, tile)
                    limit = jnp.where(hit, limits[i], limit)
                    dest_group = jnp.where(hit, dest_groups[i], dest_group)
                    key = jnp.where(hit, small_ref[0, tiles_here + i] + 1, key)
                first_table[slot] = tile
                limit_table[slot] = limit
                row = jnp.where(lane == p, dest_group, row)
                row = jnp.where(lane == per_peer + p, key, row)
            note_out[z] = row

    def normed(c, slot):
        rows = chunk_rows[c]
        values = raw[c][first_table[slot]].astype(jnp.float32)
        meansq = jnp.mean(values * values, axis=-1, keepdims=True)
        scaled = values * lax.rsqrt(jnp.maximum(meansq, 0.25)) * gain[...]
        row = starts[c] + lax.broadcasted_iota(jnp.int32, (rows, 1), 0)
        return jnp.where(row < limit_table[slot], scaled, 0.0).astype(jnp.bfloat16)

    def y_copy(c, dz, peer, origin):
        return pltpu.make_async_remote_copy(
            src_ref=first[c].at[dz - 1],
            dst_ref=arrived[c].at[pl.ds(origin * per_peer, per_peer)],
            send_sem=y_send.at[c, dz - 1],
            recv_sem=y_recv.at[c, dz - 1],
            device_id=(gx, gy, peer),
            device_id_type=MESH,
        )

    def peer_of(k):
        dx, dy = offsets[k]
        return lax.rem(gx + dx, nx), lax.rem(gy + dy, ny)

    def g_copy(c, k, px, py, origin):
        return pltpu.make_async_remote_copy(
            src_ref=outgoing[c].at[k],
            dst_ref=recv_ref.at[origin, pl.ds(starts[c], chunk_rows[c])],
            send_sem=g_send.at[c, k],
            recv_sem=g_recv.at[c, k],
            device_id=(px, py, gz),
            device_id_type=MESH,
        )

    def own_copy(c):
        return pltpu.make_async_copy(
            outgoing[c].at[groups - 1],
            recv_ref.at[group, pl.ds(starts[c], chunk_rows[c])],
            own_sem.at[c],
        )

    def note_copy(dz, peer, place):
        return pltpu.make_async_remote_copy(
            src_ref=note_out.at[peer],
            dst_ref=notes.at[place],
            send_sem=note_send.at[dz - 1],
            recv_sem=note_recv.at[dz - 1],
            device_id=(gx, gy, peer),
            device_id_type=MESH,
        )

    def key_copy(k, px, py, place):
        return pltpu.make_async_remote_copy(
            src_ref=keys_out.at[k],
            dst_ref=keys_ref.at[place],
            send_sem=key_send.at[k],
            recv_sem=key_recv.at[k],
            device_id=(px, py, gz),
            device_id_type=MESH,
        )

    def prepare(c):
        load(c).wait()
        for dz in range(1, depth):
            peer = lax.rem(gz + dz, depth)
            for p in range(per_peer):
                first[c][dz - 1, p] = normed(c, peer * per_peer + p)
        for p in range(per_peer):
            arrived[c][gz * per_peer + p] = normed(c, gz * per_peer + p)

    def send_first(c):
        for dz in range(1, depth):
            y_copy(c, dz, lax.rem(gz + dz, depth), gz).start()

    def find_slots():
        for dz in range(1, depth):
            origin = lax.rem(gz + depth - dz, depth)
            note_copy(dz, origin, origin).wait()
        tables = [
            pltpu.make_async_copy(
                notes.at[lax.rem(gz + dz, depth)], note_table.at[lax.rem(gz + dz, depth)], note_sem.at[dz]
            )
            for dz in range(1, depth)
        ]
        tables.append(pltpu.make_async_copy(note_out.at[gz], note_table.at[gz], note_sem.at[0]))
        for copy in tables:
            copy.start()
        for copy in tables:
            copy.wait()

        for k in range(groups):
            px, py = peer_of(k) if k < groups - 1 else (gx, gy)
            wanted = px * ny + py
            slot, key = jnp.int32(0), jnp.int32(0)
            for z in range(depth):
                for p in range(per_peer):
                    hit = note_table[z, 0, p] == wanted
                    slot = jnp.where(hit, z * per_peer + p, slot)
                    key = jnp.where(hit, note_table[z, 0, per_peer + p], key)
            second[k] = slot
            row = jnp.full(keys_out.shape[1:], key, jnp.int32)
            if k < groups - 1:
                keys_out[k] = row
            else:
                keys_ref[group] = row

    def forward(c):
        for dz in range(1, depth):
            origin = lax.rem(gz + depth - dz, depth)
            y_copy(c, dz, origin, origin).wait_recv()
        for k in range(groups):
            outgoing[c][k] = arrived[c][second[k]]
        for k in range(groups - 1):
            px, py = peer_of(k)
            g_copy(c, k, px, py, group).start()
        own_copy(c).start()

    small = [
        pltpu.make_async_copy(small_in, small_ref, small_sem),
        pltpu.make_async_copy(gain_ref, gain, gain_sem),
    ]
    for copy in small:
        copy.start()
    for c in range(chunks):
        load(c).start()
    barrier = pltpu.get_barrier_semaphore()
    for dz in range(1, depth):
        pl.semaphore_signal(
            barrier, inc=1, device_id=(gx, gy, lax.rem(gz + dz, depth)), device_id_type=MESH
        )
    for k in range(groups - 1):
        px, py = peer_of(k)
        pl.semaphore_signal(barrier, inc=1, device_id=(px, py, gz), device_id_type=MESH)
    for copy in small:
        copy.wait()
    fill_tables()
    prepare(0)
    pl.semaphore_wait(barrier, depth - 1 + groups - 1)
    for dz in range(1, depth):
        note_copy(dz, lax.rem(gz + dz, depth), gz).start()
    send_first(0)
    if chunks > 1:
        prepare(1)
        send_first(1)
    find_slots()
    forward(0)
    for k in range(groups - 1):
        px, py = peer_of(k)
        key_copy(k, px, py, group).start()
    for c in range(2, chunks):
        prepare(c)
        send_first(c)
        forward(c - 1)
    if chunks > 1:
        forward(chunks - 1)

    for c in range(chunks):
        for dz in range(1, depth):
            y_copy(c, dz, lax.rem(gz + dz, depth), gz).wait_send()
    sources = []
    for dx, dy in offsets:
        sources.append((lax.rem(gx + nx - dx, nx), lax.rem(gy + ny - dy, ny)))
    for k, (sx, sy) in enumerate(sources):
        key_copy(k, sx, sy, sx * ny + sy).wait()
    for c in range(chunks):
        for k, (sx, sy) in enumerate(sources):
            g_copy(c, k, sx, sy, sx * ny + sy).wait()
        own_copy(c).wait()


def place_kernel(source_ref, filled_ref, blocks_ref, out_ref, zeros, out_sem):
    cap = out_ref.shape[0]

    def store(slot):
        return pltpu.make_async_copy(blocks_ref.at[source_ref[slot]], out_ref.at[slot], out_sem.at[slot])

    for slot in range(cap):
        pl.when(filled_ref[slot] == 1)(lambda slot=slot: store(slot).start())
    zeros[...] = jnp.zeros_like(zeros)
    for slot in range(cap):

        @pl.when(filled_ref[slot] == 0)
        def _():
            pltpu.make_async_copy(zeros, out_ref.at[slot], out_sem.at[slot]).start()

    for slot in range(cap):
        store(slot).wait()


def direct(embeds, dest_device, shuffle_key, lengths, gain):
    tiles_here, tile_rows, width = embeds.shape
    nx, ny, depth = lax.axis_size("gx"), lax.axis_size("gy"), lax.axis_size("gz")
    groups = nx * ny
    per_peer = (tiles_here + depth - 1) // depth
    slots = depth * per_peer
    chunk_rows = (tile_rows,)
    if tile_rows % 128 == 0:
        chunk_rows = tuple(part * tile_rows // 16 for part in (1, 1, 2, 2, 4, 4, 2))
    chunks = len(chunk_rows)

    smem = pl.BlockSpec(memory_space=pltpu.SMEM)
    vmem = pl.BlockSpec(memory_space=pltpu.VMEM)
    hbm = pl.BlockSpec(memory_space=pl.ANY)
    lanes = -(-2 * per_peer // 128) * 128
    small = jnp.concatenate([dest_device, shuffle_key, lengths])
    small = jnp.pad(small, (0, -small.shape[0] % 128))[None, :]
    received, key_rows = pl.pallas_call(
        functools.partial(exchange_kernel, (nx, ny, depth, per_peer, chunk_rows)),
        out_shape=(
            jax.ShapeDtypeStruct((groups, tile_rows, width), jnp.bfloat16),
            jax.ShapeDtypeStruct((groups, 1, 128), jnp.int32),
        ),
        in_specs=[hbm] * 3,
        out_specs=(hbm, vmem),
        scratch_shapes=[
            pltpu.SMEM(small.shape, jnp.int32),
            pltpu.VMEM((1, width), jnp.float32),
            pltpu.SemaphoreType.DMA,
            pltpu.SMEM((slots,), jnp.int32),
            pltpu.SMEM((slots,), jnp.int32),
            pltpu.VMEM((depth, 1, lanes), jnp.int32),
            pltpu.VMEM((depth, 1, lanes), jnp.int32),
            pltpu.SMEM((depth, 1, lanes), jnp.int32),
            pltpu.SMEM((groups,), jnp.int32),
            pltpu.VMEM((groups, 1, 128), jnp.int32),
            pltpu.SemaphoreType.DMA((chunks,)),
            pltpu.SemaphoreType.DMA,
            pltpu.SemaphoreType.DMA((chunks, depth - 1)),
            pltpu.SemaphoreType.DMA((chunks, depth - 1)),
            pltpu.SemaphoreType.DMA((chunks, groups)),
            pltpu.SemaphoreType.DMA((chunks, groups)),
            pltpu.SemaphoreType.DMA((chunks,)),
            pltpu.SemaphoreType.DMA((depth,)),
            pltpu.SemaphoreType.DMA((depth,)),
            pltpu.SemaphoreType.DMA((depth,)),
            pltpu.SemaphoreType.DMA((groups,)),
            pltpu.SemaphoreType.DMA((groups,)),
        ]
        + [pltpu.VMEM((tiles_here, rows, width), jnp.bfloat16) for rows in chunk_rows]
        + [pltpu.VMEM((depth - 1, per_peer, rows, width), jnp.bfloat16) for rows in chunk_rows]
        + [pltpu.VMEM((slots, rows, width), jnp.bfloat16) for rows in chunk_rows]
        + [pltpu.VMEM((groups, rows, width), jnp.bfloat16) for rows in chunk_rows],
        compiler_params=pltpu.CompilerParams(
            collective_id=0, has_side_effects=True, vmem_limit_bytes=36 * 1024 * 1024
        ),
        name="exchange",
    )(small, embeds, gain.reshape(1, width))

    key_of = key_rows[:, 0, 0]
    valid = key_of > 0
    rank = jnp.sum((valid[None, :] & (key_of[None, :] < key_of[:, None])).astype(jnp.int32), axis=1)
    cap = 2 * tiles_here
    at = valid[None, :] & (rank[None, :] == jnp.arange(cap, dtype=jnp.int32)[:, None])
    source = jnp.sum(jnp.where(at, jnp.arange(groups, dtype=jnp.int32)[None, :], 0), axis=1).astype(jnp.int32)
    filled = jnp.sum(at.astype(jnp.int32), axis=1).astype(jnp.int32)

    return pl.pallas_call(
        place_kernel,
        out_shape=jax.ShapeDtypeStruct((cap, tile_rows, width), jnp.bfloat16),
        in_specs=[smem, smem, vmem],
        out_specs=hbm,
        scratch_shapes=[
            pltpu.VMEM((tile_rows, width), jnp.bfloat16),
            pltpu.SemaphoreType.DMA((cap,)),
        ],
        compiler_params=pltpu.CompilerParams(vmem_limit_bytes=24 * 1024 * 1024),
        name="place",
    )(source, filled, received)


def table_kernel(sizes, mine_ref, table_ref, send, recv):
    nx, ny, depth = sizes
    devices = nx * ny * depth
    me = (lax.axis_index("gx") * ny + lax.axis_index("gy")) * depth + lax.axis_index("gz")

    def place_of(device):
        return lax.div(device, ny * depth), lax.rem(lax.div(device, depth), ny), lax.rem(device, depth)

    def row_copy(step, target, row):
        return pltpu.make_async_remote_copy(
            src_ref=mine_ref,
            dst_ref=table_ref.at[row],
            send_sem=send.at[step - 1],
            recv_sem=recv.at[step - 1],
            device_id=place_of(target),
            device_id_type=MESH,
        )

    barrier = pltpu.get_barrier_semaphore()
    for step in range(1, devices):
        pl.semaphore_signal(
            barrier, inc=1, device_id=place_of(lax.rem(me + step, devices)), device_id_type=MESH
        )
    table_ref[me] = mine_ref[...]
    pl.semaphore_wait(barrier, devices - 1)
    for step in range(1, devices):
        row_copy(step, lax.rem(me + step, devices), me).start()
    for step in range(1, devices):
        source = lax.rem(me + devices - step, devices)
        row_copy(step, source, source).wait()


def line_kernel(
    sizes, plan_ref, x_ref, gain_ref, out_ref,
    plan, gain, plan_sem, gain_sem, x_sem, y_send, y_recv, a_send, a_recv, b_send, b_recv,
    g_send, g_recv, out_sem, *buffers,
):
    nx, ny, depth, per_peer, chunk_rows, near, far, back, at = sizes
    chunks = len(chunk_rows)
    starts = [sum(chunk_rows[:c]) for c in range(chunks)]
    half = ny // 2
    slots = depth * per_peer
    cap = out_ref.shape[0]
    raw, first, pool, inflow, inward, outward, outgoing, received, staged = (
        buffers[i * chunks : (i + 1) * chunks] for i in range(9)
    )
    gx, gy, gz = lax.axis_index("gx"), lax.axis_index("gy"), lax.axis_index("gz")
    low = gy < half
    level = jnp.where(low, gy, ny - 1 - gy)
    inner = jnp.where(low, gy + 1, gy - 1)
    outer = jnp.clip(jnp.where(low, gy - 1, gy + 1), 0, ny - 1)
    middle = level == half - 1

    def load(c):
        return pltpu.make_async_copy(
            x_ref.at[:, pl.ds(starts[c], chunk_rows[c])], raw[c], x_sem.at[c]
        )

    def normed(c, slot):
        rows = chunk_rows[c]
        values = raw[c][plan[0, at["tile"] + slot]].astype(jnp.float32)
        meansq = jnp.mean(values * values, axis=-1, keepdims=True)
        scaled = values * lax.rsqrt(jnp.maximum(meansq, 0.25)) * gain[...]
        row = starts[c] + lax.broadcasted_iota(jnp.int32, (rows, 1), 0)
        return jnp.where(row < plan[0, at["limit"] + slot], scaled, 0.0).astype(jnp.bfloat16)

    def y_copy(c, dz, peer, origin):
        return pltpu.make_async_remote_copy(
            src_ref=first[c].at[dz - 1],
            dst_ref=pool[c].at[pl.ds(origin * per_peer, per_peer)],
            send_sem=y_send.at[c, dz - 1],
            recv_sem=y_recv.at[c, dz - 1],
            device_id=(gx, gy, peer),
            device_id_type=MESH,
        )

    def near_copy(c, peer):
        return pltpu.make_async_remote_copy(
            src_ref=inward[c].at[pl.ds(0, near)],
            dst_ref=pool[c].at[pl.ds(slots, near)],
            send_sem=a_send.at[c],
            recv_sem=a_recv.at[c],
            device_id=(gx, peer, gz),
            device_id_type=MESH,
        )

    def cross_copy(c, peer):
        return pltpu.make_async_remote_copy(
            src_ref=inward[c],
            dst_ref=inflow[c],
            send_sem=a_send.at[c],
            recv_sem=b_recv.at[c],
            device_id=(gx, peer, gz),
            device_id_type=MESH,
        )

    def back_copy(c, peer):
        return pltpu.make_async_remote_copy(
            src_ref=outward[c],
            dst_ref=inflow[c].at[pl.ds(0, back)],
            send_sem=b_send.at[c],
            recv_sem=b_recv.at[c],
            device_id=(gx, peer, gz),
            device_id_type=MESH,
        )

    def g_copy(c, dx, peer, origin):
        return pltpu.make_async_remote_copy(
            src_ref=outgoing[c].at[dx - 1],
            dst_ref=received[c].at[pl.ds(origin * ny, ny)],
            send_sem=g_send.at[c, dx - 1],
            recv_sem=g_recv.at[c, dx - 1],
            device_id=(peer, gy, gz),
            device_id_type=MESH,
        )

    def out_copy(c):
        return pltpu.make_async_copy(
            staged[c], out_ref.at[:, pl.ds(starts[c], chunk_rows[c])], out_sem.at[c]
        )

    def prepare(c):
        load(c).wait()
        for dz in range(1, depth):
            peer = lax.rem(gz + dz, depth)
            for p in range(per_peer):
                first[c][dz - 1, p] = normed(c, peer * per_peer + p)
        for dz in range(1, depth):
            y_copy(c, dz, lax.rem(gz + dz, depth), gz).start()
        for p in range(per_peer):
            pool[c][gz * per_peer + p] = normed(c, gz * per_peer + p)

    def either(c, code):
        held = pool[c][jnp.clip(code, 0, slots + near - 1)]
        came = inflow[c][jnp.clip(code - slots - near, 0, far - 1)]
        return jnp.where(code < slots + near, held, came)

    def send_inward(c):
        for dz in range(1, depth):
            origin = lax.rem(gz + depth - dz, depth)
            y_copy(c, dz, origin, origin).wait_recv()

        @pl.when(level > 0)
        def _():
            near_copy(c, outer).wait_recv()

        @pl.loop(0, far)
        def _(p):
            inward[c][p] = pool[c][plan[0, at["inward"] + p]]

        @pl.when(middle)
        def _():
            cross_copy(c, inner).start()

        @pl.when(jnp.logical_not(middle))
        def _():
            near_copy(c, inner).start()

    def deliver(c):
        @pl.when(middle)
        def _():
            cross_copy(c, inner).wait_recv()

        @pl.when(jnp.logical_not(middle))
        def _():
            back_copy(c, inner).wait_recv()

        @pl.when(level > 0)
        def _():
            @pl.loop(0, back)
            def _(p):
                outward[c][p] = either(c, plan[0, at["outward"] + p])

            back_copy(c, outer).start()

        for dx in range(1, nx):
            peer = lax.rem(gx + dx, nx)

            @pl.loop(0, ny)
            def _(k):
                outgoing[c][dx - 1, k] = either(c, plan[0, at["deliver"] + peer * ny + k])

        for dx in range(1, nx):
            g_copy(c, dx, lax.rem(gx + dx, nx), gx).start()

        @pl.loop(0, ny)
        def _(k):
            received[c][gx * ny + k] = either(c, plan[0, at["deliver"] + gx * ny + k])

    def place(c):
        for dx in range(1, nx):
            origin = lax.rem(gx + nx - dx, nx)
            g_copy(c, dx, origin, origin).wait_recv()

        @pl.loop(0, cap)
        def _(slot):
            source = plan[0, at["place"] + slot]
            found = received[c][jnp.maximum(source, 0)]
            staged[c][slot] = jnp.where(source >= 0, found, jnp.zeros_like(found))

        out_copy(c).start()

    small = [
        pltpu.make_async_copy(plan_ref, plan, plan_sem),
        pltpu.make_async_copy(gain_ref, gain, gain_sem),
    ]
    for copy in small:
        copy.start()
    for c in range(chunks):
        load(c).start()
    barrier = pltpu.get_barrier_semaphore()
    for dz in range(1, depth):
        pl.semaphore_signal(
            barrier, inc=1, device_id=(gx, gy, lax.rem(gz + dz, depth)), device_id_type=MESH
        )
    for dx in range(1, nx):
        pl.semaphore_signal(
            barrier, inc=1, device_id=(lax.rem(gx + dx, nx), gy, gz), device_id_type=MESH
        )
    pl.semaphore_signal(barrier, inc=1, device_id=(gx, inner, gz), device_id_type=MESH)

    @pl.when(level > 0)
    def _():
        pl.semaphore_signal(barrier, inc=1, device_id=(gx, outer, gz), device_id_type=MESH)

    for copy in small:
        copy.wait()
    pl.semaphore_wait(barrier, depth - 1 + nx - 1 + 1 + jnp.where(level > 0, 1, 0))

    ahead = 4
    for step in range(chunks + ahead + 2):
        if step < chunks:
            prepare(step)
        if 0 <= step - 1 < chunks:
            send_inward(step - 1)
        if 0 <= step - 1 - ahead < chunks:
            deliver(step - 1 - ahead)
        if 0 <= step - 2 - ahead < chunks:
            place(step - 2 - ahead)

    for c in range(chunks):
        for dz in range(1, depth):
            y_copy(c, dz, lax.rem(gz + dz, depth), gz).wait_send()

        @pl.when(middle)
        def _():
            cross_copy(c, inner).wait_send()

        @pl.when(jnp.logical_not(middle))
        def _():
            near_copy(c, inner).wait_send()

        @pl.when(level > 0)
        def _():
            back_copy(c, outer).wait_send()

        for dx in range(1, nx):
            g_copy(c, dx, lax.rem(gx + dx, nx), gx).wait_send()
        out_copy(c).wait()


def count(mask):
    return jnp.sum(mask.astype(jnp.int32), axis=1)


def pick(value, mask, position, wanted):
    hit = mask[None, :] & (position[None, :] == jnp.arange(wanted, dtype=jnp.int32)[:, None])
    return jnp.sum(jnp.where(hit, value[None, :], 0), axis=1)


def shards(embeds, dest_device, shuffle_key, lengths, gain):
    tiles_here, tile_rows, width = embeds.shape
    nx, ny, depth = lax.axis_size("gx"), lax.axis_size("gy"), lax.axis_size("gz")
    devices = nx * ny * depth
    per_peer = (tiles_here + depth - 1) // depth
    slots = depth * per_peer
    half = ny // 2
    cap = 2 * tiles_here
    if ny % 2 or tile_rows % 128 or slots > tiles_here:
        return direct(embeds, dest_device, shuffle_key, lengths, gain)

    most = half * min(tiles_here, nx * half)
    near_most = max([(e + 1) * min(tiles_here, nx * (ny - 1 - e)) for e in range(half - 1)] + [1])
    back_most = max([(ny - e) * min(tiles_here, nx * e) for e in range(1, half)] + [1])
    classes = sorted({max(1, most * part // 16) for part in CLASSES})

    lanes = -(-2 * tiles_here // 128) * 128
    mine = jnp.pad(jnp.concatenate([dest_device, shuffle_key]), (0, lanes - 2 * tiles_here))[None, :]
    vmem = pl.BlockSpec(memory_space=pltpu.VMEM)
    table = pl.pallas_call(
        functools.partial(table_kernel, (nx, ny, depth)),
        out_shape=jax.ShapeDtypeStruct((devices, 1, lanes), jnp.int32),
        in_specs=[vmem],
        out_specs=vmem,
        scratch_shapes=[pltpu.SemaphoreType.DMA((devices - 1,))] * 2,
        compiler_params=pltpu.CompilerParams(collective_id=0, has_side_effects=True),
        name="tables",
    )(mine)

    gx, gy, gz = lax.axis_index("gx"), lax.axis_index("gy"), lax.axis_index("gz")
    group = gx * ny + gy
    me = group * depth + gz
    dest = table[:, 0, :tiles_here].reshape(-1)
    keys = table[:, 0, tiles_here : 2 * tiles_here].reshape(-1)
    order = jnp.arange(devices * tiles_here, dtype=jnp.int32)
    before = order[None, :] < order[:, None]
    source = order // tiles_here
    from_x, from_y = source // (ny * depth), source // depth % ny
    to_x, to_y, to_z = dest // (ny * depth), dest // depth % ny, dest % depth

    bounds = jnp.arange(ny - 1, dtype=jnp.int32)
    lane = from_x * depth + to_z
    hop_up = (from_y[None, :] <= bounds[:, None]) & (to_y[None, :] > bounds[:, None])
    hop_down = (from_y[None, :] > bounds[:, None]) & (to_y[None, :] <= bounds[:, None])
    hops = jnp.concatenate([hop_up, hop_down])
    in_lane = lane[None, :] == jnp.arange(nx * depth, dtype=jnp.int32)[:, None]
    load = jnp.max(jnp.sum((hops[:, None, :] & in_lane[None, :, :]).astype(jnp.int32), axis=2))

    low = gy < half
    level = jnp.where(low, gy, ny - 1 - gy)
    depth_from = jnp.where(low, from_y, ny - 1 - from_y)
    depth_to = jnp.where(low, to_y, ny - 1 - to_y)
    in_my_lane = (from_x == gx) & (to_z == gz)
    inward = in_my_lane & (depth_from <= level) & (depth_to > level)
    near_in = in_my_lane & (depth_from < level) & (depth_to >= level)
    outward = in_my_lane & (depth_from >= level) & (depth_to < level)
    far_in = in_my_lane & (depth_from > level) & (depth_to <= level)
    landing = in_my_lane & (depth_to == level)
    to_me = dest == me

    same_source = source[:, None] == source[None, :]
    spot = count(before & same_source & (to_z[:, None] == to_z[None, :]))
    at_inward = count(before & inward[None, :])
    at_near = count(before & near_in[None, :])
    at_outward = count(before & outward[None, :])
    at_far = count(before & far_in[None, :])
    at_landing = count(before & (landing[None, :] & (to_x[:, None] == to_x[None, :])))
    at_me = count(before & (to_me[None, :] & (from_x[:, None] == from_x[None, :])))
    rank = count((keys[None, :] < keys[:, None]) & to_me[None, :])
    own_slot = source % depth * per_peer + spot

    def plan_for(far):
        near, back = min(far, near_most), min(far, back_most)
        code = jnp.where(
            depth_from == level,
            own_slot,
            jnp.where(depth_from < level, slots + at_near, slots + near + at_far),
        )
        tile = me * tiles_here + jnp.arange(tiles_here, dtype=jnp.int32)
        length = lengths[tile // TILES_SEQ]
        limit = jnp.maximum(length - tile % TILES_SEQ * tile_rows, 0)
        here = dest_device % depth
        early = jnp.arange(tiles_here)[None, :] < jnp.arange(tiles_here)[:, None]
        my_slot = here * per_peer + count(early & (here[:, None] == here[None, :]))
        always = jnp.ones((tiles_here,), jnp.bool_)
        parts = {
            "tile": pick(jnp.arange(tiles_here, dtype=jnp.int32), always, my_slot, slots),
            "limit": pick(limit, always, my_slot, slots),
            "inward": pick(code, inward, at_inward, far),
            "outward": pick(code, outward, at_outward, back),
            "deliver": pick(code, landing, to_x * ny + at_landing, nx * ny),
            "place": pick(from_x * ny + at_me + 1, to_me, rank, cap) - 1,
        }
        at, total = {}, 0
        for name, part in parts.items():
            at[name] = total
            total += part.shape[0]
        joined = jnp.concatenate(list(parts.values()))
        return jnp.pad(joined, (0, -total % 128))[None, :], at, near, back

    chunk_rows = tuple(part * tile_rows // 16 for part in CHUNKS)
    chunks = len(chunk_rows)
    hbm = pl.BlockSpec(memory_space=pl.ANY)

    def branch(index, far):
        def run(embeds, gain):
            plan, at, near, back = plan_for(far)
            counts = (
                (tiles_here,),
                (depth - 1, per_peer),
                (slots + near,),
                (far,),
                (far,),
                (back,),
                (nx - 1, ny),
                (nx * ny,),
                (cap,),
            )
            return pl.pallas_call(
                functools.partial(
                    line_kernel, (nx, ny, depth, per_peer, chunk_rows, near, far, back, at)
                ),
                out_shape=jax.ShapeDtypeStruct((cap, tile_rows, width), jnp.bfloat16),
                in_specs=[hbm] * 3,
                out_specs=hbm,
                scratch_shapes=[
                    pltpu.SMEM(plan.shape, jnp.int32),
                    pltpu.VMEM((1, width), jnp.float32),
                    pltpu.SemaphoreType.DMA,
                    pltpu.SemaphoreType.DMA,
                    pltpu.SemaphoreType.DMA((chunks,)),
                    pltpu.SemaphoreType.DMA((chunks, depth - 1)),
                    pltpu.SemaphoreType.DMA((chunks, depth - 1)),
                    pltpu.SemaphoreType.DMA((chunks,)),
                    pltpu.SemaphoreType.DMA((chunks,)),
                    pltpu.SemaphoreType.DMA((chunks,)),
                    pltpu.SemaphoreType.DMA((chunks,)),
                    pltpu.SemaphoreType.DMA((chunks, nx - 1)),
                    pltpu.SemaphoreType.DMA((chunks, nx - 1)),
                    pltpu.SemaphoreType.DMA((chunks,)),
                ]
                + [pltpu.VMEM((*lead, rows, width), jnp.bfloat16) for lead in counts for rows in chunk_rows],
                compiler_params=pltpu.CompilerParams(
                    collective_id=1 + index, has_side_effects=True, vmem_limit_bytes=60 * 1024 * 1024
                ),
                name=f"line{far}",
            )(plan, embeds, gain)

        return run

    chosen = jnp.int32(0)
    for bound in classes[:-1]:
        chosen = chosen + (load > bound).astype(jnp.int32)
    return lax.switch(
        chosen, [branch(i, far) for i, far in enumerate(classes)], embeds, gain.reshape(1, width)
    )


def solution(mesh):
    return jax.shard_map(
        shards,
        mesh=mesh,
        in_specs=(
            P(("gx", "gy", "gz"), None, None),
            P(("gx", "gy", "gz")),
            P(("gx", "gy", "gz")),
            P(),
            P(),
        ),
        out_specs=P(("gx", "gy", "gz"), None, None),
        check_vma=False,
    )
```

```python
import functools

import jax
import jax.numpy as jnp
from jax import lax
from jax.experimental import pallas as pl
from jax.experimental.pallas import tpu as pltpu
from jax.sharding import PartitionSpec as P

TILES_SEQ = 32
CLASSES = (9, 10, 11, 12, 13, 16)
CHUNKS = (1, 1, 2, 2, 2, 2, 2, 2, 1, 1)
OUTER_AHEAD = 4
MIDDLE_AHEAD = 1
MESH = pl.DeviceIdType.MESH


def exchange_kernel(
    sizes, small_in, x_ref, gain_ref, recv_ref, keys_ref,
    small_ref, gain, small_sem, first_table, limit_table, note_out, notes, note_table, second, keys_out,
    x_sem, gain_sem, y_send, y_recv, g_send, g_recv, own_sem,
    note_send, note_recv, note_sem, key_send, key_recv, *buffers,
):
    nx, ny, depth, per_peer, chunk_rows = sizes
    chunks = len(chunk_rows)
    starts = [sum(chunk_rows[:c]) for c in range(chunks)]
    groups = nx * ny
    tiles_here, tile_rows, _ = x_ref.shape
    raw, first, arrived, outgoing = (buffers[i * chunks : (i + 1) * chunks] for i in range(4))
    gx, gy, gz = lax.axis_index("gx"), lax.axis_index("gy"), lax.axis_index("gz")
    group = gx * ny + gy
    me = group * depth + gz
    offsets = [(dx, dy) for dy in sorted(range(ny), key=lambda d: abs(d - ny // 2)) for dx in range(nx)]
    offsets.remove((0, 0))

    def load(c):
        return pltpu.make_async_copy(
            x_ref.at[:, pl.ds(starts[c], chunk_rows[c])], raw[c], x_sem.at[c]
        )

    def fill_tables():
        depths = [lax.rem(small_ref[0, i], depth) for i in range(tiles_here)]
        dest_groups = [lax.div(small_ref[0, i], depth) for i in range(tiles_here)]
        places, limits = [], []
        for i in range(tiles_here):
            spot = jnp.int32(0)
            for j in range(i):
                spot = spot + jnp.where(depths[j] == depths[i], 1, 0)
            places.append(depths[i] * per_peer + spot)
            tile = me * tiles_here + i
            length = small_ref[0, 2 * tiles_here + tile // TILES_SEQ]
            limits.append(jnp.maximum(length - tile % TILES_SEQ * tile_rows, 0))
        lane = lax.broadcasted_iota(jnp.int32, note_out.shape[1:], 1)
        for z in range(depth):
            row = jnp.zeros(note_out.shape[1:], jnp.int32)
            for p in range(per_peer):
                slot = z * per_peer + p
                tile, limit, dest_group, key = (jnp.int32(v) for v in (0, 0, -1, 0))
                for i in range(tiles_here):
                    hit = places[i] == slot
                    tile = jnp.where(hit, i, tile)
                    limit = jnp.where(hit, limits[i], limit)
                    dest_group = jnp.where(hit, dest_groups[i], dest_group)
                    key = jnp.where(hit, small_ref[0, tiles_here + i] + 1, key)
                first_table[slot] = tile
                limit_table[slot] = limit
                row = jnp.where(lane == p, dest_group, row)
                row = jnp.where(lane == per_peer + p, key, row)
            note_out[z] = row

    def normed(c, slot):
        rows = chunk_rows[c]
        values = raw[c][first_table[slot]].astype(jnp.float32)
        meansq = jnp.mean(values * values, axis=-1, keepdims=True)
        scaled = values * lax.rsqrt(jnp.maximum(meansq, 0.25)) * gain[...]
        row = starts[c] + lax.broadcasted_iota(jnp.int32, (rows, 1), 0)
        return jnp.where(row < limit_table[slot], scaled, 0.0).astype(jnp.bfloat16)

    def y_copy(c, dz, peer, origin):
        return pltpu.make_async_remote_copy(
            src_ref=first[c].at[dz - 1],
            dst_ref=arrived[c].at[pl.ds(origin * per_peer, per_peer)],
            send_sem=y_send.at[c, dz - 1],
            recv_sem=y_recv.at[c, dz - 1],
            device_id=(gx, gy, peer),
            device_id_type=MESH,
        )

    def peer_of(k):
        dx, dy = offsets[k]
        return lax.rem(gx + dx, nx), lax.rem(gy + dy, ny)

    def g_copy(c, k, px, py, origin):
        return pltpu.make_async_remote_copy(
            src_ref=outgoing[c].at[k],
            dst_ref=recv_ref.at[origin, pl.ds(starts[c], chunk_rows[c])],
            send_sem=g_send.at[c, k],
            recv_sem=g_recv.at[c, k],
            device_id=(px, py, gz),
            device_id_type=MESH,
        )

    def own_copy(c):
        return pltpu.make_async_copy(
            outgoing[c].at[groups - 1],
            recv_ref.at[group, pl.ds(starts[c], chunk_rows[c])],
            own_sem.at[c],
        )

    def note_copy(dz, peer, place):
        return pltpu.make_async_remote_copy(
            src_ref=note_out.at[peer],
            dst_ref=notes.at[place],
            send_sem=note_send.at[dz - 1],
            recv_sem=note_recv.at[dz - 1],
            device_id=(gx, gy, peer),
            device_id_type=MESH,
        )

    def key_copy(k, px, py, place):
        return pltpu.make_async_remote_copy(
            src_ref=keys_out.at[k],
            dst_ref=keys_ref.at[place],
            send_sem=key_send.at[k],
            recv_sem=key_recv.at[k],
            device_id=(px, py, gz),
            device_id_type=MESH,
        )

    def prepare(c):
        load(c).wait()
        for dz in range(1, depth):
            peer = lax.rem(gz + dz, depth)
            for p in range(per_peer):
                first[c][dz - 1, p] = normed(c, peer * per_peer + p)
        for p in range(per_peer):
            arrived[c][gz * per_peer + p] = normed(c, gz * per_peer + p)

    def send_first(c):
        for dz in range(1, depth):
            y_copy(c, dz, lax.rem(gz + dz, depth), gz).start()

    def find_slots():
        for dz in range(1, depth):
            origin = lax.rem(gz + depth - dz, depth)
            note_copy(dz, origin, origin).wait()
        tables = [
            pltpu.make_async_copy(
                notes.at[lax.rem(gz + dz, depth)], note_table.at[lax.rem(gz + dz, depth)], note_sem.at[dz]
            )
            for dz in range(1, depth)
        ]
        tables.append(pltpu.make_async_copy(note_out.at[gz], note_table.at[gz], note_sem.at[0]))
        for copy in tables:
            copy.start()
        for copy in tables:
            copy.wait()

        for k in range(groups):
            px, py = peer_of(k) if k < groups - 1 else (gx, gy)
            wanted = px * ny + py
            slot, key = jnp.int32(0), jnp.int32(0)
            for z in range(depth):
                for p in range(per_peer):
                    hit = note_table[z, 0, p] == wanted
                    slot = jnp.where(hit, z * per_peer + p, slot)
                    key = jnp.where(hit, note_table[z, 0, per_peer + p], key)
            second[k] = slot
            row = jnp.full(keys_out.shape[1:], key, jnp.int32)
            if k < groups - 1:
                keys_out[k] = row
            else:
                keys_ref[group] = row

    def forward(c):
        for dz in range(1, depth):
            origin = lax.rem(gz + depth - dz, depth)
            y_copy(c, dz, origin, origin).wait_recv()
        for k in range(groups):
            outgoing[c][k] = arrived[c][second[k]]
        for k in range(groups - 1):
            px, py = peer_of(k)
            g_copy(c, k, px, py, group).start()
        own_copy(c).start()

    small = [
        pltpu.make_async_copy(small_in, small_ref, small_sem),
        pltpu.make_async_copy(gain_ref, gain, gain_sem),
    ]
    for copy in small:
        copy.start()
    for c in range(chunks):
        load(c).start()
    barrier = pltpu.get_barrier_semaphore()
    for dz in range(1, depth):
        pl.semaphore_signal(
            barrier, inc=1, device_id=(gx, gy, lax.rem(gz + dz, depth)), device_id_type=MESH
        )
    for k in range(groups - 1):
        px, py = peer_of(k)
        pl.semaphore_signal(barrier, inc=1, device_id=(px, py, gz), device_id_type=MESH)
    for copy in small:
        copy.wait()
    fill_tables()
    prepare(0)
    pl.semaphore_wait(barrier, depth - 1 + groups - 1)
    for dz in range(1, depth):
        note_copy(dz, lax.rem(gz + dz, depth), gz).start()
    send_first(0)
    if chunks > 1:
        prepare(1)
        send_first(1)
    find_slots()
    forward(0)
    for k in range(groups - 1):
        px, py = peer_of(k)
        key_copy(k, px, py, group).start()
    for c in range(2, chunks):
        prepare(c)
        send_first(c)
        forward(c - 1)
    if chunks > 1:
        forward(chunks - 1)

    for c in range(chunks):
        for dz in range(1, depth):
            y_copy(c, dz, lax.rem(gz + dz, depth), gz).wait_send()
    sources = []
    for dx, dy in offsets:
        sources.append((lax.rem(gx + nx - dx, nx), lax.rem(gy + ny - dy, ny)))
    for k, (sx, sy) in enumerate(sources):
        key_copy(k, sx, sy, sx * ny + sy).wait()
    for c in range(chunks):
        for k, (sx, sy) in enumerate(sources):
            g_copy(c, k, sx, sy, sx * ny + sy).wait()
        own_copy(c).wait()


def place_kernel(source_ref, filled_ref, blocks_ref, out_ref, zeros, out_sem):
    cap = out_ref.shape[0]

    def store(slot):
        return pltpu.make_async_copy(blocks_ref.at[source_ref[slot]], out_ref.at[slot], out_sem.at[slot])

    for slot in range(cap):
        pl.when(filled_ref[slot] == 1)(lambda slot=slot: store(slot).start())
    zeros[...] = jnp.zeros_like(zeros)
    for slot in range(cap):

        @pl.when(filled_ref[slot] == 0)
        def _():
            pltpu.make_async_copy(zeros, out_ref.at[slot], out_sem.at[slot]).start()

    for slot in range(cap):
        store(slot).wait()


def direct(embeds, dest_device, shuffle_key, lengths, gain):
    tiles_here, tile_rows, width = embeds.shape
    nx, ny, depth = lax.axis_size("gx"), lax.axis_size("gy"), lax.axis_size("gz")
    groups = nx * ny
    per_peer = (tiles_here + depth - 1) // depth
    slots = depth * per_peer
    chunk_rows = (tile_rows,)
    if tile_rows % 128 == 0:
        chunk_rows = tuple(part * tile_rows // 16 for part in (1, 1, 2, 2, 4, 4, 2))
    chunks = len(chunk_rows)

    smem = pl.BlockSpec(memory_space=pltpu.SMEM)
    vmem = pl.BlockSpec(memory_space=pltpu.VMEM)
    hbm = pl.BlockSpec(memory_space=pl.ANY)
    lanes = -(-2 * per_peer // 128) * 128
    small = jnp.concatenate([dest_device, shuffle_key, lengths])
    small = jnp.pad(small, (0, -small.shape[0] % 128))[None, :]
    received, key_rows = pl.pallas_call(
        functools.partial(exchange_kernel, (nx, ny, depth, per_peer, chunk_rows)),
        out_shape=(
            jax.ShapeDtypeStruct((groups, tile_rows, width), jnp.bfloat16),
            jax.ShapeDtypeStruct((groups, 1, 128), jnp.int32),
        ),
        in_specs=[hbm] * 3,
        out_specs=(hbm, vmem),
        scratch_shapes=[
            pltpu.SMEM(small.shape, jnp.int32),
            pltpu.VMEM((1, width), jnp.float32),
            pltpu.SemaphoreType.DMA,
            pltpu.SMEM((slots,), jnp.int32),
            pltpu.SMEM((slots,), jnp.int32),
            pltpu.VMEM((depth, 1, lanes), jnp.int32),
            pltpu.VMEM((depth, 1, lanes), jnp.int32),
            pltpu.SMEM((depth, 1, lanes), jnp.int32),
            pltpu.SMEM((groups,), jnp.int32),
            pltpu.VMEM((groups, 1, 128), jnp.int32),
            pltpu.SemaphoreType.DMA((chunks,)),
            pltpu.SemaphoreType.DMA,
            pltpu.SemaphoreType.DMA((chunks, depth - 1)),
            pltpu.SemaphoreType.DMA((chunks, depth - 1)),
            pltpu.SemaphoreType.DMA((chunks, groups)),
            pltpu.SemaphoreType.DMA((chunks, groups)),
            pltpu.SemaphoreType.DMA((chunks,)),
            pltpu.SemaphoreType.DMA((depth,)),
            pltpu.SemaphoreType.DMA((depth,)),
            pltpu.SemaphoreType.DMA((depth,)),
            pltpu.SemaphoreType.DMA((groups,)),
            pltpu.SemaphoreType.DMA((groups,)),
        ]
        + [pltpu.VMEM((tiles_here, rows, width), jnp.bfloat16) for rows in chunk_rows]
        + [pltpu.VMEM((depth - 1, per_peer, rows, width), jnp.bfloat16) for rows in chunk_rows]
        + [pltpu.VMEM((slots, rows, width), jnp.bfloat16) for rows in chunk_rows]
        + [pltpu.VMEM((groups, rows, width), jnp.bfloat16) for rows in chunk_rows],
        compiler_params=pltpu.CompilerParams(
            collective_id=0, has_side_effects=True, vmem_limit_bytes=36 * 1024 * 1024
        ),
        name="exchange",
    )(small, embeds, gain.reshape(1, width))

    key_of = key_rows[:, 0, 0]
    valid = key_of > 0
    rank = jnp.sum((valid[None, :] & (key_of[None, :] < key_of[:, None])).astype(jnp.int32), axis=1)
    cap = 2 * tiles_here
    at = valid[None, :] & (rank[None, :] == jnp.arange(cap, dtype=jnp.int32)[:, None])
    source = jnp.sum(jnp.where(at, jnp.arange(groups, dtype=jnp.int32)[None, :], 0), axis=1).astype(jnp.int32)
    filled = jnp.sum(at.astype(jnp.int32), axis=1).astype(jnp.int32)

    return pl.pallas_call(
        place_kernel,
        out_shape=jax.ShapeDtypeStruct((cap, tile_rows, width), jnp.bfloat16),
        in_specs=[smem, smem, vmem],
        out_specs=hbm,
        scratch_shapes=[
            pltpu.VMEM((tile_rows, width), jnp.bfloat16),
            pltpu.SemaphoreType.DMA((cap,)),
        ],
        compiler_params=pltpu.CompilerParams(vmem_limit_bytes=24 * 1024 * 1024),
        name="place",
    )(source, filled, received)


def table_kernel(
    sizes, dest_hbm, key_hbm, lengths_hbm, x_ref, gain_hbm, table_ref, normed_ref,
    dest_ref, lengths_ref, dest_row, key_row, gain_ref, small_sem, mine, first_table, limit_table, raw, done, send, recv, x_sem, out_sem,
):
    nx, ny, depth, per_peer = sizes
    devices = nx * ny * depth
    tiles_here, tile_rows, width = x_ref.shape
    slots = depth * per_peer
    block = 16
    me = (lax.axis_index("gx") * ny + lax.axis_index("gy")) * depth + lax.axis_index("gz")

    def place_of(device):
        return lax.div(device, ny * depth), lax.rem(lax.div(device, depth), ny), lax.rem(device, depth)

    def row_copy(step, target, row):
        return pltpu.make_async_remote_copy(
            src_ref=mine,
            dst_ref=table_ref.at[row],
            send_sem=send.at[step - 1],
            recv_sem=recv.at[step - 1],
            device_id=place_of(target),
            device_id_type=MESH,
        )

    def normalize(slot):
        @pl.loop(0, tile_rows // block)
        def _(part):
            start = part * block
            values = raw[first_table[slot], pl.ds(start, block)].astype(jnp.float32)
            meansq = jnp.mean(values * values, axis=-1, keepdims=True)
            scaled = values * lax.rsqrt(jnp.maximum(meansq, 0.25)) * gain_ref[...]
            row = start + lax.broadcasted_iota(jnp.int32, (block, 1), 0)
            done[slot, pl.ds(start, block)] = jnp.where(row < limit_table[slot], scaled, 0.0).astype(jnp.bfloat16)

        pltpu.make_async_copy(done.at[slot], normed_ref.at[slot], out_sem.at[slot]).start()

    small = [
        pltpu.make_async_copy(dest_hbm, dest_row, small_sem.at[0]),
        pltpu.make_async_copy(key_hbm, key_row, small_sem.at[1]),
        pltpu.make_async_copy(dest_hbm, dest_ref, small_sem.at[2]),
        pltpu.make_async_copy(lengths_hbm, lengths_ref, small_sem.at[3]),
        pltpu.make_async_copy(gain_hbm, gain_ref, small_sem.at[4]),
    ]
    load = pltpu.make_async_copy(x_ref, raw, x_sem)
    for copy in small:
        copy.start()
    load.start()
    barrier = pltpu.get_barrier_semaphore()
    for step in range(1, devices):
        pl.semaphore_signal(
            barrier, inc=1, device_id=place_of(lax.rem(me + step, devices)), device_id_type=MESH
        )
    for copy in small:
        copy.wait()
    mine[...] = jnp.zeros_like(mine)
    mine[0:1, 0:tiles_here] = dest_row[...]
    mine[1:2, 0:tiles_here] = key_row[...]
    table_ref[me] = mine[...]

    depths = [lax.rem(dest_ref[0, i], depth) for i in range(tiles_here)]
    places, limits = [], []
    for i in range(tiles_here):
        spot = jnp.int32(0)
        for j in range(i):
            spot = spot + jnp.where(depths[j] == depths[i], 1, 0)
        places.append(depths[i] * per_peer + spot)
        tile = me * tiles_here + i
        limits.append(jnp.maximum(lengths_ref[0, tile // TILES_SEQ] - tile % TILES_SEQ * tile_rows, 0))
    for slot in range(slots):
        tile, limit = jnp.int32(0), jnp.int32(0)
        for i in range(tiles_here):
            tile = jnp.where(places[i] == slot, i, tile)
            limit = jnp.where(places[i] == slot, limits[i], limit)
        first_table[slot] = tile
        limit_table[slot] = limit

    load.wait()
    early = slots // 2
    for slot in range(early):
        normalize(slot)
    pl.semaphore_wait(barrier, devices - 1)
    for step in range(1, devices):
        row_copy(step, lax.rem(me + step, devices), me).start()
    for slot in range(early, slots):
        normalize(slot)
    for step in range(1, devices):
        source = lax.rem(me + devices - step, devices)
        row_copy(step, source, source).wait()
    for slot in range(slots):
        pltpu.make_async_copy(done.at[slot], normed_ref.at[slot], out_sem.at[slot]).wait()


def line_kernel(
    sizes, plan_ref, x_ref, received,
    plan, plan_sem, x_sem, y_send, y_recv, a_send, a_recv, b_send, b_recv,
    g_send, g_recv, *buffers,
):
    nx, ny, depth, per_peer, chunk_rows, near, far, back, at = sizes
    chunks = len(chunk_rows)
    starts = [sum(chunk_rows[:c]) for c in range(chunks)]
    half = ny // 2
    slots = depth * per_peer
    pool, inflow, inward, outward, outgoing = (
        buffers[i * chunks : (i + 1) * chunks] for i in range(5)
    )
    gx, gy, gz = lax.axis_index("gx"), lax.axis_index("gy"), lax.axis_index("gz")
    low = gy < half
    level = jnp.where(low, gy, ny - 1 - gy)
    inner = jnp.where(low, gy + 1, gy - 1)
    outer = jnp.clip(jnp.where(low, gy - 1, gy + 1), 0, ny - 1)
    middle = level == half - 1

    def rows(c):
        return pl.ds(starts[c], chunk_rows[c])

    def load(c):
        return pltpu.make_async_copy(
            x_ref.at[pl.ds(gz * per_peer, per_peer), rows(c)],
            pool[c].at[pl.ds(gz * per_peer, per_peer)],
            x_sem.at[c],
        )

    def y_copy(c, dz, peer, origin):
        return pltpu.make_async_remote_copy(
            src_ref=x_ref.at[pl.ds(peer * per_peer, per_peer), rows(c)],
            dst_ref=pool[c].at[pl.ds(origin * per_peer, per_peer)],
            send_sem=y_send.at[c, dz - 1],
            recv_sem=y_recv.at[c, dz - 1],
            device_id=(gx, gy, peer),
            device_id_type=MESH,
        )

    def near_copy(c, peer):
        return pltpu.make_async_remote_copy(
            src_ref=inward[c].at[pl.ds(0, near)],
            dst_ref=pool[c].at[pl.ds(slots, near)],
            send_sem=a_send.at[c],
            recv_sem=a_recv.at[c],
            device_id=(gx, peer, gz),
            device_id_type=MESH,
        )

    def cross_copy(c, peer):
        return pltpu.make_async_remote_copy(
            src_ref=inward[c],
            dst_ref=inflow[c],
            send_sem=a_send.at[c],
            recv_sem=b_recv.at[c],
            device_id=(gx, peer, gz),
            device_id_type=MESH,
        )

    def back_copy(c, peer):
        return pltpu.make_async_remote_copy(
            src_ref=outward[c],
            dst_ref=inflow[c].at[pl.ds(0, back)],
            send_sem=b_send.at[c],
            recv_sem=b_recv.at[c],
            device_id=(gx, peer, gz),
            device_id_type=MESH,
        )

    def g_copy(c, dx, peer, origin):
        return pltpu.make_async_remote_copy(
            src_ref=outgoing[c].at[dx - 1],
            dst_ref=received.at[pl.ds(origin * ny, ny), rows(c)],
            send_sem=g_send.at[c, dx - 1],
            recv_sem=g_recv.at[c, dx - 1],
            device_id=(peer, gy, gz),
            device_id_type=MESH,
        )

    def either(c, code):
        held = pool[c][jnp.clip(code, 0, slots + near - 1)]
        came = inflow[c][jnp.clip(code - slots - near, 0, far - 1)]
        return jnp.where(code < slots + near, held, came)

    def send_inward(c, crosses, relays):
        load(c).wait()
        for dz in range(1, depth):
            origin = lax.rem(gz + depth - dz, depth)
            y_copy(c, dz, origin, origin).wait_recv()
        if relays:
            near_copy(c, outer).wait_recv()

        @pl.loop(0, far if crosses else near)
        def _(p):
            inward[c][p] = pool[c][plan[0, at["inward"] + p]]

        if crosses:
            cross_copy(c, inner).start()
        else:
            near_copy(c, inner).start()

    def deliver(c, crosses, relays):
        if crosses:
            cross_copy(c, inner).wait_recv()
        else:
            back_copy(c, inner).wait_recv()
        if relays:

            @pl.loop(0, back)
            def _(p):
                outward[c][p] = either(c, plan[0, at["outward"] + p])

            back_copy(c, outer).start()
        for dx in range(1, nx):
            peer = lax.rem(gx + dx, nx)

            @pl.loop(0, ny)
            def _(k):
                outgoing[c][dx - 1, k] = either(c, plan[0, at["deliver"] + peer * ny + k])

            g_copy(c, dx, peer, gx).start()

        @pl.loop(0, ny)
        def _(k):
            received[gx * ny + k, rows(c)] = either(c, plan[0, at["deliver"] + gx * ny + k])

    def stream(ahead, crosses, relays):
        for step in range(chunks + ahead):
            if step < chunks:
                send_inward(step, crosses, relays)
            if step >= ahead:
                deliver(step - ahead, crosses, relays)
        for c in range(chunks):
            if crosses:
                cross_copy(c, inner).wait_send()
            else:
                near_copy(c, inner).wait_send()
            if relays:
                back_copy(c, outer).wait_send()

    fetch = pltpu.make_async_copy(plan_ref, plan, plan_sem)
    fetch.start()
    for c in range(chunks):
        load(c).start()
    barrier = pltpu.get_barrier_semaphore()
    for dz in range(1, depth):
        pl.semaphore_signal(
            barrier, inc=1, device_id=(gx, gy, lax.rem(gz + dz, depth)), device_id_type=MESH
        )
    for dx in range(1, nx):
        pl.semaphore_signal(
            barrier, inc=1, device_id=(lax.rem(gx + dx, nx), gy, gz), device_id_type=MESH
        )
    pl.semaphore_signal(barrier, inc=1, device_id=(gx, inner, gz), device_id_type=MESH)

    @pl.when(level > 0)
    def _():
        pl.semaphore_signal(barrier, inc=1, device_id=(gx, outer, gz), device_id_type=MESH)

    pl.semaphore_wait(barrier, depth - 1 + nx - 1 + 1 + jnp.where(level > 0, 1, 0))
    for c in range(chunks):
        for dz in range(1, depth):
            y_copy(c, dz, lax.rem(gz + dz, depth), gz).start()
    fetch.wait()

    if half == 1:
        stream(1, True, False)
    else:
        pl.when(level == 0)(lambda: stream(OUTER_AHEAD, False, False))
        pl.when(middle)(lambda: stream(MIDDLE_AHEAD, True, True))
        if half > 2:
            pl.when((level > 0) & jnp.logical_not(middle))(lambda: stream(MIDDLE_AHEAD, False, True))

    for c in range(chunks):
        for dz in range(1, depth):
            y_copy(c, dz, lax.rem(gz + dz, depth), gz).wait_send()
        for dx in range(1, nx):
            origin = lax.rem(gx + nx - dx, nx)
            g_copy(c, dx, origin, origin).wait()


def count(mask):
    return jnp.sum(mask.astype(jnp.int32), axis=1)


def pick(value, mask, position, wanted):
    hit = mask[None, :] & (position[None, :] == jnp.arange(wanted, dtype=jnp.int32)[:, None])
    return jnp.sum(jnp.where(hit, value[None, :], 0), axis=1)


def shards(embeds, dest_device, shuffle_key, lengths, gain):
    tiles_here, tile_rows, width = embeds.shape
    nx, ny, depth = lax.axis_size("gx"), lax.axis_size("gy"), lax.axis_size("gz")
    devices = nx * ny * depth
    per_peer = (tiles_here + depth - 1) // depth
    slots = depth * per_peer
    half = ny // 2
    cap = 2 * tiles_here
    if ny % 2 or tile_rows % 128 or slots > tiles_here:
        return direct(embeds, dest_device, shuffle_key, lengths, gain)

    most = half * min(tiles_here, nx * half)
    near_most = max([(e + 1) * min(tiles_here, nx * (ny - 1 - e)) for e in range(half - 1)] + [1])
    back_most = max([(ny - e) * min(tiles_here, nx * e) for e in range(1, half)] + [1])
    classes = sorted({max(1, most * part // 16) for part in CLASSES})

    vmem = pl.BlockSpec(memory_space=pltpu.VMEM)
    smem = pl.BlockSpec(memory_space=pltpu.SMEM)
    hbm = pl.BlockSpec(memory_space=pl.ANY)
    lanes = -(-tiles_here // 128) * 128
    table, normed = pl.pallas_call(
        functools.partial(table_kernel, (nx, ny, depth, per_peer)),
        out_shape=(
            jax.ShapeDtypeStruct((devices, 2, lanes), jnp.int32),
            pltpu.HBM((slots, tile_rows, width), jnp.bfloat16),
        ),
        in_specs=[pl.BlockSpec(memory_space=pltpu.HBM)] * 5,
        out_specs=(vmem, pl.BlockSpec(memory_space=pltpu.HBM)),
        scratch_shapes=[
            pltpu.SMEM((1, tiles_here), jnp.int32),
            pltpu.SMEM((1, lengths.shape[0]), jnp.int32),
            pltpu.VMEM((1, tiles_here), jnp.int32),
            pltpu.VMEM((1, tiles_here), jnp.int32),
            pltpu.VMEM((1, width), jnp.float32),
            pltpu.SemaphoreType.DMA((5,)),
            pltpu.VMEM((2, lanes), jnp.int32),
            pltpu.SMEM((slots,), jnp.int32),
            pltpu.SMEM((slots,), jnp.int32),
            pltpu.VMEM((tiles_here, tile_rows, width), jnp.bfloat16),
            pltpu.VMEM((slots, tile_rows, width), jnp.bfloat16),
            pltpu.SemaphoreType.DMA((devices - 1,)),
            pltpu.SemaphoreType.DMA((devices - 1,)),
            pltpu.SemaphoreType.DMA,
            pltpu.SemaphoreType.DMA((slots,)),
        ],
        compiler_params=pltpu.CompilerParams(
            collective_id=0, has_side_effects=True, vmem_limit_bytes=56 * 1024 * 1024
        ),
        name="tables",
    )(dest_device[None, :], shuffle_key[None, :], lengths[None, :], embeds, gain.reshape(1, width))

    gx, gy, gz = lax.axis_index("gx"), lax.axis_index("gy"), lax.axis_index("gz")
    group = gx * ny + gy
    me = group * depth + gz
    dest = table[:, 0, :tiles_here].reshape(-1)
    keys = table[:, 1, :tiles_here].reshape(-1)
    order = jnp.arange(devices * tiles_here, dtype=jnp.int32)
    before = order[None, :] < order[:, None]
    source = order // tiles_here
    from_x, from_y = source // (ny * depth), source // depth % ny
    to_x, to_y, to_z = dest // (ny * depth), dest // depth % ny, dest % depth

    bounds = jnp.arange(ny - 1, dtype=jnp.int32)
    lane = from_x * depth + to_z
    hop_up = (from_y[None, :] <= bounds[:, None]) & (to_y[None, :] > bounds[:, None])
    hop_down = (from_y[None, :] > bounds[:, None]) & (to_y[None, :] <= bounds[:, None])
    hops = jnp.concatenate([hop_up, hop_down])
    in_lane = lane[None, :] == jnp.arange(nx * depth, dtype=jnp.int32)[:, None]
    load = jnp.max(jnp.sum((hops[:, None, :] & in_lane[None, :, :]).astype(jnp.int32), axis=2))

    low = gy < half
    level = jnp.where(low, gy, ny - 1 - gy)
    depth_from = jnp.where(low, from_y, ny - 1 - from_y)
    depth_to = jnp.where(low, to_y, ny - 1 - to_y)
    in_my_lane = (from_x == gx) & (to_z == gz)
    inward = in_my_lane & (depth_from <= level) & (depth_to > level)
    near_in = in_my_lane & (depth_from < level) & (depth_to >= level)
    outward = in_my_lane & (depth_from >= level) & (depth_to < level)
    far_in = in_my_lane & (depth_from > level) & (depth_to <= level)
    landing = in_my_lane & (depth_to == level)
    to_me = dest == me

    same_source = source[:, None] == source[None, :]
    spot = count(before & same_source & (to_z[:, None] == to_z[None, :]))
    at_inward = count(before & inward[None, :])
    at_near = count(before & near_in[None, :])
    at_outward = count(before & outward[None, :])
    at_far = count(before & far_in[None, :])
    at_landing = count(before & (landing[None, :] & (to_x[:, None] == to_x[None, :])))
    at_me = count(before & (to_me[None, :] & (from_x[:, None] == from_x[None, :])))
    rank = count((keys[None, :] < keys[:, None]) & to_me[None, :])
    own_slot = source % depth * per_peer + spot

    chosen = jnp.int32(0)
    for bound in classes[:-1]:
        chosen = chosen + (load > bound).astype(jnp.int32)
    far = jnp.full((), classes[-1], jnp.int32)
    for index, bound in enumerate(classes[:-1]):
        far = jnp.where(chosen == index, bound, far)
    near = jnp.minimum(far, near_most)
    code = jnp.where(
        depth_from == level,
        own_slot,
        jnp.where(depth_from < level, slots + at_near, slots + near + at_far),
    )
    parts = {
        "inward": pick(code, inward, at_inward, most),
        "outward": pick(code, outward, at_outward, back_most),
        "deliver": pick(code, landing, to_x * ny + at_landing, nx * ny),
    }
    at, total = {}, 0
    for name, part in parts.items():
        at[name] = total
        total += part.shape[0]
    plan = jnp.pad(jnp.concatenate(list(parts.values())), (0, -total % 128))[None, :]
    which = pick(from_x * ny + at_me + 1, to_me, rank, cap)

    chunk_rows = tuple(part * tile_rows // 16 for part in CHUNKS)
    chunks = len(chunk_rows)

    def branch(index, far):
        def run(plan, normed, chosen_rows, filled):
            near, back = min(far, near_most), min(far, back_most)
            counts = ((slots + near,), (far,), (far,), (back,), (nx - 1, ny))
            received = pl.pallas_call(
                functools.partial(
                    line_kernel, (nx, ny, depth, per_peer, chunk_rows, near, far, back, at)
                ),
                out_shape=pltpu.VMEM((nx * ny, tile_rows, width), jnp.bfloat16),
                in_specs=[hbm, pl.BlockSpec(memory_space=pltpu.HBM)],
                out_specs=vmem,
                scratch_shapes=[
                    pltpu.SMEM(plan.shape, jnp.int32),
                    pltpu.SemaphoreType.DMA,
                    pltpu.SemaphoreType.DMA((chunks,)),
                    pltpu.SemaphoreType.DMA((chunks, depth - 1)),
                    pltpu.SemaphoreType.DMA((chunks, depth - 1)),
                    pltpu.SemaphoreType.DMA((chunks,)),
                    pltpu.SemaphoreType.DMA((chunks,)),
                    pltpu.SemaphoreType.DMA((chunks,)),
                    pltpu.SemaphoreType.DMA((chunks,)),
                    pltpu.SemaphoreType.DMA((chunks, nx - 1)),
                    pltpu.SemaphoreType.DMA((chunks, nx - 1)),
                ]
                + [pltpu.VMEM((*lead, rows, width), jnp.bfloat16) for lead in counts for rows in chunk_rows],
                compiler_params=pltpu.CompilerParams(
                    collective_id=1 + index, has_side_effects=True, vmem_limit_bytes=44 * 1024 * 1024
                ),
                name=f"line{far}",
            )(plan, normed)
            return pl.pallas_call(
                place_kernel,
                out_shape=pltpu.HBM((cap, tile_rows, width), jnp.bfloat16),
                in_specs=[smem, smem, vmem],
                out_specs=pl.BlockSpec(memory_space=pltpu.HBM),
                scratch_shapes=[
                    pltpu.VMEM((tile_rows, width), jnp.bfloat16),
                    pltpu.SemaphoreType.DMA((cap,)),
                ],
                compiler_params=pltpu.CompilerParams(vmem_limit_bytes=24 * 1024 * 1024),
                name="place",
            )(chosen_rows, filled, received)

        return run

    return lax.switch(
        chosen,
        [branch(i, far) for i, far in enumerate(classes)],
        plan,
        normed,
        jnp.maximum(which - 1, 0),
        (which > 0).astype(jnp.int32),
    )


def solution(mesh):
    return jax.shard_map(
        shards,
        mesh=mesh,
        in_specs=(
            P(("gx", "gy", "gz"), None, None),
            P(("gx", "gy", "gz")),
            P(("gx", "gy", "gz")),
            P(),
            P(),
        ),
        out_specs=P(("gx", "gy", "gz"), None, None),
        check_vma=False,
    )
```

```python
import functools

import jax
import jax.numpy as jnp
from jax import lax
from jax.experimental import pallas as pl
from jax.experimental.pallas import tpu as pltpu
from jax.sharding import PartitionSpec as P

TILES_SEQ = 32
CLASSES = (9, 10, 11, 12, 13, 16)
CHUNKS = (2,) * 32
LATENCY = 11
AHEAD = 1
MESH = pl.DeviceIdType.MESH


def exchange_kernel(
    sizes, small_in, x_ref, gain_ref, recv_ref, keys_ref,
    small_ref, gain, small_sem, first_table, limit_table, note_out, notes, note_table, second, keys_out,
    x_sem, gain_sem, y_send, y_recv, g_send, g_recv, own_sem,
    note_send, note_recv, note_sem, key_send, key_recv, *buffers,
):
    nx, ny, depth, per_peer, chunk_rows = sizes
    chunks = len(chunk_rows)
    starts = [sum(chunk_rows[:c]) for c in range(chunks)]
    groups = nx * ny
    tiles_here, tile_rows, _ = x_ref.shape
    raw, first, arrived, outgoing = (buffers[i * chunks : (i + 1) * chunks] for i in range(4))
    gx, gy, gz = lax.axis_index("gx"), lax.axis_index("gy"), lax.axis_index("gz")
    group = gx * ny + gy
    me = group * depth + gz
    offsets = [(dx, dy) for dy in sorted(range(ny), key=lambda d: abs(d - ny // 2)) for dx in range(nx)]
    offsets.remove((0, 0))

    def load(c):
        return pltpu.make_async_copy(
            x_ref.at[:, pl.ds(starts[c], chunk_rows[c])], raw[c], x_sem.at[c]
        )

    def fill_tables():
        depths = [lax.rem(small_ref[0, i], depth) for i in range(tiles_here)]
        dest_groups = [lax.div(small_ref[0, i], depth) for i in range(tiles_here)]
        places, limits = [], []
        for i in range(tiles_here):
            spot = jnp.int32(0)
            for j in range(i):
                spot = spot + jnp.where(depths[j] == depths[i], 1, 0)
            places.append(depths[i] * per_peer + spot)
            tile = me * tiles_here + i
            length = small_ref[0, 2 * tiles_here + tile // TILES_SEQ]
            limits.append(jnp.maximum(length - tile % TILES_SEQ * tile_rows, 0))
        lane = lax.broadcasted_iota(jnp.int32, note_out.shape[1:], 1)
        for z in range(depth):
            row = jnp.zeros(note_out.shape[1:], jnp.int32)
            for p in range(per_peer):
                slot = z * per_peer + p
                tile, limit, dest_group, key = (jnp.int32(v) for v in (0, 0, -1, 0))
                for i in range(tiles_here):
                    hit = places[i] == slot
                    tile = jnp.where(hit, i, tile)
                    limit = jnp.where(hit, limits[i], limit)
                    dest_group = jnp.where(hit, dest_groups[i], dest_group)
                    key = jnp.where(hit, small_ref[0, tiles_here + i] + 1, key)
                first_table[slot] = tile
                limit_table[slot] = limit
                row = jnp.where(lane == p, dest_group, row)
                row = jnp.where(lane == per_peer + p, key, row)
            note_out[z] = row

    def normed(c, slot):
        rows = chunk_rows[c]
        values = raw[c][first_table[slot]].astype(jnp.float32)
        meansq = jnp.mean(values * values, axis=-1, keepdims=True)
        scaled = values * lax.rsqrt(jnp.maximum(meansq, 0.25)) * gain[...]
        row = starts[c] + lax.broadcasted_iota(jnp.int32, (rows, 1), 0)
        return jnp.where(row < limit_table[slot], scaled, 0.0).astype(jnp.bfloat16)

    def y_copy(c, dz, peer, origin):
        return pltpu.make_async_remote_copy(
            src_ref=first[c].at[dz - 1],
            dst_ref=arrived[c].at[pl.ds(origin * per_peer, per_peer)],
            send_sem=y_send.at[c, dz - 1],
            recv_sem=y_recv.at[c, dz - 1],
            device_id=(gx, gy, peer),
            device_id_type=MESH,
        )

    def peer_of(k):
        dx, dy = offsets[k]
        return lax.rem(gx + dx, nx), lax.rem(gy + dy, ny)

    def g_copy(c, k, px, py, origin):
        return pltpu.make_async_remote_copy(
            src_ref=outgoing[c].at[k],
            dst_ref=recv_ref.at[origin, pl.ds(starts[c], chunk_rows[c])],
            send_sem=g_send.at[c, k],
            recv_sem=g_recv.at[c, k],
            device_id=(px, py, gz),
            device_id_type=MESH,
        )

    def own_copy(c):
        return pltpu.make_async_copy(
            outgoing[c].at[groups - 1],
            recv_ref.at[group, pl.ds(starts[c], chunk_rows[c])],
            own_sem.at[c],
        )

    def note_copy(dz, peer, place):
        return pltpu.make_async_remote_copy(
            src_ref=note_out.at[peer],
            dst_ref=notes.at[place],
            send_sem=note_send.at[dz - 1],
            recv_sem=note_recv.at[dz - 1],
            device_id=(gx, gy, peer),
            device_id_type=MESH,
        )

    def key_copy(k, px, py, place):
        return pltpu.make_async_remote_copy(
            src_ref=keys_out.at[k],
            dst_ref=keys_ref.at[place],
            send_sem=key_send.at[k],
            recv_sem=key_recv.at[k],
            device_id=(px, py, gz),
            device_id_type=MESH,
        )

    def prepare(c):
        load(c).wait()
        for dz in range(1, depth):
            peer = lax.rem(gz + dz, depth)
            for p in range(per_peer):
                first[c][dz - 1, p] = normed(c, peer * per_peer + p)
        for p in range(per_peer):
            arrived[c][gz * per_peer + p] = normed(c, gz * per_peer + p)

    def send_first(c):
        for dz in range(1, depth):
            y_copy(c, dz, lax.rem(gz + dz, depth), gz).start()

    def find_slots():
        for dz in range(1, depth):
            origin = lax.rem(gz + depth - dz, depth)
            note_copy(dz, origin, origin).wait()
        tables = [
            pltpu.make_async_copy(
                notes.at[lax.rem(gz + dz, depth)], note_table.at[lax.rem(gz + dz, depth)], note_sem.at[dz]
            )
            for dz in range(1, depth)
        ]
        tables.append(pltpu.make_async_copy(note_out.at[gz], note_table.at[gz], note_sem.at[0]))
        for copy in tables:
            copy.start()
        for copy in tables:
            copy.wait()

        for k in range(groups):
            px, py = peer_of(k) if k < groups - 1 else (gx, gy)
            wanted = px * ny + py
            slot, key = jnp.int32(0), jnp.int32(0)
            for z in range(depth):
                for p in range(per_peer):
                    hit = note_table[z, 0, p] == wanted
                    slot = jnp.where(hit, z * per_peer + p, slot)
                    key = jnp.where(hit, note_table[z, 0, per_peer + p], key)
            second[k] = slot
            row = jnp.full(keys_out.shape[1:], key, jnp.int32)
            if k < groups - 1:
                keys_out[k] = row
            else:
                keys_ref[group] = row

    def forward(c):
        for dz in range(1, depth):
            origin = lax.rem(gz + depth - dz, depth)
            y_copy(c, dz, origin, origin).wait_recv()
        for k in range(groups):
            outgoing[c][k] = arrived[c][second[k]]
        for k in range(groups - 1):
            px, py = peer_of(k)
            g_copy(c, k, px, py, group).start()
        own_copy(c).start()

    small = [
        pltpu.make_async_copy(small_in, small_ref, small_sem),
        pltpu.make_async_copy(gain_ref, gain, gain_sem),
    ]
    for copy in small:
        copy.start()
    for c in range(chunks):
        load(c).start()
    barrier = pltpu.get_barrier_semaphore()
    for dz in range(1, depth):
        pl.semaphore_signal(
            barrier, inc=1, device_id=(gx, gy, lax.rem(gz + dz, depth)), device_id_type=MESH
        )
    for k in range(groups - 1):
        px, py = peer_of(k)
        pl.semaphore_signal(barrier, inc=1, device_id=(px, py, gz), device_id_type=MESH)
    for copy in small:
        copy.wait()
    fill_tables()
    prepare(0)
    pl.semaphore_wait(barrier, depth - 1 + groups - 1)
    for dz in range(1, depth):
        note_copy(dz, lax.rem(gz + dz, depth), gz).start()
    send_first(0)
    if chunks > 1:
        prepare(1)
        send_first(1)
    find_slots()
    forward(0)
    for k in range(groups - 1):
        px, py = peer_of(k)
        key_copy(k, px, py, group).start()
    for c in range(2, chunks):
        prepare(c)
        send_first(c)
        forward(c - 1)
    if chunks > 1:
        forward(chunks - 1)

    for c in range(chunks):
        for dz in range(1, depth):
            y_copy(c, dz, lax.rem(gz + dz, depth), gz).wait_send()
    sources = []
    for dx, dy in offsets:
        sources.append((lax.rem(gx + nx - dx, nx), lax.rem(gy + ny - dy, ny)))
    for k, (sx, sy) in enumerate(sources):
        key_copy(k, sx, sy, sx * ny + sy).wait()
    for c in range(chunks):
        for k, (sx, sy) in enumerate(sources):
            g_copy(c, k, sx, sy, sx * ny + sy).wait()
        own_copy(c).wait()


def place_kernel(source_ref, filled_ref, blocks_ref, out_ref, zeros, out_sem):
    cap = out_ref.shape[0]

    def store(slot):
        return pltpu.make_async_copy(blocks_ref.at[source_ref[slot]], out_ref.at[slot], out_sem.at[slot])

    for slot in range(cap):
        pl.when(filled_ref[slot] == 1)(lambda slot=slot: store(slot).start())
    zeros[...] = jnp.zeros_like(zeros)
    for slot in range(cap):

        @pl.when(filled_ref[slot] == 0)
        def _():
            pltpu.make_async_copy(zeros, out_ref.at[slot], out_sem.at[slot]).start()

    for slot in range(cap):
        store(slot).wait()


def direct(embeds, dest_device, shuffle_key, lengths, gain):
    tiles_here, tile_rows, width = embeds.shape
    nx, ny, depth = lax.axis_size("gx"), lax.axis_size("gy"), lax.axis_size("gz")
    groups = nx * ny
    per_peer = (tiles_here + depth - 1) // depth
    slots = depth * per_peer
    chunk_rows = (tile_rows,)
    if tile_rows % 128 == 0:
        chunk_rows = tuple(part * tile_rows // 16 for part in (1, 1, 2, 2, 4, 4, 2))
    chunks = len(chunk_rows)

    smem = pl.BlockSpec(memory_space=pltpu.SMEM)
    vmem = pl.BlockSpec(memory_space=pltpu.VMEM)
    hbm = pl.BlockSpec(memory_space=pl.ANY)
    lanes = -(-2 * per_peer // 128) * 128
    small = jnp.concatenate([dest_device, shuffle_key, lengths])
    small = jnp.pad(small, (0, -small.shape[0] % 128))[None, :]
    received, key_rows = pl.pallas_call(
        functools.partial(exchange_kernel, (nx, ny, depth, per_peer, chunk_rows)),
        out_shape=(
            jax.ShapeDtypeStruct((groups, tile_rows, width), jnp.bfloat16),
            jax.ShapeDtypeStruct((groups, 1, 128), jnp.int32),
        ),
        in_specs=[hbm] * 3,
        out_specs=(hbm, vmem),
        scratch_shapes=[
            pltpu.SMEM(small.shape, jnp.int32),
            pltpu.VMEM((1, width), jnp.float32),
            pltpu.SemaphoreType.DMA,
            pltpu.SMEM((slots,), jnp.int32),
            pltpu.SMEM((slots,), jnp.int32),
            pltpu.VMEM((depth, 1, lanes), jnp.int32),
            pltpu.VMEM((depth, 1, lanes), jnp.int32),
            pltpu.SMEM((depth, 1, lanes), jnp.int32),
            pltpu.SMEM((groups,), jnp.int32),
            pltpu.VMEM((groups, 1, 128), jnp.int32),
            pltpu.SemaphoreType.DMA((chunks,)),
            pltpu.SemaphoreType.DMA,
            pltpu.SemaphoreType.DMA((chunks, depth - 1)),
            pltpu.SemaphoreType.DMA((chunks, depth - 1)),
            pltpu.SemaphoreType.DMA((chunks, groups)),
            pltpu.SemaphoreType.DMA((chunks, groups)),
            pltpu.SemaphoreType.DMA((chunks,)),
            pltpu.SemaphoreType.DMA((depth,)),
            pltpu.SemaphoreType.DMA((depth,)),
            pltpu.SemaphoreType.DMA((depth,)),
            pltpu.SemaphoreType.DMA((groups,)),
            pltpu.SemaphoreType.DMA((groups,)),
        ]
        + [pltpu.VMEM((tiles_here, rows, width), jnp.bfloat16) for rows in chunk_rows]
        + [pltpu.VMEM((depth - 1, per_peer, rows, width), jnp.bfloat16) for rows in chunk_rows]
        + [pltpu.VMEM((slots, rows, width), jnp.bfloat16) for rows in chunk_rows]
        + [pltpu.VMEM((groups, rows, width), jnp.bfloat16) for rows in chunk_rows],
        compiler_params=pltpu.CompilerParams(
            collective_id=0, has_side_effects=True, vmem_limit_bytes=36 * 1024 * 1024
        ),
        name="exchange",
    )(small, embeds, gain.reshape(1, width))

    key_of = key_rows[:, 0, 0]
    valid = key_of > 0
    rank = jnp.sum((valid[None, :] & (key_of[None, :] < key_of[:, None])).astype(jnp.int32), axis=1)
    cap = 2 * tiles_here
    at = valid[None, :] & (rank[None, :] == jnp.arange(cap, dtype=jnp.int32)[:, None])
    source = jnp.sum(jnp.where(at, jnp.arange(groups, dtype=jnp.int32)[None, :], 0), axis=1).astype(jnp.int32)
    filled = jnp.sum(at.astype(jnp.int32), axis=1).astype(jnp.int32)

    return pl.pallas_call(
        place_kernel,
        out_shape=jax.ShapeDtypeStruct((cap, tile_rows, width), jnp.bfloat16),
        in_specs=[smem, smem, vmem],
        out_specs=hbm,
        scratch_shapes=[
            pltpu.VMEM((tile_rows, width), jnp.bfloat16),
            pltpu.SemaphoreType.DMA((cap,)),
        ],
        compiler_params=pltpu.CompilerParams(vmem_limit_bytes=24 * 1024 * 1024),
        name="place",
    )(source, filled, received)


def table_kernel(
    sizes, dest_hbm, key_hbm, lengths_hbm, x_ref, gain_hbm, table_ref, normed_ref,
    dest_ref, lengths_ref, dest_row, key_row, gain_ref, small_sem, mine, first_table, limit_table, raw, done, send, recv, x_sem, out_sem,
):
    nx, ny, depth, per_peer = sizes
    devices = nx * ny * depth
    tiles_here, tile_rows, width = x_ref.shape
    slots = depth * per_peer
    block = 16
    me = (lax.axis_index("gx") * ny + lax.axis_index("gy")) * depth + lax.axis_index("gz")

    def place_of(device):
        return lax.div(device, ny * depth), lax.rem(lax.div(device, depth), ny), lax.rem(device, depth)

    def row_copy(step, target, row):
        return pltpu.make_async_remote_copy(
            src_ref=mine,
            dst_ref=table_ref.at[row],
            send_sem=send.at[step - 1],
            recv_sem=recv.at[step - 1],
            device_id=place_of(target),
            device_id_type=MESH,
        )

    def normalize(slot):
        @pl.loop(0, tile_rows // block)
        def _(part):
            start = part * block
            values = raw[first_table[slot], pl.ds(start, block)].astype(jnp.float32)
            meansq = jnp.mean(values * values, axis=-1, keepdims=True)
            scaled = values * lax.rsqrt(jnp.maximum(meansq, 0.25)) * gain_ref[...]
            row = start + lax.broadcasted_iota(jnp.int32, (block, 1), 0)
            done[slot, pl.ds(start, block)] = jnp.where(row < limit_table[slot], scaled, 0.0).astype(jnp.bfloat16)

        pltpu.make_async_copy(done.at[slot], normed_ref.at[slot], out_sem.at[slot]).start()

    small = [
        pltpu.make_async_copy(dest_hbm, dest_row, small_sem.at[0]),
        pltpu.make_async_copy(key_hbm, key_row, small_sem.at[1]),
        pltpu.make_async_copy(dest_hbm, dest_ref, small_sem.at[2]),
        pltpu.make_async_copy(lengths_hbm, lengths_ref, small_sem.at[3]),
        pltpu.make_async_copy(gain_hbm, gain_ref, small_sem.at[4]),
    ]
    load = pltpu.make_async_copy(x_ref, raw, x_sem)
    for copy in small:
        copy.start()
    load.start()
    barrier = pltpu.get_barrier_semaphore()
    for step in range(1, devices):
        pl.semaphore_signal(
            barrier, inc=1, device_id=place_of(lax.rem(me + step, devices)), device_id_type=MESH
        )
    for copy in small:
        copy.wait()
    mine[...] = jnp.zeros_like(mine)
    mine[0:1, 0:tiles_here] = dest_row[...]
    mine[1:2, 0:tiles_here] = key_row[...]
    table_ref[me] = mine[...]

    depths = [lax.rem(dest_ref[0, i], depth) for i in range(tiles_here)]
    places, limits = [], []
    for i in range(tiles_here):
        spot = jnp.int32(0)
        for j in range(i):
            spot = spot + jnp.where(depths[j] == depths[i], 1, 0)
        places.append(depths[i] * per_peer + spot)
        tile = me * tiles_here + i
        limits.append(jnp.maximum(lengths_ref[0, tile // TILES_SEQ] - tile % TILES_SEQ * tile_rows, 0))
    for slot in range(slots):
        tile, limit = jnp.int32(0), jnp.int32(0)
        for i in range(tiles_here):
            tile = jnp.where(places[i] == slot, i, tile)
            limit = jnp.where(places[i] == slot, limits[i], limit)
        first_table[slot] = tile
        limit_table[slot] = limit

    load.wait()
    early = slots // 2
    for slot in range(early):
        normalize(slot)
    pl.semaphore_wait(barrier, devices - 1)
    for step in range(1, devices):
        row_copy(step, lax.rem(me + step, devices), me).start()
    for slot in range(early, slots):
        normalize(slot)
    for step in range(1, devices):
        source = lax.rem(me + devices - step, devices)
        row_copy(step, source, source).wait()
    for slot in range(slots):
        pltpu.make_async_copy(done.at[slot], normed_ref.at[slot], out_sem.at[slot]).wait()


def line_kernel(
    sizes, plan_ref, x_ref, received,
    plan, plan_sem, x_sem, y_send, y_recv, a_send, a_recv, b_send, b_recv,
    g_send, g_recv, *buffers,
):
    nx, ny, depth, per_peer, pieces, near, far, back, at = sizes
    chunks = len(pieces)
    half = ny // 2
    slots = depth * per_peer
    pool, inflow, inward, outward, outgoing = (
        buffers[i * chunks : (i + 1) * chunks] for i in range(5)
    )
    gx, gy, gz = lax.axis_index("gx"), lax.axis_index("gy"), lax.axis_index("gz")
    low = gy < half
    level = jnp.where(low, gy, ny - 1 - gy)
    inner = jnp.where(low, gy + 1, gy - 1)
    outer = jnp.clip(jnp.where(low, gy - 1, gy + 1), 0, ny - 1)
    middle = level == half - 1

    def piece(ref, start, size, c):
        row, rows, column, columns = pieces[c]
        return ref.at[pl.ds(start, size), pl.ds(row, rows), pl.ds(column, columns)]

    def load(c):
        return pltpu.make_async_copy(
            piece(x_ref, gz * per_peer, per_peer, c),
            pool[c].at[pl.ds(gz * per_peer, per_peer)],
            x_sem.at[c],
        )

    def y_copy(c, dz, peer, origin):
        return pltpu.make_async_remote_copy(
            src_ref=piece(x_ref, peer * per_peer, per_peer, c),
            dst_ref=pool[c].at[pl.ds(origin * per_peer, per_peer)],
            send_sem=y_send.at[c, dz - 1],
            recv_sem=y_recv.at[c, dz - 1],
            device_id=(gx, gy, peer),
            device_id_type=MESH,
        )

    def near_copy(c, peer):
        return pltpu.make_async_remote_copy(
            src_ref=inward[c].at[pl.ds(0, near)],
            dst_ref=pool[c].at[pl.ds(slots, near)],
            send_sem=a_send.at[c],
            recv_sem=a_recv.at[c],
            device_id=(gx, peer, gz),
            device_id_type=MESH,
        )

    def cross_copy(c, peer):
        return pltpu.make_async_remote_copy(
            src_ref=inward[c],
            dst_ref=inflow[c],
            send_sem=a_send.at[c],
            recv_sem=b_recv.at[c],
            device_id=(gx, peer, gz),
            device_id_type=MESH,
        )

    def back_copy(c, peer):
        return pltpu.make_async_remote_copy(
            src_ref=outward[c],
            dst_ref=inflow[c].at[pl.ds(0, back)],
            send_sem=b_send.at[c],
            recv_sem=b_recv.at[c],
            device_id=(gx, peer, gz),
            device_id_type=MESH,
        )

    def g_copy(c, dx, peer, origin):
        return pltpu.make_async_remote_copy(
            src_ref=outgoing[c].at[dx - 1],
            dst_ref=piece(received, origin * ny, ny, c),
            send_sem=g_send.at[c, dx - 1],
            recv_sem=g_recv.at[c, dx - 1],
            device_id=(peer, gy, gz),
            device_id_type=MESH,
        )

    def either(c, code):
        held = pool[c][jnp.clip(code, 0, slots + near - 1)]
        came = inflow[c][jnp.clip(code - slots - near, 0, far - 1)]
        return jnp.where(code < slots + near, held, came)

    def send_inward(c, crosses, relays):
        load(c).wait()
        for dz in range(1, depth):
            origin = lax.rem(gz + depth - dz, depth)
            y_copy(c, dz, origin, origin).wait_recv()
        if relays:
            near_copy(c, outer).wait_recv()

        @pl.loop(0, far if crosses else near)
        def _(p):
            inward[c][p] = pool[c][plan[0, at["inward"] + p]]

        if crosses:
            cross_copy(c, inner).start()
        else:
            near_copy(c, inner).start()

    def deliver(c, crosses, relays):
        if crosses:
            cross_copy(c, inner).wait_recv()
        else:
            back_copy(c, inner).wait_recv()
        if relays:

            @pl.loop(0, back)
            def _(p):
                outward[c][p] = either(c, plan[0, at["outward"] + p])

            back_copy(c, outer).start()
        for dx in range(1, nx):
            peer = lax.rem(gx + dx, nx)

            @pl.loop(0, ny)
            def _(k):
                outgoing[c][dx - 1, k] = either(c, plan[0, at["deliver"] + peer * ny + k])

            g_copy(c, dx, peer, gx).start()

        @pl.loop(0, ny)
        def _(k):
            row, rows, column, columns = pieces[c]
            received[gx * ny + k, pl.ds(row, rows), pl.ds(column, columns)] = either(c, plan[0, at["deliver"] + gx * ny + k])

    def stream(crosses, relays):
        area = [rows * columns / (pieces[-1][0] + pieces[-1][1]) for _, rows, _, columns in pieces]
        area = [a * 16 / sum(area) for a in area]
        events = []
        for c in range(chunks):
            upto = sum(area[: c + 1])
            sent = near * (upto - area[c])
            landed = near * area[0] + far * (upto + area[c]) + LATENCY
            if crosses or relays:
                sent, landed = c, c + AHEAD + 0.5
            events.append((sent, 0, c))
            events.append((landed, 1, c))
        for _, kind, c in sorted(events):
            if kind == 0:
                send_inward(c, crosses, relays)
            else:
                deliver(c, crosses, relays)
        for c in range(chunks):
            if crosses:
                cross_copy(c, inner).wait_send()
            else:
                near_copy(c, inner).wait_send()
            if relays:
                back_copy(c, outer).wait_send()

    fetch = pltpu.make_async_copy(plan_ref, plan, plan_sem)
    fetch.start()
    for c in range(chunks):
        load(c).start()
    barrier = pltpu.get_barrier_semaphore()
    for dz in range(1, depth):
        pl.semaphore_signal(
            barrier, inc=1, device_id=(gx, gy, lax.rem(gz + dz, depth)), device_id_type=MESH
        )
    for dx in range(1, nx):
        pl.semaphore_signal(
            barrier, inc=1, device_id=(lax.rem(gx + dx, nx), gy, gz), device_id_type=MESH
        )
    pl.semaphore_signal(barrier, inc=1, device_id=(gx, inner, gz), device_id_type=MESH)

    @pl.when(level > 0)
    def _():
        pl.semaphore_signal(barrier, inc=1, device_id=(gx, outer, gz), device_id_type=MESH)

    pl.semaphore_wait(barrier, depth - 1 + nx - 1 + 1 + jnp.where(level > 0, 1, 0))
    for c in range(chunks):
        for dz in range(1, depth):
            y_copy(c, dz, lax.rem(gz + dz, depth), gz).start()
    fetch.wait()

    if half == 1:
        stream(True, False)
    else:
        pl.when(level == 0)(lambda: stream(False, False))
        pl.when(middle)(lambda: stream(True, True))
        if half > 2:
            pl.when((level > 0) & jnp.logical_not(middle))(lambda: stream(False, True))

    for c in range(chunks):
        for dz in range(1, depth):
            y_copy(c, dz, lax.rem(gz + dz, depth), gz).wait_send()
        for dx in range(1, nx):
            origin = lax.rem(gx + nx - dx, nx)
            g_copy(c, dx, origin, origin).wait()


def count(mask):
    return jnp.sum(mask.astype(jnp.int32), axis=1)


def pick(value, mask, position, wanted):
    hit = mask[None, :] & (position[None, :] == jnp.arange(wanted, dtype=jnp.int32)[:, None])
    return jnp.sum(jnp.where(hit, value[None, :], 0), axis=1)


def shards(embeds, dest_device, shuffle_key, lengths, gain):
    tiles_here, tile_rows, width = embeds.shape
    nx, ny, depth = lax.axis_size("gx"), lax.axis_size("gy"), lax.axis_size("gz")
    devices = nx * ny * depth
    per_peer = (tiles_here + depth - 1) // depth
    slots = depth * per_peer
    half = ny // 2
    cap = 2 * tiles_here
    if ny % 2 or tile_rows % 128 or width % 512 or slots > tiles_here:
        return direct(embeds, dest_device, shuffle_key, lengths, gain)

    most = half * min(tiles_here, nx * half)
    near_most = max([(e + 1) * min(tiles_here, nx * (ny - 1 - e)) for e in range(half - 1)] + [1])
    back_most = max([(ny - e) * min(tiles_here, nx * e) for e in range(1, half)] + [1])
    classes = sorted({max(1, most * part // 16) for part in CLASSES})

    vmem = pl.BlockSpec(memory_space=pltpu.VMEM)
    smem = pl.BlockSpec(memory_space=pltpu.SMEM)
    hbm = pl.BlockSpec(memory_space=pl.ANY)
    lanes = -(-tiles_here // 128) * 128
    table, normed = pl.pallas_call(
        functools.partial(table_kernel, (nx, ny, depth, per_peer)),
        out_shape=(
            jax.ShapeDtypeStruct((devices, 2, lanes), jnp.int32),
            pltpu.HBM((slots, tile_rows, width), jnp.bfloat16),
        ),
        in_specs=[pl.BlockSpec(memory_space=pltpu.HBM)] * 5,
        out_specs=(vmem, pl.BlockSpec(memory_space=pltpu.HBM)),
        scratch_shapes=[
            pltpu.SMEM((1, tiles_here), jnp.int32),
            pltpu.SMEM((1, lengths.shape[0]), jnp.int32),
            pltpu.VMEM((1, tiles_here), jnp.int32),
            pltpu.VMEM((1, tiles_here), jnp.int32),
            pltpu.VMEM((1, width), jnp.float32),
            pltpu.SemaphoreType.DMA((5,)),
            pltpu.VMEM((2, lanes), jnp.int32),
            pltpu.SMEM((slots,), jnp.int32),
            pltpu.SMEM((slots,), jnp.int32),
            pltpu.VMEM((tiles_here, tile_rows, width), jnp.bfloat16),
            pltpu.VMEM((slots, tile_rows, width), jnp.bfloat16),
            pltpu.SemaphoreType.DMA((devices - 1,)),
            pltpu.SemaphoreType.DMA((devices - 1,)),
            pltpu.SemaphoreType.DMA,
            pltpu.SemaphoreType.DMA((slots,)),
        ],
        compiler_params=pltpu.CompilerParams(
            collective_id=0, has_side_effects=True, vmem_limit_bytes=56 * 1024 * 1024
        ),
        name="tables",
    )(dest_device[None, :], shuffle_key[None, :], lengths[None, :], embeds, gain.reshape(1, width))

    gx, gy, gz = lax.axis_index("gx"), lax.axis_index("gy"), lax.axis_index("gz")
    group = gx * ny + gy
    me = group * depth + gz
    dest = table[:, 0, :tiles_here].reshape(-1)
    keys = table[:, 1, :tiles_here].reshape(-1)
    order = jnp.arange(devices * tiles_here, dtype=jnp.int32)
    before = order[None, :] < order[:, None]
    source = order // tiles_here
    from_x, from_y = source // (ny * depth), source // depth % ny
    to_x, to_y, to_z = dest // (ny * depth), dest // depth % ny, dest % depth

    bounds = jnp.arange(ny - 1, dtype=jnp.int32)
    lane = from_x * depth + to_z
    hop_up = (from_y[None, :] <= bounds[:, None]) & (to_y[None, :] > bounds[:, None])
    hop_down = (from_y[None, :] > bounds[:, None]) & (to_y[None, :] <= bounds[:, None])
    hops = jnp.concatenate([hop_up, hop_down])
    in_lane = lane[None, :] == jnp.arange(nx * depth, dtype=jnp.int32)[:, None]
    load = jnp.max(jnp.sum((hops[:, None, :] & in_lane[None, :, :]).astype(jnp.int32), axis=2))

    low = gy < half
    level = jnp.where(low, gy, ny - 1 - gy)
    depth_from = jnp.where(low, from_y, ny - 1 - from_y)
    depth_to = jnp.where(low, to_y, ny - 1 - to_y)
    in_my_lane = (from_x == gx) & (to_z == gz)
    inward = in_my_lane & (depth_from <= level) & (depth_to > level)
    near_in = in_my_lane & (depth_from < level) & (depth_to >= level)
    outward = in_my_lane & (depth_from >= level) & (depth_to < level)
    far_in = in_my_lane & (depth_from > level) & (depth_to <= level)
    landing = in_my_lane & (depth_to == level)
    to_me = dest == me

    same_source = source[:, None] == source[None, :]
    spot = count(before & same_source & (to_z[:, None] == to_z[None, :]))
    at_inward = count(before & inward[None, :])
    at_near = count(before & near_in[None, :])
    at_outward = count(before & outward[None, :])
    at_far = count(before & far_in[None, :])
    at_landing = count(before & (landing[None, :] & (to_x[:, None] == to_x[None, :])))
    at_me = count(before & (to_me[None, :] & (from_x[:, None] == from_x[None, :])))
    rank = count((keys[None, :] < keys[:, None]) & to_me[None, :])
    own_slot = source % depth * per_peer + spot

    chosen = jnp.int32(0)
    for bound in classes[:-1]:
        chosen = chosen + (load > bound).astype(jnp.int32)
    far = jnp.full((), classes[-1], jnp.int32)
    for index, bound in enumerate(classes[:-1]):
        far = jnp.where(chosen == index, bound, far)
    near = jnp.minimum(far, near_most)
    code = jnp.where(
        depth_from == level,
        own_slot,
        jnp.where(depth_from < level, slots + at_near, slots + near + at_far),
    )
    parts = {
        "inward": pick(code, inward, at_inward, most),
        "outward": pick(code, outward, at_outward, back_most),
        "deliver": pick(code, landing, to_x * ny + at_landing, nx * ny),
    }
    at, total = {}, 0
    for name, part in parts.items():
        at[name] = total
        total += part.shape[0]
    plan = jnp.pad(jnp.concatenate(list(parts.values())), (0, -total % 128))[None, :]
    which = pick(from_x * ny + at_me + 1, to_me, rank, cap)

    pieces, done = [], 0
    for part in CHUNKS:
        row, column = done // 4 * tile_rows // 16, done % 4 * width // 4
        if part % 4 == 0:
            pieces.append((row, part // 4 * tile_rows // 16, 0, width))
        else:
            pieces.append((row, tile_rows // 16, column, part * width // 4))
        done += part
    pieces = tuple(pieces)
    chunks = len(pieces)

    def branch(index, far):
        def run(plan, normed, chosen_rows, filled):
            near, back = min(far, near_most), min(far, back_most)
            counts = ((slots + near,), (far,), (far,), (back,), (nx - 1, ny))
            received = pl.pallas_call(
                functools.partial(
                    line_kernel, (nx, ny, depth, per_peer, pieces, near, far, back, at)
                ),
                out_shape=pltpu.VMEM((nx * ny, tile_rows, width), jnp.bfloat16),
                in_specs=[hbm, pl.BlockSpec(memory_space=pltpu.HBM)],
                out_specs=vmem,
                scratch_shapes=[
                    pltpu.SMEM(plan.shape, jnp.int32),
                    pltpu.SemaphoreType.DMA,
                    pltpu.SemaphoreType.DMA((chunks,)),
                    pltpu.SemaphoreType.DMA((chunks, depth - 1)),
                    pltpu.SemaphoreType.DMA((chunks, depth - 1)),
                    pltpu.SemaphoreType.DMA((chunks,)),
                    pltpu.SemaphoreType.DMA((chunks,)),
                    pltpu.SemaphoreType.DMA((chunks,)),
                    pltpu.SemaphoreType.DMA((chunks,)),
                    pltpu.SemaphoreType.DMA((chunks, nx - 1)),
                    pltpu.SemaphoreType.DMA((chunks, nx - 1)),
                ]
                + [
                    pltpu.VMEM((*lead, rows, columns), jnp.bfloat16)
                    for lead in counts
                    for _, rows, _, columns in pieces
                ],
                compiler_params=pltpu.CompilerParams(
                    collective_id=1 + index, has_side_effects=True, vmem_limit_bytes=44 * 1024 * 1024
                ),
                name=f"line{far}",
            )(plan, normed)
            return pl.pallas_call(
                place_kernel,
                out_shape=pltpu.HBM((cap, tile_rows, width), jnp.bfloat16),
                in_specs=[smem, smem, vmem],
                out_specs=pl.BlockSpec(memory_space=pltpu.HBM),
                scratch_shapes=[
                    pltpu.VMEM((tile_rows, width), jnp.bfloat16),
                    pltpu.SemaphoreType.DMA((cap,)),
                ],
                compiler_params=pltpu.CompilerParams(vmem_limit_bytes=24 * 1024 * 1024),
                name="place",
            )(chosen_rows, filled, received)

        return run

    return lax.switch(
        chosen,
        [branch(i, far) for i, far in enumerate(classes)],
        plan,
        normed,
        jnp.maximum(which - 1, 0),
        (which > 0).astype(jnp.int32),
    )


def solution(mesh):
    return jax.shard_map(
        shards,
        mesh=mesh,
        in_specs=(
            P(("gx", "gy", "gz"), None, None),
            P(("gx", "gy", "gz")),
            P(("gx", "gy", "gz")),
            P(),
            P(),
        ),
        out_specs=P(("gx", "gy", "gz"), None, None),
        check_vma=False,
    )
```

```python
import functools

import jax
import jax.numpy as jnp
from jax import lax
from jax.experimental import pallas as pl
from jax.experimental.pallas import tpu as pltpu
from jax.sharding import PartitionSpec as P

TILES_SEQ = 32
CLASSES = (9, 10, 11, 12, 13, 16)
CHUNKS = (2,) * 32
LATENCY = 11
AHEAD = 1
MESH = pl.DeviceIdType.MESH


def exchange_kernel(
    sizes, small_in, x_ref, gain_ref, recv_ref, keys_ref,
    small_ref, gain, small_sem, first_table, limit_table, note_out, notes, note_table, second, keys_out,
    x_sem, gain_sem, y_send, y_recv, g_send, g_recv, own_sem,
    note_send, note_recv, note_sem, key_send, key_recv, *buffers,
):
    nx, ny, depth, per_peer, chunk_rows = sizes
    chunks = len(chunk_rows)
    starts = [sum(chunk_rows[:c]) for c in range(chunks)]
    groups = nx * ny
    tiles_here, tile_rows, _ = x_ref.shape
    raw, first, arrived, outgoing = (buffers[i * chunks : (i + 1) * chunks] for i in range(4))
    gx, gy, gz = lax.axis_index("gx"), lax.axis_index("gy"), lax.axis_index("gz")
    group = gx * ny + gy
    me = group * depth + gz
    offsets = [(dx, dy) for dy in sorted(range(ny), key=lambda d: abs(d - ny // 2)) for dx in range(nx)]
    offsets.remove((0, 0))

    def load(c):
        return pltpu.make_async_copy(
            x_ref.at[:, pl.ds(starts[c], chunk_rows[c])], raw[c], x_sem.at[c]
        )

    def fill_tables():
        depths = [lax.rem(small_ref[0, i], depth) for i in range(tiles_here)]
        dest_groups = [lax.div(small_ref[0, i], depth) for i in range(tiles_here)]
        places, limits = [], []
        for i in range(tiles_here):
            spot = jnp.int32(0)
            for j in range(i):
                spot = spot + jnp.where(depths[j] == depths[i], 1, 0)
            places.append(depths[i] * per_peer + spot)
            tile = me * tiles_here + i
            length = small_ref[0, 2 * tiles_here + tile // TILES_SEQ]
            limits.append(jnp.maximum(length - tile % TILES_SEQ * tile_rows, 0))
        lane = lax.broadcasted_iota(jnp.int32, note_out.shape[1:], 1)
        for z in range(depth):
            row = jnp.zeros(note_out.shape[1:], jnp.int32)
            for p in range(per_peer):
                slot = z * per_peer + p
                tile, limit, dest_group, key = (jnp.int32(v) for v in (0, 0, -1, 0))
                for i in range(tiles_here):
                    hit = places[i] == slot
                    tile = jnp.where(hit, i, tile)
                    limit = jnp.where(hit, limits[i], limit)
                    dest_group = jnp.where(hit, dest_groups[i], dest_group)
                    key = jnp.where(hit, small_ref[0, tiles_here + i] + 1, key)
                first_table[slot] = tile
                limit_table[slot] = limit
                row = jnp.where(lane == p, dest_group, row)
                row = jnp.where(lane == per_peer + p, key, row)
            note_out[z] = row

    def normed(c, slot):
        rows = chunk_rows[c]
        values = raw[c][first_table[slot]].astype(jnp.float32)
        meansq = jnp.mean(values * values, axis=-1, keepdims=True)
        scaled = values * lax.rsqrt(jnp.maximum(meansq, 0.25)) * gain[...]
        row = starts[c] + lax.broadcasted_iota(jnp.int32, (rows, 1), 0)
        return jnp.where(row < limit_table[slot], scaled, 0.0).astype(jnp.bfloat16)

    def y_copy(c, dz, peer, origin):
        return pltpu.make_async_remote_copy(
            src_ref=first[c].at[dz - 1],
            dst_ref=arrived[c].at[pl.ds(origin * per_peer, per_peer)],
            send_sem=y_send.at[c, dz - 1],
            recv_sem=y_recv.at[c, dz - 1],
            device_id=(gx, gy, peer),
            device_id_type=MESH,
        )

    def peer_of(k):
        dx, dy = offsets[k]
        return lax.rem(gx + dx, nx), lax.rem(gy + dy, ny)

    def g_copy(c, k, px, py, origin):
        return pltpu.make_async_remote_copy(
            src_ref=outgoing[c].at[k],
            dst_ref=recv_ref.at[origin, pl.ds(starts[c], chunk_rows[c])],
            send_sem=g_send.at[c, k],
            recv_sem=g_recv.at[c, k],
            device_id=(px, py, gz),
            device_id_type=MESH,
        )

    def own_copy(c):
        return pltpu.make_async_copy(
            outgoing[c].at[groups - 1],
            recv_ref.at[group, pl.ds(starts[c], chunk_rows[c])],
            own_sem.at[c],
        )

    def note_copy(dz, peer, place):
        return pltpu.make_async_remote_copy(
            src_ref=note_out.at[peer],
            dst_ref=notes.at[place],
            send_sem=note_send.at[dz - 1],
            recv_sem=note_recv.at[dz - 1],
            device_id=(gx, gy, peer),
            device_id_type=MESH,
        )

    def key_copy(k, px, py, place):
        return pltpu.make_async_remote_copy(
            src_ref=keys_out.at[k],
            dst_ref=keys_ref.at[place],
            send_sem=key_send.at[k],
            recv_sem=key_recv.at[k],
            device_id=(px, py, gz),
            device_id_type=MESH,
        )

    def prepare(c):
        load(c).wait()
        for dz in range(1, depth):
            peer = lax.rem(gz + dz, depth)
            for p in range(per_peer):
                first[c][dz - 1, p] = normed(c, peer * per_peer + p)
        for p in range(per_peer):
            arrived[c][gz * per_peer + p] = normed(c, gz * per_peer + p)

    def send_first(c):
        for dz in range(1, depth):
            y_copy(c, dz, lax.rem(gz + dz, depth), gz).start()

    def find_slots():
        for dz in range(1, depth):
            origin = lax.rem(gz + depth - dz, depth)
            note_copy(dz, origin, origin).wait()
        tables = [
            pltpu.make_async_copy(
                notes.at[lax.rem(gz + dz, depth)], note_table.at[lax.rem(gz + dz, depth)], note_sem.at[dz]
            )
            for dz in range(1, depth)
        ]
        tables.append(pltpu.make_async_copy(note_out.at[gz], note_table.at[gz], note_sem.at[0]))
        for copy in tables:
            copy.start()
        for copy in tables:
            copy.wait()

        for k in range(groups):
            px, py = peer_of(k) if k < groups - 1 else (gx, gy)
            wanted = px * ny + py
            slot, key = jnp.int32(0), jnp.int32(0)
            for z in range(depth):
                for p in range(per_peer):
                    hit = note_table[z, 0, p] == wanted
                    slot = jnp.where(hit, z * per_peer + p, slot)
                    key = jnp.where(hit, note_table[z, 0, per_peer + p], key)
            second[k] = slot
            row = jnp.full(keys_out.shape[1:], key, jnp.int32)
            if k < groups - 1:
                keys_out[k] = row
            else:
                keys_ref[group] = row

    def forward(c):
        for dz in range(1, depth):
            origin = lax.rem(gz + depth - dz, depth)
            y_copy(c, dz, origin, origin).wait_recv()
        for k in range(groups):
            outgoing[c][k] = arrived[c][second[k]]
        for k in range(groups - 1):
            px, py = peer_of(k)
            g_copy(c, k, px, py, group).start()
        own_copy(c).start()

    small = [
        pltpu.make_async_copy(small_in, small_ref, small_sem),
        pltpu.make_async_copy(gain_ref, gain, gain_sem),
    ]
    for copy in small:
        copy.start()
    for c in range(chunks):
        load(c).start()
    barrier = pltpu.get_barrier_semaphore()
    for dz in range(1, depth):
        pl.semaphore_signal(
            barrier, inc=1, device_id=(gx, gy, lax.rem(gz + dz, depth)), device_id_type=MESH
        )
    for k in range(groups - 1):
        px, py = peer_of(k)
        pl.semaphore_signal(barrier, inc=1, device_id=(px, py, gz), device_id_type=MESH)
    for copy in small:
        copy.wait()
    fill_tables()
    prepare(0)
    pl.semaphore_wait(barrier, depth - 1 + groups - 1)
    for dz in range(1, depth):
        note_copy(dz, lax.rem(gz + dz, depth), gz).start()
    send_first(0)
    if chunks > 1:
        prepare(1)
        send_first(1)
    find_slots()
    forward(0)
    for k in range(groups - 1):
        px, py = peer_of(k)
        key_copy(k, px, py, group).start()
    for c in range(2, chunks):
        prepare(c)
        send_first(c)
        forward(c - 1)
    if chunks > 1:
        forward(chunks - 1)

    for c in range(chunks):
        for dz in range(1, depth):
            y_copy(c, dz, lax.rem(gz + dz, depth), gz).wait_send()
    sources = []
    for dx, dy in offsets:
        sources.append((lax.rem(gx + nx - dx, nx), lax.rem(gy + ny - dy, ny)))
    for k, (sx, sy) in enumerate(sources):
        key_copy(k, sx, sy, sx * ny + sy).wait()
    for c in range(chunks):
        for k, (sx, sy) in enumerate(sources):
            g_copy(c, k, sx, sy, sx * ny + sy).wait()
        own_copy(c).wait()


def place_kernel(source_ref, filled_ref, blocks_ref, out_ref, zeros, out_sem):
    cap = out_ref.shape[0]

    def store(slot):
        return pltpu.make_async_copy(blocks_ref.at[source_ref[slot]], out_ref.at[slot], out_sem.at[slot])

    for slot in range(cap):
        pl.when(filled_ref[slot] == 1)(lambda slot=slot: store(slot).start())
    zeros[...] = jnp.zeros_like(zeros)
    for slot in range(cap):

        @pl.when(filled_ref[slot] == 0)
        def _():
            pltpu.make_async_copy(zeros, out_ref.at[slot], out_sem.at[slot]).start()

    for slot in range(cap):
        store(slot).wait()


def direct(embeds, dest_device, shuffle_key, lengths, gain):
    tiles_here, tile_rows, width = embeds.shape
    nx, ny, depth = lax.axis_size("gx"), lax.axis_size("gy"), lax.axis_size("gz")
    groups = nx * ny
    per_peer = (tiles_here + depth - 1) // depth
    slots = depth * per_peer
    chunk_rows = (tile_rows,)
    if tile_rows % 128 == 0:
        chunk_rows = tuple(part * tile_rows // 16 for part in (1, 1, 2, 2, 4, 4, 2))
    chunks = len(chunk_rows)

    smem = pl.BlockSpec(memory_space=pltpu.SMEM)
    vmem = pl.BlockSpec(memory_space=pltpu.VMEM)
    hbm = pl.BlockSpec(memory_space=pl.ANY)
    lanes = -(-2 * per_peer // 128) * 128
    small = jnp.concatenate([dest_device, shuffle_key, lengths])
    small = jnp.pad(small, (0, -small.shape[0] % 128))[None, :]
    received, key_rows = pl.pallas_call(
        functools.partial(exchange_kernel, (nx, ny, depth, per_peer, chunk_rows)),
        out_shape=(
            jax.ShapeDtypeStruct((groups, tile_rows, width), jnp.bfloat16),
            jax.ShapeDtypeStruct((groups, 1, 128), jnp.int32),
        ),
        in_specs=[hbm] * 3,
        out_specs=(hbm, vmem),
        scratch_shapes=[
            pltpu.SMEM(small.shape, jnp.int32),
            pltpu.VMEM((1, width), jnp.float32),
            pltpu.SemaphoreType.DMA,
            pltpu.SMEM((slots,), jnp.int32),
            pltpu.SMEM((slots,), jnp.int32),
            pltpu.VMEM((depth, 1, lanes), jnp.int32),
            pltpu.VMEM((depth, 1, lanes), jnp.int32),
            pltpu.SMEM((depth, 1, lanes), jnp.int32),
            pltpu.SMEM((groups,), jnp.int32),
            pltpu.VMEM((groups, 1, 128), jnp.int32),
            pltpu.SemaphoreType.DMA((chunks,)),
            pltpu.SemaphoreType.DMA,
            pltpu.SemaphoreType.DMA((chunks, depth - 1)),
            pltpu.SemaphoreType.DMA((chunks, depth - 1)),
            pltpu.SemaphoreType.DMA((chunks, groups)),
            pltpu.SemaphoreType.DMA((chunks, groups)),
            pltpu.SemaphoreType.DMA((chunks,)),
            pltpu.SemaphoreType.DMA((depth,)),
            pltpu.SemaphoreType.DMA((depth,)),
            pltpu.SemaphoreType.DMA((depth,)),
            pltpu.SemaphoreType.DMA((groups,)),
            pltpu.SemaphoreType.DMA((groups,)),
        ]
        + [pltpu.VMEM((tiles_here, rows, width), jnp.bfloat16) for rows in chunk_rows]
        + [pltpu.VMEM((depth - 1, per_peer, rows, width), jnp.bfloat16) for rows in chunk_rows]
        + [pltpu.VMEM((slots, rows, width), jnp.bfloat16) for rows in chunk_rows]
        + [pltpu.VMEM((groups, rows, width), jnp.bfloat16) for rows in chunk_rows],
        compiler_params=pltpu.CompilerParams(
            collective_id=0, has_side_effects=True, vmem_limit_bytes=36 * 1024 * 1024
        ),
        name="exchange",
    )(small, embeds, gain.reshape(1, width))

    key_of = key_rows[:, 0, 0]
    valid = key_of > 0
    rank = jnp.sum((valid[None, :] & (key_of[None, :] < key_of[:, None])).astype(jnp.int32), axis=1)
    cap = 2 * tiles_here
    at = valid[None, :] & (rank[None, :] == jnp.arange(cap, dtype=jnp.int32)[:, None])
    source = jnp.sum(jnp.where(at, jnp.arange(groups, dtype=jnp.int32)[None, :], 0), axis=1).astype(jnp.int32)
    filled = jnp.sum(at.astype(jnp.int32), axis=1).astype(jnp.int32)

    return pl.pallas_call(
        place_kernel,
        out_shape=jax.ShapeDtypeStruct((cap, tile_rows, width), jnp.bfloat16),
        in_specs=[smem, smem, vmem],
        out_specs=hbm,
        scratch_shapes=[
            pltpu.VMEM((tile_rows, width), jnp.bfloat16),
            pltpu.SemaphoreType.DMA((cap,)),
        ],
        compiler_params=pltpu.CompilerParams(vmem_limit_bytes=24 * 1024 * 1024),
        name="place",
    )(source, filled, received)


def table_kernel(
    sizes, dest_hbm, key_hbm, lengths_hbm, x_ref, gain_hbm, table_ref, normed_ref,
    dest_ref, lengths_ref, dest_row, key_row, gain_ref, small_sem, mine, first_table, limit_table, raw, done, send, recv, x_sem, out_sem,
):
    nx, ny, depth, per_peer = sizes
    devices = nx * ny * depth
    tiles_here, tile_rows, width = x_ref.shape
    slots = depth * per_peer
    block = 16
    me = (lax.axis_index("gx") * ny + lax.axis_index("gy")) * depth + lax.axis_index("gz")

    def place_of(device):
        return lax.div(device, ny * depth), lax.rem(lax.div(device, depth), ny), lax.rem(device, depth)

    def row_copy(step, target, row):
        return pltpu.make_async_remote_copy(
            src_ref=mine,
            dst_ref=table_ref.at[row],
            send_sem=send.at[step - 1],
            recv_sem=recv.at[step - 1],
            device_id=place_of(target),
            device_id_type=MESH,
        )

    def normalize(slot):
        @pl.loop(0, tile_rows // block)
        def _(part):
            start = part * block
            values = raw[first_table[slot], pl.ds(start, block)].astype(jnp.float32)
            meansq = jnp.mean(values * values, axis=-1, keepdims=True)
            scaled = values * lax.rsqrt(jnp.maximum(meansq, 0.25)) * gain_ref[...]
            row = start + lax.broadcasted_iota(jnp.int32, (block, 1), 0)
            done[slot, pl.ds(start, block)] = jnp.where(row < limit_table[slot], scaled, 0.0).astype(jnp.bfloat16)

        pltpu.make_async_copy(done.at[slot], normed_ref.at[slot], out_sem.at[slot]).start()

    small = [
        pltpu.make_async_copy(dest_hbm, dest_row, small_sem.at[0]),
        pltpu.make_async_copy(key_hbm, key_row, small_sem.at[1]),
        pltpu.make_async_copy(dest_hbm, dest_ref, small_sem.at[2]),
        pltpu.make_async_copy(lengths_hbm, lengths_ref, small_sem.at[3]),
        pltpu.make_async_copy(gain_hbm, gain_ref, small_sem.at[4]),
    ]
    load = pltpu.make_async_copy(x_ref, raw, x_sem)
    for copy in small:
        copy.start()
    load.start()
    barrier = pltpu.get_barrier_semaphore()
    for step in range(1, devices):
        pl.semaphore_signal(
            barrier, inc=1, device_id=place_of(lax.rem(me + step, devices)), device_id_type=MESH
        )
    for copy in small:
        copy.wait()
    mine[...] = jnp.zeros_like(mine)
    mine[0:1, 0:tiles_here] = dest_row[...]
    mine[1:2, 0:tiles_here] = key_row[...]
    table_ref[me] = mine[...]

    pl.semaphore_wait(barrier, devices - 1)
    for step in range(1, devices):
        row_copy(step, lax.rem(me + step, devices), me).start()
    depths = [lax.rem(dest_ref[0, i], depth) for i in range(tiles_here)]
    places, limits = [], []
    for i in range(tiles_here):
        spot = jnp.int32(0)
        for j in range(i):
            spot = spot + jnp.where(depths[j] == depths[i], 1, 0)
        places.append(depths[i] * per_peer + spot)
        tile = me * tiles_here + i
        limits.append(jnp.maximum(lengths_ref[0, tile // TILES_SEQ] - tile % TILES_SEQ * tile_rows, 0))
    for slot in range(slots):
        tile, limit = jnp.int32(0), jnp.int32(0)
        for i in range(tiles_here):
            tile = jnp.where(places[i] == slot, i, tile)
            limit = jnp.where(places[i] == slot, limits[i], limit)
        first_table[slot] = tile
        limit_table[slot] = limit

    load.wait()
    for slot in range(slots):
        normalize(slot)
    for step in range(1, devices):
        source = lax.rem(me + devices - step, devices)
        row_copy(step, source, source).wait()
    for slot in range(slots):
        pltpu.make_async_copy(done.at[slot], normed_ref.at[slot], out_sem.at[slot]).wait()


def line_kernel(
    sizes, plan_ref, x_ref, received,
    plan, plan_sem, x_sem, y_send, y_recv, a_send, a_recv, b_send, b_recv,
    g_send, g_recv, *buffers,
):
    nx, ny, depth, per_peer, pieces, near, far, back, at = sizes
    chunks = len(pieces)
    half = ny // 2
    slots = depth * per_peer
    pool, inflow, inward, outward, outgoing = (
        buffers[i * chunks : (i + 1) * chunks] for i in range(5)
    )
    gx, gy, gz = lax.axis_index("gx"), lax.axis_index("gy"), lax.axis_index("gz")
    low = gy < half
    level = jnp.where(low, gy, ny - 1 - gy)
    inner = jnp.where(low, gy + 1, gy - 1)
    outer = jnp.clip(jnp.where(low, gy - 1, gy + 1), 0, ny - 1)
    middle = level == half - 1

    def piece(ref, start, size, c):
        row, rows, column, columns = pieces[c]
        return ref.at[pl.ds(start, size), pl.ds(row, rows), pl.ds(column, columns)]

    def load(c):
        return pltpu.make_async_copy(
            piece(x_ref, gz * per_peer, per_peer, c),
            pool[c].at[pl.ds(gz * per_peer, per_peer)],
            x_sem.at[c],
        )

    def y_copy(c, dz, peer, origin):
        return pltpu.make_async_remote_copy(
            src_ref=piece(x_ref, peer * per_peer, per_peer, c),
            dst_ref=pool[c].at[pl.ds(origin * per_peer, per_peer)],
            send_sem=y_send.at[c, dz - 1],
            recv_sem=y_recv.at[c, dz - 1],
            device_id=(gx, gy, peer),
            device_id_type=MESH,
        )

    def near_copy(c, peer):
        return pltpu.make_async_remote_copy(
            src_ref=inward[c].at[pl.ds(0, near)],
            dst_ref=pool[c].at[pl.ds(slots, near)],
            send_sem=a_send.at[c],
            recv_sem=a_recv.at[c],
            device_id=(gx, peer, gz),
            device_id_type=MESH,
        )

    def cross_copy(c, peer):
        return pltpu.make_async_remote_copy(
            src_ref=inward[c],
            dst_ref=inflow[c],
            send_sem=a_send.at[c],
            recv_sem=b_recv.at[c],
            device_id=(gx, peer, gz),
            device_id_type=MESH,
        )

    def back_copy(c, peer):
        return pltpu.make_async_remote_copy(
            src_ref=outward[c],
            dst_ref=inflow[c].at[pl.ds(0, back)],
            send_sem=b_send.at[c],
            recv_sem=b_recv.at[c],
            device_id=(gx, peer, gz),
            device_id_type=MESH,
        )

    def g_copy(c, dx, peer, origin):
        return pltpu.make_async_remote_copy(
            src_ref=outgoing[c].at[pl.ds((dx - 1) * ny, ny)],
            dst_ref=piece(received, origin * ny, ny, c),
            send_sem=g_send.at[c, dx - 1],
            recv_sem=g_recv.at[c, dx - 1],
            device_id=(peer, gy, gz),
            device_id_type=MESH,
        )

    def either(c, code):
        held = pool[c][jnp.minimum(code, slots + near - 1)]
        came = inflow[c][jnp.clip(code - slots - near, 0, far - 1)]
        return jnp.where(code < slots + near, held, came)

    def send_inward(c, crosses, relays):
        load(c).wait()
        for dz in range(1, depth):
            origin = lax.rem(gz + depth - dz, depth)
            y_copy(c, dz, origin, origin).wait_recv()
        if relays:
            near_copy(c, outer).wait_recv()

        @pl.loop(0, far if crosses else near)
        def _(p):
            inward[c][p] = pool[c][plan[0, at["inward"] + p]]

        if crosses:
            cross_copy(c, inner).start()
        else:
            near_copy(c, inner).start()

    def deliver(c, crosses, relays):
        if crosses:
            cross_copy(c, inner).wait_recv()
        else:
            back_copy(c, inner).wait_recv()
        if relays:

            @pl.loop(0, back)
            def _(p):
                outward[c][p] = either(c, plan[0, at["outward"] + p])

            back_copy(c, outer).start()

        @pl.loop(0, (nx - 1) * ny)
        def _(k):
            outgoing[c][k] = either(c, plan[0, at["deliver"] + ny + k])

        for dx in range(1, nx):
            g_copy(c, dx, lax.rem(gx + dx, nx), gx).start()

        @pl.loop(0, ny)
        def _(k):
            row, rows, column, columns = pieces[c]
            received[gx * ny + k, pl.ds(row, rows), pl.ds(column, columns)] = either(
                c, plan[0, at["deliver"] + k]
            )

    def stream(crosses, relays):
        area = [rows * columns / (pieces[-1][0] + pieces[-1][1]) for _, rows, _, columns in pieces]
        area = [a * 16 / sum(area) for a in area]
        events = []
        for c in range(chunks):
            upto = sum(area[: c + 1])
            sent = near * (upto - area[c])
            landed = near * area[0] + far * (upto + area[c]) + LATENCY
            if crosses or relays:
                sent, landed = c, c + AHEAD + 0.5
            events.append((sent, 0, c))
            events.append((landed, 1, c))
        for _, kind, c in sorted(events):
            if kind == 0:
                send_inward(c, crosses, relays)
            else:
                deliver(c, crosses, relays)
        for c in range(chunks):
            if crosses:
                cross_copy(c, inner).wait_send()
            else:
                near_copy(c, inner).wait_send()
            if relays:
                back_copy(c, outer).wait_send()

    fetch = pltpu.make_async_copy(plan_ref, plan, plan_sem)
    fetch.start()
    for c in range(chunks):
        load(c).start()
    barrier = pltpu.get_barrier_semaphore()
    for dz in range(1, depth):
        pl.semaphore_signal(
            barrier, inc=1, device_id=(gx, gy, lax.rem(gz + dz, depth)), device_id_type=MESH
        )
    for dx in range(1, nx):
        pl.semaphore_signal(
            barrier, inc=1, device_id=(lax.rem(gx + dx, nx), gy, gz), device_id_type=MESH
        )
    pl.semaphore_signal(barrier, inc=1, device_id=(gx, inner, gz), device_id_type=MESH)

    @pl.when(level > 0)
    def _():
        pl.semaphore_signal(barrier, inc=1, device_id=(gx, outer, gz), device_id_type=MESH)

    pl.semaphore_wait(barrier, depth - 1 + nx - 1 + 1 + jnp.where(level > 0, 1, 0))
    for c in range(chunks):
        for dz in range(1, depth):
            y_copy(c, dz, lax.rem(gz + dz, depth), gz).start()
    fetch.wait()

    if half == 1:
        stream(True, False)
    else:
        pl.when(level == 0)(lambda: stream(False, False))
        pl.when(middle)(lambda: stream(True, True))
        if half > 2:
            pl.when((level > 0) & jnp.logical_not(middle))(lambda: stream(False, True))

    for c in range(chunks):
        for dz in range(1, depth):
            y_copy(c, dz, lax.rem(gz + dz, depth), gz).wait_send()
        for dx in range(1, nx):
            origin = lax.rem(gx + nx - dx, nx)
            g_copy(c, dx, origin, origin).wait()


def count(mask):
    return jnp.sum(mask.astype(jnp.int32), axis=1)


def pick(value, mask, position, wanted):
    hit = mask[None, :] & (position[None, :] == jnp.arange(wanted, dtype=jnp.int32)[:, None])
    return jnp.sum(jnp.where(hit, value[None, :], 0), axis=1)


def shards(embeds, dest_device, shuffle_key, lengths, gain):
    tiles_here, tile_rows, width = embeds.shape
    nx, ny, depth = lax.axis_size("gx"), lax.axis_size("gy"), lax.axis_size("gz")
    devices = nx * ny * depth
    per_peer = (tiles_here + depth - 1) // depth
    slots = depth * per_peer
    half = ny // 2
    cap = 2 * tiles_here
    if ny % 2 or tile_rows % 128 or width % 512 or slots > tiles_here:
        return direct(embeds, dest_device, shuffle_key, lengths, gain)

    most = half * min(tiles_here, nx * half)
    near_most = max([(e + 1) * min(tiles_here, nx * (ny - 1 - e)) for e in range(half - 1)] + [1])
    back_most = max([(ny - e) * min(tiles_here, nx * e) for e in range(1, half)] + [1])
    classes = sorted({max(near_most, most * part // 16) for part in CLASSES})

    vmem = pl.BlockSpec(memory_space=pltpu.VMEM)
    smem = pl.BlockSpec(memory_space=pltpu.SMEM)
    hbm = pl.BlockSpec(memory_space=pl.ANY)
    lanes = -(-tiles_here // 128) * 128
    table, normed = pl.pallas_call(
        functools.partial(table_kernel, (nx, ny, depth, per_peer)),
        out_shape=(
            jax.ShapeDtypeStruct((devices, 2, lanes), jnp.int32),
            pltpu.HBM((slots, tile_rows, width), jnp.bfloat16),
        ),
        in_specs=[pl.BlockSpec(memory_space=pltpu.HBM)] * 5,
        out_specs=(vmem, pl.BlockSpec(memory_space=pltpu.HBM)),
        scratch_shapes=[
            pltpu.SMEM((1, tiles_here), jnp.int32),
            pltpu.SMEM((1, lengths.shape[0]), jnp.int32),
            pltpu.VMEM((1, tiles_here), jnp.int32),
            pltpu.VMEM((1, tiles_here), jnp.int32),
            pltpu.VMEM((1, width), jnp.float32),
            pltpu.SemaphoreType.DMA((5,)),
            pltpu.VMEM((2, lanes), jnp.int32),
            pltpu.SMEM((slots,), jnp.int32),
            pltpu.SMEM((slots,), jnp.int32),
            pltpu.VMEM((tiles_here, tile_rows, width), jnp.bfloat16),
            pltpu.VMEM((slots, tile_rows, width), jnp.bfloat16),
            pltpu.SemaphoreType.DMA((devices - 1,)),
            pltpu.SemaphoreType.DMA((devices - 1,)),
            pltpu.SemaphoreType.DMA,
            pltpu.SemaphoreType.DMA((slots,)),
        ],
        compiler_params=pltpu.CompilerParams(
            collective_id=0, has_side_effects=True, vmem_limit_bytes=56 * 1024 * 1024
        ),
        name="tables",
    )(dest_device[None, :], shuffle_key[None, :], lengths[None, :], embeds, gain.reshape(1, width))

    gx, gy, gz = lax.axis_index("gx"), lax.axis_index("gy"), lax.axis_index("gz")
    group = gx * ny + gy
    me = group * depth + gz
    dest = table[:, 0, :tiles_here].reshape(-1)
    keys = table[:, 1, :tiles_here].reshape(-1)
    order = jnp.arange(devices * tiles_here, dtype=jnp.int32)
    before = order[None, :] < order[:, None]
    source = order // tiles_here
    from_x, from_y = source // (ny * depth), source // depth % ny
    to_x, to_y, to_z = dest // (ny * depth), dest // depth % ny, dest % depth

    bounds = jnp.arange(ny - 1, dtype=jnp.int32)
    lane = from_x * depth + to_z
    hop_up = (from_y[None, :] <= bounds[:, None]) & (to_y[None, :] > bounds[:, None])
    hop_down = (from_y[None, :] > bounds[:, None]) & (to_y[None, :] <= bounds[:, None])
    hops = jnp.concatenate([hop_up, hop_down])
    in_lane = lane[None, :] == jnp.arange(nx * depth, dtype=jnp.int32)[:, None]
    load = jnp.sum((hops[:, None, :] & in_lane[None, :, :]).astype(jnp.int32), axis=2)

    low = gy < half
    level = jnp.where(low, gy, ny - 1 - gy)
    depth_from = jnp.where(low, from_y, ny - 1 - from_y)
    depth_to = jnp.where(low, to_y, ny - 1 - to_y)
    in_my_lane = (from_x == gx) & (to_z == gz)
    inward = in_my_lane & (depth_from <= level) & (depth_to > level)
    near_in = in_my_lane & (depth_from < level) & (depth_to >= level)
    outward = in_my_lane & (depth_from >= level) & (depth_to < level)
    far_in = in_my_lane & (depth_from > level) & (depth_to <= level)
    landing = in_my_lane & (depth_to == level)
    to_me = dest == me

    same_source = source[:, None] == source[None, :]
    spot = count(before & same_source & (to_z[:, None] == to_z[None, :]))
    at_inward = count(before & inward[None, :])
    at_near = count(before & near_in[None, :])
    at_outward = count(before & outward[None, :])
    at_far = count(before & far_in[None, :])
    at_landing = count(before & (landing[None, :] & (to_x[:, None] == to_x[None, :])))
    at_me = count(before & (to_me[None, :] & (from_x[:, None] == from_x[None, :])))
    rank = count((keys[None, :] < keys[:, None]) & to_me[None, :])
    own_slot = source % depth * per_peer + spot

    over = load.reshape(-1)[None, :] > jnp.array(classes[:-1], jnp.int32)[:, None]
    chosen = jnp.sum(jnp.any(over, axis=1).astype(jnp.int32))
    code = jnp.where(
        depth_from == level,
        own_slot,
        jnp.where(depth_from < level, slots + at_near, slots + near_most + at_far),
    )
    parts = {
        "inward": pick(code, inward, at_inward, most),
        "outward": pick(code, outward, at_outward, back_most),
        "deliver": pick(code, landing, (to_x - gx) % nx * ny + at_landing, nx * ny),
    }
    at, total = {}, 0
    for name, part in parts.items():
        at[name] = total
        total += part.shape[0]
    plan = jnp.pad(jnp.concatenate(list(parts.values())), (0, -total % 128))[None, :]
    which = pick(from_x * ny + at_me + 1, to_me, rank, cap)

    pieces, done = [], 0
    for part in CHUNKS:
        row, column = done // 4 * tile_rows // 16, done % 4 * width // 4
        if part % 4 == 0:
            pieces.append((row, part // 4 * tile_rows // 16, 0, width))
        else:
            pieces.append((row, tile_rows // 16, column, part * width // 4))
        done += part
    pieces = tuple(pieces)
    chunks = len(pieces)

    def branch(index, far):
        def run(plan, normed, chosen_rows, filled):
            near, back = near_most, min(far, back_most)
            counts = ((slots + near,), (far,), (far,), (back,), ((nx - 1) * ny,))
            received = pl.pallas_call(
                functools.partial(
                    line_kernel, (nx, ny, depth, per_peer, pieces, near, far, back, at)
                ),
                out_shape=pltpu.VMEM((nx * ny, tile_rows, width), jnp.bfloat16),
                in_specs=[hbm, pl.BlockSpec(memory_space=pltpu.HBM)],
                out_specs=vmem,
                scratch_shapes=[
                    pltpu.SMEM(plan.shape, jnp.int32),
                    pltpu.SemaphoreType.DMA,
                    pltpu.SemaphoreType.DMA((chunks,)),
                    pltpu.SemaphoreType.DMA((chunks, depth - 1)),
                    pltpu.SemaphoreType.DMA((chunks, depth - 1)),
                    pltpu.SemaphoreType.DMA((chunks,)),
                    pltpu.SemaphoreType.DMA((chunks,)),
                    pltpu.SemaphoreType.DMA((chunks,)),
                    pltpu.SemaphoreType.DMA((chunks,)),
                    pltpu.SemaphoreType.DMA((chunks, nx - 1)),
                    pltpu.SemaphoreType.DMA((chunks, nx - 1)),
                ]
                + [
                    pltpu.VMEM((*lead, rows, columns), jnp.bfloat16)
                    for lead in counts
                    for _, rows, _, columns in pieces
                ],
                compiler_params=pltpu.CompilerParams(
                    collective_id=1 + index, has_side_effects=True, vmem_limit_bytes=44 * 1024 * 1024
                ),
                name=f"line{far}",
            )(plan, normed)
            return pl.pallas_call(
                place_kernel,
                out_shape=pltpu.HBM((cap, tile_rows, width), jnp.bfloat16),
                in_specs=[smem, smem, vmem],
                out_specs=pl.BlockSpec(memory_space=pltpu.HBM),
                scratch_shapes=[
                    pltpu.VMEM((tile_rows, width), jnp.bfloat16),
                    pltpu.SemaphoreType.DMA((cap,)),
                ],
                compiler_params=pltpu.CompilerParams(vmem_limit_bytes=24 * 1024 * 1024),
                name="place",
            )(chosen_rows, filled, received)

        return run

    return lax.switch(
        chosen,
        [branch(i, far) for i, far in enumerate(classes)],
        plan,
        normed,
        jnp.maximum(which - 1, 0),
        (which > 0).astype(jnp.int32),
    )


def solution(mesh):
    return jax.shard_map(
        shards,
        mesh=mesh,
        in_specs=(
            P(("gx", "gy", "gz"), None, None),
            P(("gx", "gy", "gz")),
            P(("gx", "gy", "gz")),
            P(),
            P(),
        ),
        out_specs=P(("gx", "gy", "gz"), None, None),
        check_vma=False,
    )
```

```python
import functools

import jax
import jax.numpy as jnp
from jax import lax
from jax.experimental import pallas as pl
from jax.experimental.pallas import tpu as pltpu
from jax.sharding import PartitionSpec as P

TILES_SEQ = 32
CLASSES = (9, 10, 11, 12, 13, 16)
CHUNKS = (2,) * 32
LATENCY = 11
AHEAD = 1
MESH = pl.DeviceIdType.MESH


def exchange_kernel(
    sizes, small_in, x_ref, gain_ref, recv_ref, keys_ref,
    small_ref, gain, small_sem, first_table, limit_table, note_out, notes, note_table, second, keys_out,
    x_sem, gain_sem, y_send, y_recv, g_send, g_recv, own_sem,
    note_send, note_recv, note_sem, key_send, key_recv, *buffers,
):
    nx, ny, depth, per_peer, chunk_rows = sizes
    chunks = len(chunk_rows)
    starts = [sum(chunk_rows[:c]) for c in range(chunks)]
    groups = nx * ny
    tiles_here, tile_rows, _ = x_ref.shape
    raw, first, arrived, outgoing = (buffers[i * chunks : (i + 1) * chunks] for i in range(4))
    gx, gy, gz = lax.axis_index("gx"), lax.axis_index("gy"), lax.axis_index("gz")
    group = gx * ny + gy
    me = group * depth + gz
    offsets = [(dx, dy) for dy in sorted(range(ny), key=lambda d: abs(d - ny // 2)) for dx in range(nx)]
    offsets.remove((0, 0))

    def load(c):
        return pltpu.make_async_copy(
            x_ref.at[:, pl.ds(starts[c], chunk_rows[c])], raw[c], x_sem.at[c]
        )

    def fill_tables():
        depths = [lax.rem(small_ref[0, i], depth) for i in range(tiles_here)]
        dest_groups = [lax.div(small_ref[0, i], depth) for i in range(tiles_here)]
        places, limits = [], []
        for i in range(tiles_here):
            spot = jnp.int32(0)
            for j in range(i):
                spot = spot + jnp.where(depths[j] == depths[i], 1, 0)
            places.append(depths[i] * per_peer + spot)
            tile = me * tiles_here + i
            length = small_ref[0, 2 * tiles_here + tile // TILES_SEQ]
            limits.append(jnp.maximum(length - tile % TILES_SEQ * tile_rows, 0))
        lane = lax.broadcasted_iota(jnp.int32, note_out.shape[1:], 1)
        for z in range(depth):
            row = jnp.zeros(note_out.shape[1:], jnp.int32)
            for p in range(per_peer):
                slot = z * per_peer + p
                tile, limit, dest_group, key = (jnp.int32(v) for v in (0, 0, -1, 0))
                for i in range(tiles_here):
                    hit = places[i] == slot
                    tile = jnp.where(hit, i, tile)
                    limit = jnp.where(hit, limits[i], limit)
                    dest_group = jnp.where(hit, dest_groups[i], dest_group)
                    key = jnp.where(hit, small_ref[0, tiles_here + i] + 1, key)
                first_table[slot] = tile
                limit_table[slot] = limit
                row = jnp.where(lane == p, dest_group, row)
                row = jnp.where(lane == per_peer + p, key, row)
            note_out[z] = row

    def normed(c, slot):
        rows = chunk_rows[c]
        values = raw[c][first_table[slot]].astype(jnp.float32)
        meansq = jnp.mean(values * values, axis=-1, keepdims=True)
        scaled = values * lax.rsqrt(jnp.maximum(meansq, 0.25)) * gain[...]
        row = starts[c] + lax.broadcasted_iota(jnp.int32, (rows, 1), 0)
        return jnp.where(row < limit_table[slot], scaled, 0.0).astype(jnp.bfloat16)

    def y_copy(c, dz, peer, origin):
        return pltpu.make_async_remote_copy(
            src_ref=first[c].at[dz - 1],
            dst_ref=arrived[c].at[pl.ds(origin * per_peer, per_peer)],
            send_sem=y_send.at[c, dz - 1],
            recv_sem=y_recv.at[c, dz - 1],
            device_id=(gx, gy, peer),
            device_id_type=MESH,
        )

    def peer_of(k):
        dx, dy = offsets[k]
        return lax.rem(gx + dx, nx), lax.rem(gy + dy, ny)

    def g_copy(c, k, px, py, origin):
        return pltpu.make_async_remote_copy(
            src_ref=outgoing[c].at[k],
            dst_ref=recv_ref.at[origin, pl.ds(starts[c], chunk_rows[c])],
            send_sem=g_send.at[c, k],
            recv_sem=g_recv.at[c, k],
            device_id=(px, py, gz),
            device_id_type=MESH,
        )

    def own_copy(c):
        return pltpu.make_async_copy(
            outgoing[c].at[groups - 1],
            recv_ref.at[group, pl.ds(starts[c], chunk_rows[c])],
            own_sem.at[c],
        )

    def note_copy(dz, peer, place):
        return pltpu.make_async_remote_copy(
            src_ref=note_out.at[peer],
            dst_ref=notes.at[place],
            send_sem=note_send.at[dz - 1],
            recv_sem=note_recv.at[dz - 1],
            device_id=(gx, gy, peer),
            device_id_type=MESH,
        )

    def key_copy(k, px, py, place):
        return pltpu.make_async_remote_copy(
            src_ref=keys_out.at[k],
            dst_ref=keys_ref.at[place],
            send_sem=key_send.at[k],
            recv_sem=key_recv.at[k],
            device_id=(px, py, gz),
            device_id_type=MESH,
        )

    def prepare(c):
        load(c).wait()
        for dz in range(1, depth):
            peer = lax.rem(gz + dz, depth)
            for p in range(per_peer):
                first[c][dz - 1, p] = normed(c, peer * per_peer + p)
        for p in range(per_peer):
            arrived[c][gz * per_peer + p] = normed(c, gz * per_peer + p)

    def send_first(c):
        for dz in range(1, depth):
            y_copy(c, dz, lax.rem(gz + dz, depth), gz).start()

    def find_slots():
        for dz in range(1, depth):
            origin = lax.rem(gz + depth - dz, depth)
            note_copy(dz, origin, origin).wait()
        tables = [
            pltpu.make_async_copy(
                notes.at[lax.rem(gz + dz, depth)], note_table.at[lax.rem(gz + dz, depth)], note_sem.at[dz]
            )
            for dz in range(1, depth)
        ]
        tables.append(pltpu.make_async_copy(note_out.at[gz], note_table.at[gz], note_sem.at[0]))
        for copy in tables:
            copy.start()
        for copy in tables:
            copy.wait()

        for k in range(groups):
            px, py = peer_of(k) if k < groups - 1 else (gx, gy)
            wanted = px * ny + py
            slot, key = jnp.int32(0), jnp.int32(0)
            for z in range(depth):
                for p in range(per_peer):
                    hit = note_table[z, 0, p] == wanted
                    slot = jnp.where(hit, z * per_peer + p, slot)
                    key = jnp.where(hit, note_table[z, 0, per_peer + p], key)
            second[k] = slot
            row = jnp.full(keys_out.shape[1:], key, jnp.int32)
            if k < groups - 1:
                keys_out[k] = row
            else:
                keys_ref[group] = row

    def forward(c):
        for dz in range(1, depth):
            origin = lax.rem(gz + depth - dz, depth)
            y_copy(c, dz, origin, origin).wait_recv()
        for k in range(groups):
            outgoing[c][k] = arrived[c][second[k]]
        for k in range(groups - 1):
            px, py = peer_of(k)
            g_copy(c, k, px, py, group).start()
        own_copy(c).start()

    small = [
        pltpu.make_async_copy(small_in, small_ref, small_sem),
        pltpu.make_async_copy(gain_ref, gain, gain_sem),
    ]
    for copy in small:
        copy.start()
    for c in range(chunks):
        load(c).start()
    barrier = pltpu.get_barrier_semaphore()
    for dz in range(1, depth):
        pl.semaphore_signal(
            barrier, inc=1, device_id=(gx, gy, lax.rem(gz + dz, depth)), device_id_type=MESH
        )
    for k in range(groups - 1):
        px, py = peer_of(k)
        pl.semaphore_signal(barrier, inc=1, device_id=(px, py, gz), device_id_type=MESH)
    for copy in small:
        copy.wait()
    fill_tables()
    prepare(0)
    pl.semaphore_wait(barrier, depth - 1 + groups - 1)
    for dz in range(1, depth):
        note_copy(dz, lax.rem(gz + dz, depth), gz).start()
    send_first(0)
    if chunks > 1:
        prepare(1)
        send_first(1)
    find_slots()
    forward(0)
    for k in range(groups - 1):
        px, py = peer_of(k)
        key_copy(k, px, py, group).start()
    for c in range(2, chunks):
        prepare(c)
        send_first(c)
        forward(c - 1)
    if chunks > 1:
        forward(chunks - 1)

    for c in range(chunks):
        for dz in range(1, depth):
            y_copy(c, dz, lax.rem(gz + dz, depth), gz).wait_send()
    sources = []
    for dx, dy in offsets:
        sources.append((lax.rem(gx + nx - dx, nx), lax.rem(gy + ny - dy, ny)))
    for k, (sx, sy) in enumerate(sources):
        key_copy(k, sx, sy, sx * ny + sy).wait()
    for c in range(chunks):
        for k, (sx, sy) in enumerate(sources):
            g_copy(c, k, sx, sy, sx * ny + sy).wait()
        own_copy(c).wait()


def place_kernel(source_ref, filled_ref, blocks_ref, out_ref, zeros, out_sem):
    cap = out_ref.shape[0]

    def store(slot):
        return pltpu.make_async_copy(blocks_ref.at[source_ref[slot]], out_ref.at[slot], out_sem.at[slot])

    for slot in range(cap):
        pl.when(filled_ref[slot] == 1)(lambda slot=slot: store(slot).start())
    zeros[...] = jnp.zeros_like(zeros)
    for slot in range(cap):

        @pl.when(filled_ref[slot] == 0)
        def _():
            pltpu.make_async_copy(zeros, out_ref.at[slot], out_sem.at[slot]).start()

    for slot in range(cap):
        store(slot).wait()


def direct(embeds, dest_device, shuffle_key, lengths, gain):
    tiles_here, tile_rows, width = embeds.shape
    nx, ny, depth = lax.axis_size("gx"), lax.axis_size("gy"), lax.axis_size("gz")
    groups = nx * ny
    per_peer = (tiles_here + depth - 1) // depth
    slots = depth * per_peer
    chunk_rows = (tile_rows,)
    if tile_rows % 128 == 0:
        chunk_rows = tuple(part * tile_rows // 16 for part in (1, 1, 2, 2, 4, 4, 2))
    chunks = len(chunk_rows)

    smem = pl.BlockSpec(memory_space=pltpu.SMEM)
    vmem = pl.BlockSpec(memory_space=pltpu.VMEM)
    hbm = pl.BlockSpec(memory_space=pl.ANY)
    lanes = -(-2 * per_peer // 128) * 128
    small = jnp.concatenate([dest_device, shuffle_key, lengths])
    small = jnp.pad(small, (0, -small.shape[0] % 128))[None, :]
    received, key_rows = pl.pallas_call(
        functools.partial(exchange_kernel, (nx, ny, depth, per_peer, chunk_rows)),
        out_shape=(
            jax.ShapeDtypeStruct((groups, tile_rows, width), jnp.bfloat16),
            jax.ShapeDtypeStruct((groups, 1, 128), jnp.int32),
        ),
        in_specs=[hbm] * 3,
        out_specs=(hbm, vmem),
        scratch_shapes=[
            pltpu.SMEM(small.shape, jnp.int32),
            pltpu.VMEM((1, width), jnp.float32),
            pltpu.SemaphoreType.DMA,
            pltpu.SMEM((slots,), jnp.int32),
            pltpu.SMEM((slots,), jnp.int32),
            pltpu.VMEM((depth, 1, lanes), jnp.int32),
            pltpu.VMEM((depth, 1, lanes), jnp.int32),
            pltpu.SMEM((depth, 1, lanes), jnp.int32),
            pltpu.SMEM((groups,), jnp.int32),
            pltpu.VMEM((groups, 1, 128), jnp.int32),
            pltpu.SemaphoreType.DMA((chunks,)),
            pltpu.SemaphoreType.DMA,
            pltpu.SemaphoreType.DMA((chunks, depth - 1)),
            pltpu.SemaphoreType.DMA((chunks, depth - 1)),
            pltpu.SemaphoreType.DMA((chunks, groups)),
            pltpu.SemaphoreType.DMA((chunks, groups)),
            pltpu.SemaphoreType.DMA((chunks,)),
            pltpu.SemaphoreType.DMA((depth,)),
            pltpu.SemaphoreType.DMA((depth,)),
            pltpu.SemaphoreType.DMA((depth,)),
            pltpu.SemaphoreType.DMA((groups,)),
            pltpu.SemaphoreType.DMA((groups,)),
        ]
        + [pltpu.VMEM((tiles_here, rows, width), jnp.bfloat16) for rows in chunk_rows]
        + [pltpu.VMEM((depth - 1, per_peer, rows, width), jnp.bfloat16) for rows in chunk_rows]
        + [pltpu.VMEM((slots, rows, width), jnp.bfloat16) for rows in chunk_rows]
        + [pltpu.VMEM((groups, rows, width), jnp.bfloat16) for rows in chunk_rows],
        compiler_params=pltpu.CompilerParams(
            collective_id=0, has_side_effects=True, vmem_limit_bytes=36 * 1024 * 1024
        ),
        name="exchange",
    )(small, embeds, gain.reshape(1, width))

    key_of = key_rows[:, 0, 0]
    valid = key_of > 0
    rank = jnp.sum((valid[None, :] & (key_of[None, :] < key_of[:, None])).astype(jnp.int32), axis=1)
    cap = 2 * tiles_here
    at = valid[None, :] & (rank[None, :] == jnp.arange(cap, dtype=jnp.int32)[:, None])
    source = jnp.sum(jnp.where(at, jnp.arange(groups, dtype=jnp.int32)[None, :], 0), axis=1).astype(jnp.int32)
    filled = jnp.sum(at.astype(jnp.int32), axis=1).astype(jnp.int32)

    return pl.pallas_call(
        place_kernel,
        out_shape=jax.ShapeDtypeStruct((cap, tile_rows, width), jnp.bfloat16),
        in_specs=[smem, smem, vmem],
        out_specs=hbm,
        scratch_shapes=[
            pltpu.VMEM((tile_rows, width), jnp.bfloat16),
            pltpu.SemaphoreType.DMA((cap,)),
        ],
        compiler_params=pltpu.CompilerParams(vmem_limit_bytes=24 * 1024 * 1024),
        name="place",
    )(source, filled, received)


def table_kernel(
    sizes, dest_hbm, key_hbm, lengths_hbm, x_ref, gain_hbm, table_ref, normed_ref,
    dest_ref, lengths_ref, dest_row, key_row, gain_ref, small_sem, mine, first_table, limit_table, raw, done, send, recv, x_sem, out_sem,
):
    nx, ny, depth, per_peer = sizes
    devices = nx * ny * depth
    tiles_here, tile_rows, width = x_ref.shape
    slots = depth * per_peer
    block = 16
    me = (lax.axis_index("gx") * ny + lax.axis_index("gy")) * depth + lax.axis_index("gz")

    def place_of(device):
        return lax.div(device, ny * depth), lax.rem(lax.div(device, depth), ny), lax.rem(device, depth)

    def row_copy(step, target, row):
        return pltpu.make_async_remote_copy(
            src_ref=mine,
            dst_ref=table_ref.at[row],
            send_sem=send.at[step - 1],
            recv_sem=recv.at[step - 1],
            device_id=place_of(target),
            device_id_type=MESH,
        )

    def normalize(slot):
        @pl.loop(0, tile_rows // block, unroll=4)
        def _(part):
            start = part * block
            values = raw[first_table[slot], pl.ds(start, block)].astype(jnp.float32)
            meansq = jnp.mean(values * values, axis=-1, keepdims=True)
            scaled = values * lax.rsqrt(jnp.maximum(meansq, 0.25)) * gain_ref[...]
            row = start + lax.broadcasted_iota(jnp.int32, (block, 1), 0)
            done[slot, pl.ds(start, block)] = jnp.where(row < limit_table[slot], scaled, 0.0).astype(jnp.bfloat16)

        pltpu.make_async_copy(done.at[slot], normed_ref.at[slot], out_sem.at[slot]).start()

    small = [
        pltpu.make_async_copy(dest_hbm, dest_row, small_sem.at[0]),
        pltpu.make_async_copy(key_hbm, key_row, small_sem.at[1]),
        pltpu.make_async_copy(dest_hbm, dest_ref, small_sem.at[2]),
        pltpu.make_async_copy(lengths_hbm, lengths_ref, small_sem.at[3]),
        pltpu.make_async_copy(gain_hbm, gain_ref, small_sem.at[4]),
    ]
    load = pltpu.make_async_copy(x_ref, raw, x_sem)
    for copy in small:
        copy.start()
    load.start()
    barrier = pltpu.get_barrier_semaphore()
    for step in range(1, devices):
        pl.semaphore_signal(
            barrier, inc=1, device_id=place_of(lax.rem(me + step, devices)), device_id_type=MESH
        )
    for copy in small:
        copy.wait()
    mine[...] = jnp.zeros_like(mine)
    mine[0:1, 0:tiles_here] = dest_row[...]
    mine[1:2, 0:tiles_here] = key_row[...]
    table_ref[me] = mine[...]

    pl.semaphore_wait(barrier, devices - 1)
    for step in range(1, devices):
        row_copy(step, lax.rem(me + step, devices), me).start()
    depths = [lax.rem(dest_ref[0, i], depth) for i in range(tiles_here)]
    places, limits = [], []
    for i in range(tiles_here):
        spot = jnp.int32(0)
        for j in range(i):
            spot = spot + jnp.where(depths[j] == depths[i], 1, 0)
        places.append(depths[i] * per_peer + spot)
        tile = me * tiles_here + i
        limits.append(jnp.maximum(lengths_ref[0, tile // TILES_SEQ] - tile % TILES_SEQ * tile_rows, 0))
    for slot in range(slots):
        tile, limit = jnp.int32(0), jnp.int32(0)
        for i in range(tiles_here):
            tile = jnp.where(places[i] == slot, i, tile)
            limit = jnp.where(places[i] == slot, limits[i], limit)
        first_table[slot] = tile
        limit_table[slot] = limit

    load.wait()
    for slot in range(slots):
        normalize(slot)
    for step in range(1, devices):
        source = lax.rem(me + devices - step, devices)
        row_copy(step, source, source).wait()
    for slot in range(slots):
        pltpu.make_async_copy(done.at[slot], normed_ref.at[slot], out_sem.at[slot]).wait()


def line_kernel(
    sizes, plan_ref, x_ref, received,
    plan, plan_sem, x_sem, y_send, y_recv, a_send, a_recv, b_send, b_recv,
    g_send, g_recv, *buffers,
):
    nx, ny, depth, per_peer, pieces, near, far, back, at = sizes
    chunks = len(pieces)
    half = ny // 2
    slots = depth * per_peer
    pool, inflow, inward, outward, outgoing = (
        buffers[i * chunks : (i + 1) * chunks] for i in range(5)
    )
    gx, gy, gz = lax.axis_index("gx"), lax.axis_index("gy"), lax.axis_index("gz")
    low = gy < half
    level = jnp.where(low, gy, ny - 1 - gy)
    inner = jnp.where(low, gy + 1, gy - 1)
    outer = jnp.clip(jnp.where(low, gy - 1, gy + 1), 0, ny - 1)
    middle = level == half - 1

    def piece(ref, start, size, c):
        row, rows, column, columns = pieces[c]
        return ref.at[pl.ds(start, size), pl.ds(row, rows), pl.ds(column, columns)]

    def load(c):
        return pltpu.make_async_copy(
            piece(x_ref, gz * per_peer, per_peer, c),
            pool[c].at[pl.ds(gz * per_peer, per_peer)],
            x_sem.at[c],
        )

    def y_copy(c, dz, peer, origin):
        return pltpu.make_async_remote_copy(
            src_ref=piece(x_ref, peer * per_peer, per_peer, c),
            dst_ref=pool[c].at[pl.ds(origin * per_peer, per_peer)],
            send_sem=y_send.at[c, dz - 1],
            recv_sem=y_recv.at[c, dz - 1],
            device_id=(gx, gy, peer),
            device_id_type=MESH,
        )

    def near_copy(c, peer):
        return pltpu.make_async_remote_copy(
            src_ref=inward[c].at[pl.ds(0, near)],
            dst_ref=pool[c].at[pl.ds(slots, near)],
            send_sem=a_send.at[c],
            recv_sem=a_recv.at[c],
            device_id=(gx, peer, gz),
            device_id_type=MESH,
        )

    def cross_copy(c, peer):
        return pltpu.make_async_remote_copy(
            src_ref=inward[c],
            dst_ref=inflow[c],
            send_sem=a_send.at[c],
            recv_sem=b_recv.at[c],
            device_id=(gx, peer, gz),
            device_id_type=MESH,
        )

    def back_copy(c, peer):
        return pltpu.make_async_remote_copy(
            src_ref=outward[c],
            dst_ref=inflow[c].at[pl.ds(0, back)],
            send_sem=b_send.at[c],
            recv_sem=b_recv.at[c],
            device_id=(gx, peer, gz),
            device_id_type=MESH,
        )

    def g_copy(c, dx, peer, origin):
        return pltpu.make_async_remote_copy(
            src_ref=outgoing[c].at[pl.ds((dx - 1) * ny, ny)],
            dst_ref=piece(received, origin * ny, ny, c),
            send_sem=g_send.at[c, dx - 1],
            recv_sem=g_recv.at[c, dx - 1],
            device_id=(peer, gy, gz),
            device_id_type=MESH,
        )

    def either(c, code):
        held = pool[c][jnp.minimum(code, slots + near - 1)]
        came = inflow[c][jnp.clip(code - slots - near, 0, far - 1)]
        return jnp.where(code < slots + near, held, came)

    def send_inward(c, crosses, relays):
        load(c).wait()
        for dz in range(1, depth):
            origin = lax.rem(gz + depth - dz, depth)
            y_copy(c, dz, origin, origin).wait_recv()
        if relays:
            near_copy(c, outer).wait_recv()

        @pl.loop(0, far if crosses else near)
        def _(p):
            inward[c][p] = pool[c][plan[0, at["inward"] + p]]

        if crosses:
            cross_copy(c, inner).start()
        else:
            near_copy(c, inner).start()

    def deliver(c, crosses, relays):
        if crosses:
            cross_copy(c, inner).wait_recv()
        else:
            back_copy(c, inner).wait_recv()
        if relays:

            @pl.loop(0, back)
            def _(p):
                outward[c][p] = either(c, plan[0, at["outward"] + p])

            back_copy(c, outer).start()

        @pl.loop(0, (nx - 1) * ny)
        def _(k):
            outgoing[c][k] = either(c, plan[0, at["deliver"] + ny + k])

        for dx in range(1, nx):
            g_copy(c, dx, lax.rem(gx + dx, nx), gx).start()

        @pl.loop(0, ny)
        def _(k):
            row, rows, column, columns = pieces[c]
            received[gx * ny + k, pl.ds(row, rows), pl.ds(column, columns)] = either(
                c, plan[0, at["deliver"] + k]
            )

    def stream(crosses, relays):
        area = [rows * columns / (pieces[-1][0] + pieces[-1][1]) for _, rows, _, columns in pieces]
        area = [a * 16 / sum(area) for a in area]
        events = []
        for c in range(chunks):
            upto = sum(area[: c + 1])
            sent = near * (upto - area[c])
            landed = near * area[0] + far * (upto + area[c]) + LATENCY
            if crosses or relays:
                sent, landed = c, c + AHEAD + 0.5
            events.append((sent, 0, c))
            events.append((landed, 1, c))
        for _, kind, c in sorted(events):
            if kind == 0:
                send_inward(c, crosses, relays)
            else:
                deliver(c, crosses, relays)
        for c in range(chunks):
            if crosses:
                cross_copy(c, inner).wait_send()
            else:
                near_copy(c, inner).wait_send()
            if relays:
                back_copy(c, outer).wait_send()

    fetch = pltpu.make_async_copy(plan_ref, plan, plan_sem)
    fetch.start()
    for c in range(chunks):
        load(c).start()
    barrier = pltpu.get_barrier_semaphore()
    for dz in range(1, depth):
        pl.semaphore_signal(
            barrier, inc=1, device_id=(gx, gy, lax.rem(gz + dz, depth)), device_id_type=MESH
        )
    for dx in range(1, nx):
        pl.semaphore_signal(
            barrier, inc=1, device_id=(lax.rem(gx + dx, nx), gy, gz), device_id_type=MESH
        )
    pl.semaphore_signal(barrier, inc=1, device_id=(gx, inner, gz), device_id_type=MESH)

    @pl.when(level > 0)
    def _():
        pl.semaphore_signal(barrier, inc=1, device_id=(gx, outer, gz), device_id_type=MESH)

    pl.semaphore_wait(barrier, depth - 1 + nx - 1 + 1 + jnp.where(level > 0, 1, 0))
    for c in range(chunks):
        for dz in range(1, depth):
            y_copy(c, dz, lax.rem(gz + dz, depth), gz).start()
    fetch.wait()

    if half == 1:
        stream(True, False)
    else:
        pl.when(level == 0)(lambda: stream(False, False))
        pl.when(middle)(lambda: stream(True, True))
        if half > 2:
            pl.when((level > 0) & jnp.logical_not(middle))(lambda: stream(False, True))

    for c in range(chunks):
        for dz in range(1, depth):
            y_copy(c, dz, lax.rem(gz + dz, depth), gz).wait_send()
        for dx in range(1, nx):
            origin = lax.rem(gx + nx - dx, nx)
            g_copy(c, dx, origin, origin).wait()


def count(mask):
    return jnp.sum(mask.astype(jnp.int32), axis=1)


def pick(value, mask, position, wanted):
    hit = mask[None, :] & (position[None, :] == jnp.arange(wanted, dtype=jnp.int32)[:, None])
    return jnp.sum(jnp.where(hit, value[None, :], 0), axis=1)


def shards(embeds, dest_device, shuffle_key, lengths, gain):
    tiles_here, tile_rows, width = embeds.shape
    nx, ny, depth = lax.axis_size("gx"), lax.axis_size("gy"), lax.axis_size("gz")
    devices = nx * ny * depth
    per_peer = (tiles_here + depth - 1) // depth
    slots = depth * per_peer
    half = ny // 2
    cap = 2 * tiles_here
    if ny % 2 or tile_rows % 128 or width % 512 or slots > tiles_here:
        return direct(embeds, dest_device, shuffle_key, lengths, gain)

    most = half * min(tiles_here, nx * half)
    near_most = max([(e + 1) * min(tiles_here, nx * (ny - 1 - e)) for e in range(half - 1)] + [1])
    back_most = max([(ny - e) * min(tiles_here, nx * e) for e in range(1, half)] + [1])
    classes = sorted({max(near_most, most * part // 16) for part in CLASSES})

    vmem = pl.BlockSpec(memory_space=pltpu.VMEM)
    smem = pl.BlockSpec(memory_space=pltpu.SMEM)
    hbm = pl.BlockSpec(memory_space=pl.ANY)
    lanes = -(-tiles_here // 128) * 128
    table, normed = pl.pallas_call(
        functools.partial(table_kernel, (nx, ny, depth, per_peer)),
        out_shape=(
            jax.ShapeDtypeStruct((devices, 2, lanes), jnp.int32),
            pltpu.HBM((slots, tile_rows, width), jnp.bfloat16),
        ),
        in_specs=[pl.BlockSpec(memory_space=pltpu.HBM)] * 5,
        out_specs=(vmem, pl.BlockSpec(memory_space=pltpu.HBM)),
        scratch_shapes=[
            pltpu.SMEM((1, tiles_here), jnp.int32),
            pltpu.SMEM((1, lengths.shape[0]), jnp.int32),
            pltpu.VMEM((1, tiles_here), jnp.int32),
            pltpu.VMEM((1, tiles_here), jnp.int32),
            pltpu.VMEM((1, width), jnp.float32),
            pltpu.SemaphoreType.DMA((5,)),
            pltpu.VMEM((2, lanes), jnp.int32),
            pltpu.SMEM((slots,), jnp.int32),
            pltpu.SMEM((slots,), jnp.int32),
            pltpu.VMEM((tiles_here, tile_rows, width), jnp.bfloat16),
            pltpu.VMEM((slots, tile_rows, width), jnp.bfloat16),
            pltpu.SemaphoreType.DMA((devices - 1,)),
            pltpu.SemaphoreType.DMA((devices - 1,)),
            pltpu.SemaphoreType.DMA,
            pltpu.SemaphoreType.DMA((slots,)),
        ],
        compiler_params=pltpu.CompilerParams(
            collective_id=0, has_side_effects=True, vmem_limit_bytes=56 * 1024 * 1024
        ),
        name="tables",
    )(dest_device[None, :], shuffle_key[None, :], lengths[None, :], embeds, gain.reshape(1, width))

    gx, gy, gz = lax.axis_index("gx"), lax.axis_index("gy"), lax.axis_index("gz")
    group = gx * ny + gy
    me = group * depth + gz
    dest = table[:, 0, :tiles_here].reshape(-1)
    keys = table[:, 1, :tiles_here].reshape(-1)
    order = jnp.arange(devices * tiles_here, dtype=jnp.int32)
    before = order[None, :] < order[:, None]
    source = order // tiles_here
    from_x, from_y = source // (ny * depth), source // depth % ny
    to_x, to_y, to_z = dest // (ny * depth), dest // depth % ny, dest % depth

    bounds = jnp.arange(ny - 1, dtype=jnp.int32)
    lane = from_x * depth + to_z
    hop_up = (from_y[None, :] <= bounds[:, None]) & (to_y[None, :] > bounds[:, None])
    hop_down = (from_y[None, :] > bounds[:, None]) & (to_y[None, :] <= bounds[:, None])
    hops = jnp.concatenate([hop_up, hop_down])
    in_lane = lane[None, :] == jnp.arange(nx * depth, dtype=jnp.int32)[:, None]
    load = jnp.sum((hops[:, None, :] & in_lane[None, :, :]).astype(jnp.int32), axis=2)

    low = gy < half
    level = jnp.where(low, gy, ny - 1 - gy)
    depth_from = jnp.where(low, from_y, ny - 1 - from_y)
    depth_to = jnp.where(low, to_y, ny - 1 - to_y)
    in_my_lane = (from_x == gx) & (to_z == gz)
    inward = in_my_lane & (depth_from <= level) & (depth_to > level)
    near_in = in_my_lane & (depth_from < level) & (depth_to >= level)
    outward = in_my_lane & (depth_from >= level) & (depth_to < level)
    far_in = in_my_lane & (depth_from > level) & (depth_to <= level)
    landing = in_my_lane & (depth_to == level)
    to_me = dest == me

    same_source = source[:, None] == source[None, :]
    spot = count(before & same_source & (to_z[:, None] == to_z[None, :]))
    at_inward = count(before & inward[None, :])
    at_near = count(before & near_in[None, :])
    at_outward = count(before & outward[None, :])
    at_far = count(before & far_in[None, :])
    at_landing = count(before & (landing[None, :] & (to_x[:, None] == to_x[None, :])))
    at_me = count(before & (to_me[None, :] & (from_x[:, None] == from_x[None, :])))
    rank = count((keys[None, :] < keys[:, None]) & to_me[None, :])
    own_slot = source % depth * per_peer + spot

    over = load.reshape(-1)[None, :] > jnp.array(classes[:-1], jnp.int32)[:, None]
    chosen = jnp.sum(jnp.any(over, axis=1).astype(jnp.int32))
    code = jnp.where(
        depth_from == level,
        own_slot,
        jnp.where(depth_from < level, slots + at_near, slots + near_most + at_far),
    )
    parts = {
        "inward": pick(code, inward, at_inward, most),
        "outward": pick(code, outward, at_outward, back_most),
        "deliver": pick(code, landing, (to_x - gx) % nx * ny + at_landing, nx * ny),
    }
    at, total = {}, 0
    for name, part in parts.items():
        at[name] = total
        total += part.shape[0]
    plan = jnp.pad(jnp.concatenate(list(parts.values())), (0, -total % 128))[None, :]
    which = pick(from_x * ny + at_me + 1, to_me, rank, cap)

    pieces, done = [], 0
    for part in CHUNKS:
        row, column = done // 4 * tile_rows // 16, done % 4 * width // 4
        if part % 4 == 0:
            pieces.append((row, part // 4 * tile_rows // 16, 0, width))
        else:
            pieces.append((row, tile_rows // 16, column, part * width // 4))
        done += part
    pieces = tuple(pieces)
    chunks = len(pieces)

    def branch(index, far):
        def run(plan, normed, chosen_rows, filled):
            near, back = near_most, min(far, back_most)
            counts = ((slots + near,), (far,), (far,), (back,), ((nx - 1) * ny,))
            received = pl.pallas_call(
                functools.partial(
                    line_kernel, (nx, ny, depth, per_peer, pieces, near, far, back, at)
                ),
                out_shape=pltpu.VMEM((nx * ny, tile_rows, width), jnp.bfloat16),
                in_specs=[hbm, pl.BlockSpec(memory_space=pltpu.HBM)],
                out_specs=vmem,
                scratch_shapes=[
                    pltpu.SMEM(plan.shape, jnp.int32),
                    pltpu.SemaphoreType.DMA,
                    pltpu.SemaphoreType.DMA((chunks,)),
                    pltpu.SemaphoreType.DMA((chunks, depth - 1)),
                    pltpu.SemaphoreType.DMA((chunks, depth - 1)),
                    pltpu.SemaphoreType.DMA((chunks,)),
                    pltpu.SemaphoreType.DMA((chunks,)),
                    pltpu.SemaphoreType.DMA((chunks,)),
                    pltpu.SemaphoreType.DMA((chunks,)),
                    pltpu.SemaphoreType.DMA((chunks, nx - 1)),
                    pltpu.SemaphoreType.DMA((chunks, nx - 1)),
                ]
                + [
                    pltpu.VMEM((*lead, rows, columns), jnp.bfloat16)
                    for lead in counts
                    for _, rows, _, columns in pieces
                ],
                compiler_params=pltpu.CompilerParams(
                    collective_id=1 + index, has_side_effects=True, vmem_limit_bytes=44 * 1024 * 1024
                ),
                name=f"line{far}",
            )(plan, normed)
            return pl.pallas_call(
                place_kernel,
                out_shape=pltpu.HBM((cap, tile_rows, width), jnp.bfloat16),
                in_specs=[smem, smem, vmem],
                out_specs=pl.BlockSpec(memory_space=pltpu.HBM),
                scratch_shapes=[
                    pltpu.VMEM((tile_rows, width), jnp.bfloat16),
                    pltpu.SemaphoreType.DMA((cap,)),
                ],
                compiler_params=pltpu.CompilerParams(vmem_limit_bytes=24 * 1024 * 1024),
                name="place",
            )(chosen_rows, filled, received)

        return run

    return lax.switch(
        chosen,
        [branch(i, far) for i, far in enumerate(classes)],
        plan,
        normed,
        jnp.maximum(which - 1, 0),
        (which > 0).astype(jnp.int32),
    )


def solution(mesh):
    return jax.shard_map(
        shards,
        mesh=mesh,
        in_specs=(
            P(("gx", "gy", "gz"), None, None),
            P(("gx", "gy", "gz")),
            P(("gx", "gy", "gz")),
            P(),
            P(),
        ),
        out_specs=P(("gx", "gy", "gz"), None, None),
        check_vma=False,
    )
```

```python
import functools

import jax
import jax.numpy as jnp
from jax import lax
from jax.experimental import pallas as pl
from jax.experimental.pallas import tpu as pltpu
from jax.sharding import PartitionSpec as P

TILES_SEQ = 32
CLASSES = (9, 10, 11, 12, 13, 16)
CHUNKS = (2,) * 32
LATENCY = 11
AHEAD = 1
MESH = pl.DeviceIdType.MESH


def exchange_kernel(
    sizes, small_in, x_ref, gain_ref, recv_ref, keys_ref,
    small_ref, gain, small_sem, first_table, limit_table, note_out, notes, note_table, second, keys_out,
    x_sem, gain_sem, y_send, y_recv, g_send, g_recv, own_sem,
    note_send, note_recv, note_sem, key_send, key_recv, *buffers,
):
    nx, ny, depth, per_peer, chunk_rows = sizes
    chunks = len(chunk_rows)
    starts = [sum(chunk_rows[:c]) for c in range(chunks)]
    groups = nx * ny
    tiles_here, tile_rows, _ = x_ref.shape
    raw, first, arrived, outgoing = (buffers[i * chunks : (i + 1) * chunks] for i in range(4))
    gx, gy, gz = lax.axis_index("gx"), lax.axis_index("gy"), lax.axis_index("gz")
    group = gx * ny + gy
    me = group * depth + gz
    offsets = [(dx, dy) for dy in sorted(range(ny), key=lambda d: abs(d - ny // 2)) for dx in range(nx)]
    offsets.remove((0, 0))

    def load(c):
        return pltpu.make_async_copy(
            x_ref.at[:, pl.ds(starts[c], chunk_rows[c])], raw[c], x_sem.at[c]
        )

    def fill_tables():
        depths = [lax.rem(small_ref[0, i], depth) for i in range(tiles_here)]
        dest_groups = [lax.div(small_ref[0, i], depth) for i in range(tiles_here)]
        places, limits = [], []
        for i in range(tiles_here):
            spot = jnp.int32(0)
            for j in range(i):
                spot = spot + jnp.where(depths[j] == depths[i], 1, 0)
            places.append(depths[i] * per_peer + spot)
            tile = me * tiles_here + i
            length = small_ref[0, 2 * tiles_here + tile // TILES_SEQ]
            limits.append(jnp.maximum(length - tile % TILES_SEQ * tile_rows, 0))
        lane = lax.broadcasted_iota(jnp.int32, note_out.shape[1:], 1)
        for z in range(depth):
            row = jnp.zeros(note_out.shape[1:], jnp.int32)
            for p in range(per_peer):
                slot = z * per_peer + p
                tile, limit, dest_group, key = (jnp.int32(v) for v in (0, 0, -1, 0))
                for i in range(tiles_here):
                    hit = places[i] == slot
                    tile = jnp.where(hit, i, tile)
                    limit = jnp.where(hit, limits[i], limit)
                    dest_group = jnp.where(hit, dest_groups[i], dest_group)
                    key = jnp.where(hit, small_ref[0, tiles_here + i] + 1, key)
                first_table[slot] = tile
                limit_table[slot] = limit
                row = jnp.where(lane == p, dest_group, row)
                row = jnp.where(lane == per_peer + p, key, row)
            note_out[z] = row

    def normed(c, slot):
        rows = chunk_rows[c]
        values = raw[c][first_table[slot]].astype(jnp.float32)
        meansq = jnp.mean(values * values, axis=-1, keepdims=True)
        scaled = values * lax.rsqrt(jnp.maximum(meansq, 0.25)) * gain[...]
        row = starts[c] + lax.broadcasted_iota(jnp.int32, (rows, 1), 0)
        return jnp.where(row < limit_table[slot], scaled, 0.0).astype(jnp.bfloat16)

    def y_copy(c, dz, peer, origin):
        return pltpu.make_async_remote_copy(
            src_ref=first[c].at[dz - 1],
            dst_ref=arrived[c].at[pl.ds(origin * per_peer, per_peer)],
            send_sem=y_send.at[c, dz - 1],
            recv_sem=y_recv.at[c, dz - 1],
            device_id=(gx, gy, peer),
            device_id_type=MESH,
        )

    def peer_of(k):
        dx, dy = offsets[k]
        return lax.rem(gx + dx, nx), lax.rem(gy + dy, ny)

    def g_copy(c, k, px, py, origin):
        return pltpu.make_async_remote_copy(
            src_ref=outgoing[c].at[k],
            dst_ref=recv_ref.at[origin, pl.ds(starts[c], chunk_rows[c])],
            send_sem=g_send.at[c, k],
            recv_sem=g_recv.at[c, k],
            device_id=(px, py, gz),
            device_id_type=MESH,
        )

    def own_copy(c):
        return pltpu.make_async_copy(
            outgoing[c].at[groups - 1],
            recv_ref.at[group, pl.ds(starts[c], chunk_rows[c])],
            own_sem.at[c],
        )

    def note_copy(dz, peer, place):
        return pltpu.make_async_remote_copy(
            src_ref=note_out.at[peer],
            dst_ref=notes.at[place],
            send_sem=note_send.at[dz - 1],
            recv_sem=note_recv.at[dz - 1],
            device_id=(gx, gy, peer),
            device_id_type=MESH,
        )

    def key_copy(k, px, py, place):
        return pltpu.make_async_remote_copy(
            src_ref=keys_out.at[k],
            dst_ref=keys_ref.at[place],
            send_sem=key_send.at[k],
            recv_sem=key_recv.at[k],
            device_id=(px, py, gz),
            device_id_type=MESH,
        )

    def prepare(c):
        load(c).wait()
        for dz in range(1, depth):
            peer = lax.rem(gz + dz, depth)
            for p in range(per_peer):
                first[c][dz - 1, p] = normed(c, peer * per_peer + p)
        for p in range(per_peer):
            arrived[c][gz * per_peer + p] = normed(c, gz * per_peer + p)

    def send_first(c):
        for dz in range(1, depth):
            y_copy(c, dz, lax.rem(gz + dz, depth), gz).start()

    def find_slots():
        for dz in range(1, depth):
            origin = lax.rem(gz + depth - dz, depth)
            note_copy(dz, origin, origin).wait()
        tables = [
            pltpu.make_async_copy(
                notes.at[lax.rem(gz + dz, depth)], note_table.at[lax.rem(gz + dz, depth)], note_sem.at[dz]
            )
            for dz in range(1, depth)
        ]
        tables.append(pltpu.make_async_copy(note_out.at[gz], note_table.at[gz], note_sem.at[0]))
        for copy in tables:
            copy.start()
        for copy in tables:
            copy.wait()

        for k in range(groups):
            px, py = peer_of(k) if k < groups - 1 else (gx, gy)
            wanted = px * ny + py
            slot, key = jnp.int32(0), jnp.int32(0)
            for z in range(depth):
                for p in range(per_peer):
                    hit = note_table[z, 0, p] == wanted
                    slot = jnp.where(hit, z * per_peer + p, slot)
                    key = jnp.where(hit, note_table[z, 0, per_peer + p], key)
            second[k] = slot
            row = jnp.full(keys_out.shape[1:], key, jnp.int32)
            if k < groups - 1:
                keys_out[k] = row
            else:
                keys_ref[group] = row

    def forward(c):
        for dz in range(1, depth):
            origin = lax.rem(gz + depth - dz, depth)
            y_copy(c, dz, origin, origin).wait_recv()
        for k in range(groups):
            outgoing[c][k] = arrived[c][second[k]]
        for k in range(groups - 1):
            px, py = peer_of(k)
            g_copy(c, k, px, py, group).start()
        own_copy(c).start()

    small = [
        pltpu.make_async_copy(small_in, small_ref, small_sem),
        pltpu.make_async_copy(gain_ref, gain, gain_sem),
    ]
    for copy in small:
        copy.start()
    for c in range(chunks):
        load(c).start()
    barrier = pltpu.get_barrier_semaphore()
    for dz in range(1, depth):
        pl.semaphore_signal(
            barrier, inc=1, device_id=(gx, gy, lax.rem(gz + dz, depth)), device_id_type=MESH
        )
    for k in range(groups - 1):
        px, py = peer_of(k)
        pl.semaphore_signal(barrier, inc=1, device_id=(px, py, gz), device_id_type=MESH)
    for copy in small:
        copy.wait()
    fill_tables()
    prepare(0)
    pl.semaphore_wait(barrier, depth - 1 + groups - 1)
    for dz in range(1, depth):
        note_copy(dz, lax.rem(gz + dz, depth), gz).start()
    send_first(0)
    if chunks > 1:
        prepare(1)
        send_first(1)
    find_slots()
    forward(0)
    for k in range(groups - 1):
        px, py = peer_of(k)
        key_copy(k, px, py, group).start()
    for c in range(2, chunks):
        prepare(c)
        send_first(c)
        forward(c - 1)
    if chunks > 1:
        forward(chunks - 1)

    for c in range(chunks):
        for dz in range(1, depth):
            y_copy(c, dz, lax.rem(gz + dz, depth), gz).wait_send()
    sources = []
    for dx, dy in offsets:
        sources.append((lax.rem(gx + nx - dx, nx), lax.rem(gy + ny - dy, ny)))
    for k, (sx, sy) in enumerate(sources):
        key_copy(k, sx, sy, sx * ny + sy).wait()
    for c in range(chunks):
        for k, (sx, sy) in enumerate(sources):
            g_copy(c, k, sx, sy, sx * ny + sy).wait()
        own_copy(c).wait()


def place_kernel(source_ref, filled_ref, blocks_ref, out_ref, zeros, out_sem):
    cap = out_ref.shape[0]

    def store(slot):
        return pltpu.make_async_copy(blocks_ref.at[source_ref[slot]], out_ref.at[slot], out_sem.at[slot])

    for slot in range(cap):
        pl.when(filled_ref[slot] == 1)(lambda slot=slot: store(slot).start())
    zeros[...] = jnp.zeros_like(zeros)
    for slot in range(cap):

        @pl.when(filled_ref[slot] == 0)
        def _():
            pltpu.make_async_copy(zeros, out_ref.at[slot], out_sem.at[slot]).start()

    for slot in range(cap):
        store(slot).wait()


def direct(embeds, dest_device, shuffle_key, lengths, gain):
    tiles_here, tile_rows, width = embeds.shape
    nx, ny, depth = lax.axis_size("gx"), lax.axis_size("gy"), lax.axis_size("gz")
    groups = nx * ny
    per_peer = (tiles_here + depth - 1) // depth
    slots = depth * per_peer
    chunk_rows = (tile_rows,)
    if tile_rows % 128 == 0:
        chunk_rows = tuple(part * tile_rows // 16 for part in (1, 1, 2, 2, 4, 4, 2))
    chunks = len(chunk_rows)

    smem = pl.BlockSpec(memory_space=pltpu.SMEM)
    vmem = pl.BlockSpec(memory_space=pltpu.VMEM)
    hbm = pl.BlockSpec(memory_space=pl.ANY)
    lanes = -(-2 * per_peer // 128) * 128
    small = jnp.concatenate([dest_device, shuffle_key, lengths])
    small = jnp.pad(small, (0, -small.shape[0] % 128))[None, :]
    received, key_rows = pl.pallas_call(
        functools.partial(exchange_kernel, (nx, ny, depth, per_peer, chunk_rows)),
        out_shape=(
            jax.ShapeDtypeStruct((groups, tile_rows, width), jnp.bfloat16),
            jax.ShapeDtypeStruct((groups, 1, 128), jnp.int32),
        ),
        in_specs=[hbm] * 3,
        out_specs=(hbm, vmem),
        scratch_shapes=[
            pltpu.SMEM(small.shape, jnp.int32),
            pltpu.VMEM((1, width), jnp.float32),
            pltpu.SemaphoreType.DMA,
            pltpu.SMEM((slots,), jnp.int32),
            pltpu.SMEM((slots,), jnp.int32),
            pltpu.VMEM((depth, 1, lanes), jnp.int32),
            pltpu.VMEM((depth, 1, lanes), jnp.int32),
            pltpu.SMEM((depth, 1, lanes), jnp.int32),
            pltpu.SMEM((groups,), jnp.int32),
            pltpu.VMEM((groups, 1, 128), jnp.int32),
            pltpu.SemaphoreType.DMA((chunks,)),
            pltpu.SemaphoreType.DMA,
            pltpu.SemaphoreType.DMA((chunks, depth - 1)),
            pltpu.SemaphoreType.DMA((chunks, depth - 1)),
            pltpu.SemaphoreType.DMA((chunks, groups)),
            pltpu.SemaphoreType.DMA((chunks, groups)),
            pltpu.SemaphoreType.DMA((chunks,)),
            pltpu.SemaphoreType.DMA((depth,)),
            pltpu.SemaphoreType.DMA((depth,)),
            pltpu.SemaphoreType.DMA((depth,)),
            pltpu.SemaphoreType.DMA((groups,)),
            pltpu.SemaphoreType.DMA((groups,)),
        ]
        + [pltpu.VMEM((tiles_here, rows, width), jnp.bfloat16) for rows in chunk_rows]
        + [pltpu.VMEM((depth - 1, per_peer, rows, width), jnp.bfloat16) for rows in chunk_rows]
        + [pltpu.VMEM((slots, rows, width), jnp.bfloat16) for rows in chunk_rows]
        + [pltpu.VMEM((groups, rows, width), jnp.bfloat16) for rows in chunk_rows],
        compiler_params=pltpu.CompilerParams(
            collective_id=0, has_side_effects=True, vmem_limit_bytes=36 * 1024 * 1024
        ),
        name="exchange",
    )(small, embeds, gain.reshape(1, width))

    key_of = key_rows[:, 0, 0]
    valid = key_of > 0
    rank = jnp.sum((valid[None, :] & (key_of[None, :] < key_of[:, None])).astype(jnp.int32), axis=1)
    cap = 2 * tiles_here
    at = valid[None, :] & (rank[None, :] == jnp.arange(cap, dtype=jnp.int32)[:, None])
    source = jnp.sum(jnp.where(at, jnp.arange(groups, dtype=jnp.int32)[None, :], 0), axis=1).astype(jnp.int32)
    filled = jnp.sum(at.astype(jnp.int32), axis=1).astype(jnp.int32)

    return pl.pallas_call(
        place_kernel,
        out_shape=jax.ShapeDtypeStruct((cap, tile_rows, width), jnp.bfloat16),
        in_specs=[smem, smem, vmem],
        out_specs=hbm,
        scratch_shapes=[
            pltpu.VMEM((tile_rows, width), jnp.bfloat16),
            pltpu.SemaphoreType.DMA((cap,)),
        ],
        compiler_params=pltpu.CompilerParams(vmem_limit_bytes=24 * 1024 * 1024),
        name="place",
    )(source, filled, received)


def table_kernel(
    sizes, dest_hbm, key_hbm, lengths_hbm, x_ref, gain_hbm, table_ref, normed_ref, early_ref,
    dest_ref, lengths_ref, dest_row, key_row, gain_ref, small_sem, mine, first_table, limit_table, raw, done, send, recv, x_sem, out_sem, y_send, y_recv,
):
    nx, ny, depth, per_peer = sizes
    devices = nx * ny * depth
    tiles_here, tile_rows, width = x_ref.shape
    slots = depth * per_peer
    block = 16
    me = (lax.axis_index("gx") * ny + lax.axis_index("gy")) * depth + lax.axis_index("gz")

    def place_of(device):
        return lax.div(device, ny * depth), lax.rem(lax.div(device, depth), ny), lax.rem(device, depth)

    def row_copy(step, target, row):
        return pltpu.make_async_remote_copy(
            src_ref=mine,
            dst_ref=table_ref.at[row],
            send_sem=send.at[step - 1],
            recv_sem=recv.at[step - 1],
            device_id=place_of(target),
            device_id_type=MESH,
        )

    gx, gy, gz = lax.axis_index("gx"), lax.axis_index("gy"), lax.axis_index("gz")

    def early_copy(dz, peer, origin):
        return pltpu.make_async_remote_copy(
            src_ref=done.at[pl.ds(peer * per_peer, per_peer), pl.ds(0, early_ref.shape[1])],
            dst_ref=early_ref.at[pl.ds(origin * per_peer, per_peer)],
            send_sem=y_send.at[dz - 1],
            recv_sem=y_recv.at[dz - 1],
            device_id=(gx, gy, peer),
            device_id_type=MESH,
        )

    def store(part):
        rows = pl.ds(part * block, block)
        return pltpu.make_async_copy(done.at[:, rows], normed_ref.at[:, rows], out_sem.at[part])

    def normalize(part):
        start = part * block

        @pl.loop(0, slots, unroll=4)
        def _(slot):
            values = raw[first_table[slot], pl.ds(start, block)].astype(jnp.float32)
            meansq = jnp.mean(values * values, axis=-1, keepdims=True)
            scaled = values * lax.rsqrt(jnp.maximum(meansq, 0.25)) * gain_ref[...]
            row = start + lax.broadcasted_iota(jnp.int32, (block, 1), 0)
            done[slot, pl.ds(start, block)] = jnp.where(row < limit_table[slot], scaled, 0.0).astype(jnp.bfloat16)

        store(part).start()

    small = [
        pltpu.make_async_copy(dest_hbm, dest_row, small_sem.at[0]),
        pltpu.make_async_copy(key_hbm, key_row, small_sem.at[1]),
        pltpu.make_async_copy(dest_hbm, dest_ref, small_sem.at[2]),
        pltpu.make_async_copy(lengths_hbm, lengths_ref, small_sem.at[3]),
        pltpu.make_async_copy(gain_hbm, gain_ref, small_sem.at[4]),
    ]
    load = pltpu.make_async_copy(x_ref, raw, x_sem)
    for copy in small:
        copy.start()
    load.start()
    barrier = pltpu.get_barrier_semaphore()
    for step in range(1, devices):
        pl.semaphore_signal(
            barrier, inc=1, device_id=place_of(lax.rem(me + step, devices)), device_id_type=MESH
        )
    for copy in small:
        copy.wait()
    mine[...] = jnp.zeros_like(mine)
    mine[0:1, 0:tiles_here] = dest_row[...]
    mine[1:2, 0:tiles_here] = key_row[...]
    table_ref[me] = mine[...]

    pl.semaphore_wait(barrier, devices - 1)
    for step in range(1, devices):
        row_copy(step, lax.rem(me + step, devices), me).start()
    depths = [lax.rem(dest_ref[0, i], depth) for i in range(tiles_here)]
    places, limits = [], []
    for i in range(tiles_here):
        spot = jnp.int32(0)
        for j in range(i):
            spot = spot + jnp.where(depths[j] == depths[i], 1, 0)
        places.append(depths[i] * per_peer + spot)
        tile = me * tiles_here + i
        limits.append(jnp.maximum(lengths_ref[0, tile // TILES_SEQ] - tile % TILES_SEQ * tile_rows, 0))
    for slot in range(slots):
        tile, limit = jnp.int32(0), jnp.int32(0)
        for i in range(tiles_here):
            tile = jnp.where(places[i] == slot, i, tile)
            limit = jnp.where(places[i] == slot, limits[i], limit)
        first_table[slot] = tile
        limit_table[slot] = limit

    load.wait()
    for part in range(tile_rows // block):
        normalize(part)
        if part == 0:
            for dz in range(1, depth):
                early_copy(dz, lax.rem(gz + dz, depth), gz).start()
    for step in range(1, devices):
        source = lax.rem(me + devices - step, devices)
        row_copy(step, source, source).wait()
    for dz in range(1, depth):
        origin = lax.rem(gz + depth - dz, depth)
        early_copy(dz, origin, origin).wait()
    for part in range(tile_rows // block):
        store(part).wait()


def line_kernel(
    sizes, plan_ref, x_ref, early_ref, received,
    plan, plan_sem, x_sem, early_sem, y_send, y_recv, a_send, a_recv, b_send, b_recv,
    g_send, g_recv, *buffers,
):
    nx, ny, depth, per_peer, pieces, near, far, back, at = sizes
    chunks = len(pieces)
    half = ny // 2
    slots = depth * per_peer
    pool, inflow, inward, outward, outgoing = (
        buffers[i * chunks : (i + 1) * chunks] for i in range(5)
    )
    gx, gy, gz = lax.axis_index("gx"), lax.axis_index("gy"), lax.axis_index("gz")
    low = gy < half
    level = jnp.where(low, gy, ny - 1 - gy)
    inner = jnp.where(low, gy + 1, gy - 1)
    outer = jnp.clip(jnp.where(low, gy - 1, gy + 1), 0, ny - 1)
    middle = level == half - 1

    def piece(ref, start, size, c):
        row, rows, column, columns = pieces[c]
        return ref.at[pl.ds(start, size), pl.ds(row, rows), pl.ds(column, columns)]

    def load(c):
        return pltpu.make_async_copy(
            piece(x_ref, gz * per_peer, per_peer, c),
            pool[c].at[pl.ds(gz * per_peer, per_peer)],
            x_sem.at[c],
        )

    ready = [c for c in range(chunks) if pieces[c][0] + pieces[c][1] <= early_ref.shape[1]]

    def early_load(c, dz):
        origin = lax.rem(gz + depth - dz, depth)
        return pltpu.make_async_copy(
            piece(early_ref, origin * per_peer, per_peer, c),
            pool[c].at[pl.ds(origin * per_peer, per_peer)],
            early_sem.at[c, dz - 1],
        )

    def y_copy(c, dz, peer, origin):
        return pltpu.make_async_remote_copy(
            src_ref=piece(x_ref, peer * per_peer, per_peer, c),
            dst_ref=pool[c].at[pl.ds(origin * per_peer, per_peer)],
            send_sem=y_send.at[c, dz - 1],
            recv_sem=y_recv.at[c, dz - 1],
            device_id=(gx, gy, peer),
            device_id_type=MESH,
        )

    def near_copy(c, peer):
        return pltpu.make_async_remote_copy(
            src_ref=inward[c].at[pl.ds(0, near)],
            dst_ref=pool[c].at[pl.ds(slots, near)],
            send_sem=a_send.at[c],
            recv_sem=a_recv.at[c],
            device_id=(gx, peer, gz),
            device_id_type=MESH,
        )

    def cross_copy(c, peer):
        return pltpu.make_async_remote_copy(
            src_ref=inward[c],
            dst_ref=inflow[c],
            send_sem=a_send.at[c],
            recv_sem=b_recv.at[c],
            device_id=(gx, peer, gz),
            device_id_type=MESH,
        )

    def back_copy(c, peer):
        return pltpu.make_async_remote_copy(
            src_ref=outward[c],
            dst_ref=inflow[c].at[pl.ds(0, back)],
            send_sem=b_send.at[c],
            recv_sem=b_recv.at[c],
            device_id=(gx, peer, gz),
            device_id_type=MESH,
        )

    def g_copy(c, dx, peer, origin):
        return pltpu.make_async_remote_copy(
            src_ref=outgoing[c].at[pl.ds((dx - 1) * ny, ny)],
            dst_ref=piece(received, origin * ny, ny, c),
            send_sem=g_send.at[c, dx - 1],
            recv_sem=g_recv.at[c, dx - 1],
            device_id=(peer, gy, gz),
            device_id_type=MESH,
        )

    def either(c, code):
        held = pool[c][jnp.minimum(code, slots + near - 1)]
        came = inflow[c][jnp.clip(code - slots - near, 0, far - 1)]
        return jnp.where(code < slots + near, held, came)

    def send_inward(c, crosses, relays):
        load(c).wait()
        for dz in range(1, depth):
            origin = lax.rem(gz + depth - dz, depth)
            if c in ready:
                early_load(c, dz).wait()
            else:
                y_copy(c, dz, origin, origin).wait_recv()
        if relays:
            near_copy(c, outer).wait_recv()

        @pl.loop(0, far if crosses else near)
        def _(p):
            inward[c][p] = pool[c][plan[0, at["inward"] + p]]

        if crosses:
            cross_copy(c, inner).start()
        else:
            near_copy(c, inner).start()

    def deliver(c, crosses, relays):
        if crosses:
            cross_copy(c, inner).wait_recv()
        else:
            back_copy(c, inner).wait_recv()
        if relays:

            @pl.loop(0, back)
            def _(p):
                outward[c][p] = either(c, plan[0, at["outward"] + p])

            back_copy(c, outer).start()

        @pl.loop(0, (nx - 1) * ny)
        def _(k):
            outgoing[c][k] = either(c, plan[0, at["deliver"] + ny + k])

        for dx in range(1, nx):
            g_copy(c, dx, lax.rem(gx + dx, nx), gx).start()

        @pl.loop(0, ny)
        def _(k):
            row, rows, column, columns = pieces[c]
            received[gx * ny + k, pl.ds(row, rows), pl.ds(column, columns)] = either(
                c, plan[0, at["deliver"] + k]
            )

    def stream(crosses, relays):
        area = [rows * columns / (pieces[-1][0] + pieces[-1][1]) for _, rows, _, columns in pieces]
        area = [a * 16 / sum(area) for a in area]
        events = []
        for c in range(chunks):
            upto = sum(area[: c + 1])
            sent = near * (upto - area[c])
            landed = near * area[0] + far * (upto + area[c]) + LATENCY
            if crosses or relays:
                sent, landed = c, c + AHEAD + 0.5
            events.append((sent, 0, c))
            events.append((landed, 1, c))
        for _, kind, c in sorted(events):
            if kind == 0:
                send_inward(c, crosses, relays)
            else:
                deliver(c, crosses, relays)
        for c in range(chunks):
            if crosses:
                cross_copy(c, inner).wait_send()
            else:
                near_copy(c, inner).wait_send()
            if relays:
                back_copy(c, outer).wait_send()

    fetch = pltpu.make_async_copy(plan_ref, plan, plan_sem)
    fetch.start()
    for c in range(chunks):
        load(c).start()
        if c in ready:
            for dz in range(1, depth):
                early_load(c, dz).start()
    barrier = pltpu.get_barrier_semaphore()
    for dz in range(1, depth):
        pl.semaphore_signal(
            barrier, inc=1, device_id=(gx, gy, lax.rem(gz + dz, depth)), device_id_type=MESH
        )
    for dx in range(1, nx):
        pl.semaphore_signal(
            barrier, inc=1, device_id=(lax.rem(gx + dx, nx), gy, gz), device_id_type=MESH
        )
    pl.semaphore_signal(barrier, inc=1, device_id=(gx, inner, gz), device_id_type=MESH)

    @pl.when(level > 0)
    def _():
        pl.semaphore_signal(barrier, inc=1, device_id=(gx, outer, gz), device_id_type=MESH)

    pl.semaphore_wait(barrier, depth - 1 + nx - 1 + 1 + jnp.where(level > 0, 1, 0))
    for c in range(len(ready), chunks):
        for dz in range(1, depth):
            y_copy(c, dz, lax.rem(gz + dz, depth), gz).start()
    fetch.wait()

    if half == 1:
        stream(True, False)
    else:
        pl.when(level == 0)(lambda: stream(False, False))
        pl.when(middle)(lambda: stream(True, True))
        if half > 2:
            pl.when((level > 0) & jnp.logical_not(middle))(lambda: stream(False, True))

    for c in range(chunks):
        if c not in ready:
            for dz in range(1, depth):
                y_copy(c, dz, lax.rem(gz + dz, depth), gz).wait_send()
        for dx in range(1, nx):
            origin = lax.rem(gx + nx - dx, nx)
            g_copy(c, dx, origin, origin).wait()


def count(mask):
    return jnp.sum(mask.astype(jnp.int32), axis=1)


def pick(value, mask, position, wanted):
    hit = mask[None, :] & (position[None, :] == jnp.arange(wanted, dtype=jnp.int32)[:, None])
    return jnp.sum(jnp.where(hit, value[None, :], 0), axis=1)


def shards(embeds, dest_device, shuffle_key, lengths, gain):
    tiles_here, tile_rows, width = embeds.shape
    nx, ny, depth = lax.axis_size("gx"), lax.axis_size("gy"), lax.axis_size("gz")
    devices = nx * ny * depth
    per_peer = (tiles_here + depth - 1) // depth
    slots = depth * per_peer
    half = ny // 2
    cap = 2 * tiles_here
    if ny % 2 or tile_rows % 128 or width % 512 or slots > tiles_here:
        return direct(embeds, dest_device, shuffle_key, lengths, gain)

    most = half * min(tiles_here, nx * half)
    near_most = max([(e + 1) * min(tiles_here, nx * (ny - 1 - e)) for e in range(half - 1)] + [1])
    back_most = max([(ny - e) * min(tiles_here, nx * e) for e in range(1, half)] + [1])
    classes = sorted({max(near_most, most * part // 16) for part in CLASSES})

    vmem = pl.BlockSpec(memory_space=pltpu.VMEM)
    smem = pl.BlockSpec(memory_space=pltpu.SMEM)
    hbm = pl.BlockSpec(memory_space=pl.ANY)
    lanes = -(-tiles_here // 128) * 128
    early_rows = tile_rows // 16
    table, normed, early = pl.pallas_call(
        functools.partial(table_kernel, (nx, ny, depth, per_peer)),
        out_shape=(
            jax.ShapeDtypeStruct((devices, 2, lanes), jnp.int32),
            pltpu.HBM((slots, tile_rows, width), jnp.bfloat16),
            pltpu.HBM((slots, early_rows, width), jnp.bfloat16),
        ),
        in_specs=[pl.BlockSpec(memory_space=pltpu.HBM)] * 5,
        out_specs=(vmem, pl.BlockSpec(memory_space=pltpu.HBM), pl.BlockSpec(memory_space=pltpu.HBM)),
        scratch_shapes=[
            pltpu.SMEM((1, tiles_here), jnp.int32),
            pltpu.SMEM((1, lengths.shape[0]), jnp.int32),
            pltpu.VMEM((1, tiles_here), jnp.int32),
            pltpu.VMEM((1, tiles_here), jnp.int32),
            pltpu.VMEM((1, width), jnp.float32),
            pltpu.SemaphoreType.DMA((5,)),
            pltpu.VMEM((2, lanes), jnp.int32),
            pltpu.SMEM((slots,), jnp.int32),
            pltpu.SMEM((slots,), jnp.int32),
            pltpu.VMEM((tiles_here, tile_rows, width), jnp.bfloat16),
            pltpu.VMEM((slots, tile_rows, width), jnp.bfloat16),
            pltpu.SemaphoreType.DMA((devices - 1,)),
            pltpu.SemaphoreType.DMA((devices - 1,)),
            pltpu.SemaphoreType.DMA,
            pltpu.SemaphoreType.DMA((tile_rows // 16,)),
            pltpu.SemaphoreType.DMA((depth - 1,)),
            pltpu.SemaphoreType.DMA((depth - 1,)),
        ],
        compiler_params=pltpu.CompilerParams(
            collective_id=0, has_side_effects=True, vmem_limit_bytes=56 * 1024 * 1024
        ),
        name="tables",
    )(dest_device[None, :], shuffle_key[None, :], lengths[None, :], embeds, gain.reshape(1, width))

    gx, gy, gz = lax.axis_index("gx"), lax.axis_index("gy"), lax.axis_index("gz")
    group = gx * ny + gy
    me = group * depth + gz
    dest = table[:, 0, :tiles_here].reshape(-1)
    keys = table[:, 1, :tiles_here].reshape(-1)
    order = jnp.arange(devices * tiles_here, dtype=jnp.int32)
    before = order[None, :] < order[:, None]
    source = order // tiles_here
    from_x, from_y = source // (ny * depth), source // depth % ny
    to_x, to_y, to_z = dest // (ny * depth), dest // depth % ny, dest % depth

    bounds = jnp.arange(ny - 1, dtype=jnp.int32)
    lane = from_x * depth + to_z
    hop_up = (from_y[None, :] <= bounds[:, None]) & (to_y[None, :] > bounds[:, None])
    hop_down = (from_y[None, :] > bounds[:, None]) & (to_y[None, :] <= bounds[:, None])
    hops = jnp.concatenate([hop_up, hop_down])
    in_lane = lane[None, :] == jnp.arange(nx * depth, dtype=jnp.int32)[:, None]
    load = jnp.sum((hops[:, None, :] & in_lane[None, :, :]).astype(jnp.int32), axis=2)

    low = gy < half
    level = jnp.where(low, gy, ny - 1 - gy)
    depth_from = jnp.where(low, from_y, ny - 1 - from_y)
    depth_to = jnp.where(low, to_y, ny - 1 - to_y)
    in_my_lane = (from_x == gx) & (to_z == gz)
    inward = in_my_lane & (depth_from <= level) & (depth_to > level)
    near_in = in_my_lane & (depth_from < level) & (depth_to >= level)
    outward = in_my_lane & (depth_from >= level) & (depth_to < level)
    far_in = in_my_lane & (depth_from > level) & (depth_to <= level)
    landing = in_my_lane & (depth_to == level)
    to_me = dest == me

    same_source = source[:, None] == source[None, :]
    spot = count(before & same_source & (to_z[:, None] == to_z[None, :]))
    at_inward = count(before & inward[None, :])
    at_near = count(before & near_in[None, :])
    at_outward = count(before & outward[None, :])
    at_far = count(before & far_in[None, :])
    at_landing = count(before & (landing[None, :] & (to_x[:, None] == to_x[None, :])))
    at_me = count(before & (to_me[None, :] & (from_x[:, None] == from_x[None, :])))
    rank = count((keys[None, :] < keys[:, None]) & to_me[None, :])
    own_slot = source % depth * per_peer + spot

    over = load.reshape(-1)[None, :] > jnp.array(classes[:-1], jnp.int32)[:, None]
    chosen = jnp.sum(jnp.any(over, axis=1).astype(jnp.int32))
    code = jnp.where(
        depth_from == level,
        own_slot,
        jnp.where(depth_from < level, slots + at_near, slots + near_most + at_far),
    )
    parts = {
        "inward": pick(code, inward, at_inward, most),
        "outward": pick(code, outward, at_outward, back_most),
        "deliver": pick(code, landing, (to_x - gx) % nx * ny + at_landing, nx * ny),
    }
    at, total = {}, 0
    for name, part in parts.items():
        at[name] = total
        total += part.shape[0]
    plan = jnp.pad(jnp.concatenate(list(parts.values())), (0, -total % 128))[None, :]
    which = pick(from_x * ny + at_me + 1, to_me, rank, cap)

    pieces, done = [], 0
    for part in CHUNKS:
        row, column = done // 4 * tile_rows // 16, done % 4 * width // 4
        if part % 4 == 0:
            pieces.append((row, part // 4 * tile_rows // 16, 0, width))
        else:
            pieces.append((row, tile_rows // 16, column, part * width // 4))
        done += part
    pieces = tuple(pieces)
    chunks = len(pieces)

    def branch(index, far):
        def run(plan, normed, early, chosen_rows, filled):
            near, back = near_most, min(far, back_most)
            counts = ((slots + near,), (far,), (far,), (back,), ((nx - 1) * ny,))
            received = pl.pallas_call(
                functools.partial(
                    line_kernel, (nx, ny, depth, per_peer, pieces, near, far, back, at)
                ),
                out_shape=pltpu.VMEM((nx * ny, tile_rows, width), jnp.bfloat16),
                in_specs=[hbm] + [pl.BlockSpec(memory_space=pltpu.HBM)] * 2,
                out_specs=vmem,
                scratch_shapes=[
                    pltpu.SMEM(plan.shape, jnp.int32),
                    pltpu.SemaphoreType.DMA,
                    pltpu.SemaphoreType.DMA((chunks,)),
                    pltpu.SemaphoreType.DMA((chunks, depth - 1)),
                    pltpu.SemaphoreType.DMA((chunks, depth - 1)),
                    pltpu.SemaphoreType.DMA((chunks, depth - 1)),
                    pltpu.SemaphoreType.DMA((chunks,)),
                    pltpu.SemaphoreType.DMA((chunks,)),
                    pltpu.SemaphoreType.DMA((chunks,)),
                    pltpu.SemaphoreType.DMA((chunks,)),
                    pltpu.SemaphoreType.DMA((chunks, nx - 1)),
                    pltpu.SemaphoreType.DMA((chunks, nx - 1)),
                ]
                + [
                    pltpu.VMEM((*lead, rows, columns), jnp.bfloat16)
                    for lead in counts
                    for _, rows, _, columns in pieces
                ],
                compiler_params=pltpu.CompilerParams(
                    collective_id=1 + index, has_side_effects=True, vmem_limit_bytes=44 * 1024 * 1024
                ),
                name=f"line{far}",
            )(plan, normed, early)
            return pl.pallas_call(
                place_kernel,
                out_shape=pltpu.HBM((cap, tile_rows, width), jnp.bfloat16),
                in_specs=[smem, smem, vmem],
                out_specs=pl.BlockSpec(memory_space=pltpu.HBM),
                scratch_shapes=[
                    pltpu.VMEM((tile_rows, width), jnp.bfloat16),
                    pltpu.SemaphoreType.DMA((cap,)),
                ],
                compiler_params=pltpu.CompilerParams(vmem_limit_bytes=24 * 1024 * 1024),
                name="place",
            )(chosen_rows, filled, received)

        return run

    return lax.switch(
        chosen,
        [branch(i, far) for i, far in enumerate(classes)],
        plan,
        normed,
        early,
        jnp.maximum(which - 1, 0),
        (which > 0).astype(jnp.int32),
    )


def solution(mesh):
    return jax.shard_map(
        shards,
        mesh=mesh,
        in_specs=(
            P(("gx", "gy", "gz"), None, None),
            P(("gx", "gy", "gz")),
            P(("gx", "gy", "gz")),
            P(),
            P(),
        ),
        out_specs=P(("gx", "gy", "gz"), None, None),
        check_vma=False,
    )
```
